32 devices in a mesh: gx: 2 (over x), gy: 4 (over z), gz: 4 (over y, core).
Axes of the slice: x: 2, y: 2, z: 4, core: 2. Of those that a mesh axis runs over, the one named last changes fastest.
Arguments:
- state_old: float32 [5, 32, 128, 512], P(None, 'gx', 'gy', 'gz'), as said below
- state_section: float32 [5, 32, 128, 512], P(None, 'gx', 'gy', 'gz'), as said below
- panel_record: bfloat16 [131072, 512], P(('gx', 'gy', 'gz')), may hold values from -6 to 6
- panel_cell: int32 [1024, 128], P(('gx', 'gy', 'gz')), may hold values from 0 to 65535
- panel_angles: float32 [2, 131072], P(None, ('gx', 'gy', 'gz')), may hold values from -3.140625 to 3.140625
- owned_blocks: int32 [32], P(('gx', 'gy', 'gz')), may hold values from 1 to 32, 256 in all
- listener_angles: float32 [2, 1024], replicated, may hold values from -3.140625 to 3.140625
- listener_range: float32 [1024], replicated, may hold values from 1.2 to 2.5
Outputs:
- state_next: float32 [5, 32, 128, 512], P(None, 'gx', 'gy', 'gz')
- observer_spectra: float32 [2, 1024, 128], P(None, 'gz')
The draws below stay inside these ranges and needn't reach their ends.
Inputs may be any that keep to these rules, and one draw needn't show every extreme that they name: `state_old`: density between 0.5 and 2, velocity components of magnitude 0.3 at most, stiffened-gas pressure between 0.3 and 2. `state_section`: density between 0.5 and 2, velocity components of magnitude 0.3 at most, stiffened-gas pressure between 0.3 and 2. A device's live blocks fill its first owned_blocks slots; some device owns 32 blocks, and they total 8 times the number of devices.
All inputs are finite; a program needn't handle non-finite values.
Results may differ from the reference program's by a relative error of at most 0.0003.
The reference program's roundings to bfloat16 on the way count: a program that leaves them out, or rounds other values in their place, can miss the bound.
Values may be sent and summed in bfloat16 or wider, within the bound.
No kernel may reach another device: no remote copies, remote signals or barrier semaphores. Data moves between devices by JAX's collectives and lax.ppermute only.
A program may use at most 64 MiB of HBM per device.

```python
import math
import jax
import jax.numpy as jnp
import numpy as np
from jax import lax

CX = 16
CY = 32
CZ = 128
SAMPLES = 512
FREQS = 128
BLOCK_PANELS = 128
SLOTS = 32
LIVE_DEV = 8
NX = 32
NY = 128
NZ = 512
CELLS = 65536
BLOCKS = 1024
PANELS = 131072
OBS = 1024
N_GX = 2
N_GY = 4
N_GZ = 4
DEVICES = 32


GAMMA_GAS = 4.4


PRESSURE_INF = 1.0


def state_field(base_key):
    subkeys = jax.random.split(base_key, 3)
    grid_shape = (NX, NY, NZ)
    density = jnp.exp(jax.random.uniform(subkeys[0], grid_shape, jnp.float32, math.log(0.5), math.log(2.0)))
    velocity = jax.random.uniform(subkeys[1], (3,) + grid_shape, jnp.float32, -0.3, 0.3)
    pressure = jax.random.uniform(subkeys[2], grid_shape, jnp.float32, 0.3, 2.0)
    momenta = density[None] * velocity
    energy = (pressure + GAMMA_GAS * PRESSURE_INF) / (GAMMA_GAS - 1.0) + 0.5 * density * jnp.sum(velocity * velocity, axis=0)
    return jnp.concatenate([density[None], momenta, energy[None]], axis=0)


def draw_state_old(key, part):
    return state_field(jax.random.fold_in(key, 11))


def draw_state_section(key, part):
    return state_field(jax.random.fold_in(key, 23))


def touch_ends(values, stream_key, least, largest):
    longest = values.shape.index(max(values.shape))
    spots = []
    for shift in (0, 1):
        where = [jax.random.randint(jax.random.fold_in(stream_key, axis), (), 0, length) for axis, length in enumerate(values.shape)]
        where[longest] = (where[longest] + shift) % values.shape[longest]
        spots.append(tuple(where))
    return values.at[spots[0]].set(least).at[spots[1]].set(largest)


def steps_of(rng, extent, cuts, low, high):
    level, own = 1.0, jax.random.fold_in(rng, 6)
    for position, shards_of in cuts:
        steps = jnp.exp(jax.random.uniform(jax.random.fold_in(own, position), (shards_of,), jnp.float32, low / len(cuts), high / len(cuts)))
        level = level * jnp.repeat(steps, extent[position] // shards_of).reshape([-1 if axis == position else 1 for axis in range(len(extent))])
    return level


def profile(count, total, bound, lean):
    portions = [(1 << 20) // math.isqrt(grade ** lean) + 1 for grade in range(2, count + 1)]
    spare, given = total - bound - (count - 1), [1] * (count - 1)
    while spare > 0:
        movable = [i for i in range(count - 1) if given[i] < bound]
        whole, left = sum([portions[i] for i in movable]), spare
        for i in movable:
            more = min(bound - given[i], max(1, left * portions[i] // whole), spare)
            given[i] = given[i] + more
            spare = spare - more
    return np.array([bound] + given)


def uneven(rng, number_of, total, reach, skew):
    if number_of == 2:
        one = jax.random.randint(rng, (), max(1, total - reach), min(reach, total - 1) + 1)
        return jnp.stack([one, total - one])
    sizes = jnp.asarray(profile(number_of, total, reach, skew), jnp.int32)
    pairs = (number_of - 1) // 2
    donor, sink = sizes[1:1 + 2 * pairs:2], sizes[2:2 + 2 * pairs:2]
    slack = jnp.minimum(donor - 1, reach - sink)
    moved = jax.random.randint(jax.random.fold_in(rng, 1), (pairs,), 0, 1 << 20) % (slack + 1)
    sizes = sizes.at[1:1 + 2 * pairs:2].set(donor - moved).at[2:2 + 2 * pairs:2].set(sink + moved)
    return sizes[jax.random.permutation(jax.random.fold_in(rng, 2), number_of)]


def noise(rng, dims, spread, bound, cuts=(), held_as=jnp.bfloat16):
    result = jax.random.normal(rng, dims, jnp.float32) * spread
    if len(cuts) > 0:
        result = steps_of(rng, dims, cuts, -0.22, 0.18) * result
    return jnp.clip(result, min=-bound, max=bound).astype(held_as)


def setup_inputs(seed: int = 0) -> dict:
    keys = jax.random.split(jax.random.key(seed), 9)
    return {
        "state_old": draw_state_old(jax.random.fold_in(keys[8], 71), 0),
        "state_section": draw_state_section(jax.random.fold_in(keys[8], 71), 0),
        "panel_record": noise(keys[2], (PANELS, SAMPLES), 1.0, 6.0, ((0, 32),)),
        "panel_cell": touch_ends(jax.random.randint(keys[3], (BLOCKS, BLOCK_PANELS), 0, CELLS), jax.random.fold_in(keys[3], 1), 0, CELLS - 1).astype(jnp.int32),
        "panel_angles": jnp.clip(jax.random.uniform(keys[4], (2, PANELS), jnp.float32, -3.140625, 3.140625), -3.140625, 3.140625),
        "owned_blocks": uneven(keys[5], DEVICES, LIVE_DEV * DEVICES, SLOTS, 2).astype(jnp.int32),
        "listener_angles": jnp.clip(jax.random.uniform(keys[6], (2, OBS), jnp.float32, -3.140625, 3.140625), -3.140625, 3.140625),
        "listener_range": jnp.clip(jnp.exp(jax.random.uniform(keys[7], (OBS,), jnp.float32, math.log(1.2), math.log(2.5))), 1.2, 2.5),
    }


GAMMA_GAS = 4.4
PRESSURE_INF = 1.0
WENO_EPS = 1e-06
WAVE_STEP = 0.25
COURANT = 0.08

def weno_face(far_left, near_left, middle, near_right, far_right):
    cand_a = (2.0 * far_left - 7.0 * near_left + 11.0 * middle) / 6.0
    cand_b = (-near_left + 5.0 * middle + 2.0 * near_right) / 6.0
    cand_c = (2.0 * middle + 5.0 * near_right - far_right) / 6.0
    rough_a = 13.0 / 12.0 * (far_left - 2.0 * near_left + middle) ** 2 + 0.25 * (far_left - 4.0 * near_left + 3.0 * middle) ** 2
    rough_b = 13.0 / 12.0 * (near_left - 2.0 * middle + near_right) ** 2 + 0.25 * (near_left - near_right) ** 2
    rough_c = 13.0 / 12.0 * (middle - 2.0 * near_right + far_right) ** 2 + 0.25 * (3.0 * middle - 4.0 * near_right + far_right) ** 2
    weight_a = 0.1 / (WENO_EPS + rough_a) ** 2
    weight_b = 0.6 / (WENO_EPS + rough_b) ** 2
    weight_c = 0.3 / (WENO_EPS + rough_c) ** 2
    return (weight_a * cand_a + weight_b * cand_b + weight_c * cand_c) / (weight_a + weight_b + weight_c)

def euler_flux(state_slab, axis_d):
    density = state_slab[0]
    momenta = state_slab[1:4]
    energy = state_slab[4]
    velocity = momenta / density[None]
    kinetic = 0.5 * lax.optimization_barrier(jnp.sum(momenta * velocity, axis=0))
    pressure = (GAMMA_GAS - 1.0) * (energy - kinetic) - GAMMA_GAS * PRESSURE_INF
    normal_speed = velocity[axis_d]
    sound_speed = jnp.sqrt(GAMMA_GAS * (pressure + PRESSURE_INF) / density)
    rows_out = [momenta[axis_d]]
    for component in range(3):
        carried = momenta[component] * normal_speed
        if component == axis_d:
            carried = carried + pressure
        rows_out.append(carried)
    rows_out.append((energy + pressure) * normal_speed)
    return (jnp.stack(rows_out), jnp.abs(normal_speed) + sound_speed)

def face_difference(padded, axis_d, count_d):
    array_axis = axis_d + 1
    picker = [slice(None), slice(3, -3), slice(3, -3), slice(3, -3)]
    picker[array_axis] = slice(None)
    state_slab = padded[tuple(picker)]
    fluxes, speeds = euler_flux(state_slab, axis_d)
    cell_count = state_slab.shape[array_axis] - 6

    def shifted(values, offset, along):
        return lax.slice_in_dim(values, offset, offset + cell_count + 1, axis=along)
    wave_speed = shifted(speeds, 0, axis_d)
    for offset in range(1, 6):
        wave_speed = jnp.maximum(wave_speed, shifted(speeds, offset, axis_d))
    split_up = [0.5 * (shifted(fluxes, offset, array_axis) + wave_speed[None] * shifted(state_slab, offset, array_axis)) for offset in range(6)]
    split_down = [0.5 * (shifted(fluxes, offset, array_axis) - wave_speed[None] * shifted(state_slab, offset, array_axis)) for offset in range(6)]
    face_flux = weno_face(split_up[0], split_up[1], split_up[2], split_up[3], split_up[4]) + weno_face(split_down[5], split_down[4], split_down[3], split_down[2], split_down[1])
    after = lax.slice_in_dim(face_flux, 1, cell_count + 1, axis=array_axis)
    before = lax.slice_in_dim(face_flux, 0, cell_count, axis=array_axis)
    return (after - before) * float(count_d)

def section_update(padded, old_block, counts, step_size):
    change = face_difference(padded, 0, counts[0]) + face_difference(padded, 1, counts[1]) + face_difference(padded, 2, counts[2])
    return 0.75 * old_block + 0.25 * (padded[:, 3:-3, 3:-3, 3:-3] - step_size * change)

def directions(angles):
    polar_angle = 0.5 * angles[0]
    azimuth = angles[1]
    return jnp.stack([jnp.cos(polar_angle) * jnp.cos(azimuth), jnp.cos(polar_angle) * jnp.sin(azimuth), jnp.sin(polar_angle)])

def panel_places(cell_rows, block_x, block_y, block_z, cells_x, cells_y, cells_z, counts):
    along_x = cell_rows // (cells_y * cells_z)
    along_y = cell_rows // cells_z % cells_y
    along_z = cell_rows % cells_z
    place_x = ((block_x * cells_x + along_x).astype(jnp.float32) + 0.5) / counts[0]
    place_y = ((block_y * cells_y + along_y).astype(jnp.float32) + 0.5) / counts[1]
    place_z = ((block_z * cells_z + along_z).astype(jnp.float32) + 0.5) / counts[2]
    return jnp.stack([place_x, place_y, place_z], axis=1)

def dft_table(sample_count, freq_count):
    times = jnp.arange(sample_count, dtype=jnp.int32)[:, None]
    orders = jnp.arange(1, freq_count + 1, dtype=jnp.int32)[None, :]
    phases = 2.0 * math.pi / sample_count * (times * orders % sample_count).astype(jnp.float32)
    scaling = 1.0 / math.sqrt(sample_count)
    return (jnp.concatenate([jnp.cos(phases), -jnp.sin(phases)], axis=1) * scaling).astype(jnp.bfloat16)

def observer_terms(sources, places, normals, live_flags, dft_rows, listeners, wave_numbers):
    spectra = jnp.einsum('gpt,tk->gpk', sources.astype(jnp.float32), dft_rows.astype(jnp.float32)).astype(jnp.bfloat16)
    offsets = listeners[None, :, :, None] - places[:, :, None, :]
    dist_sq = lax.optimization_barrier(jnp.sum(offsets * offsets, axis=1))
    facing = lax.optimization_barrier(jnp.sum(normals[:, :, None, :] * offsets, axis=1))
    weights = (facing / (4.0 * math.pi * dist_sq)).astype(jnp.bfloat16)
    product = jnp.einsum('gop,gpk->gok', weights.astype(jnp.float32), spectra.astype(jnp.float32))
    centres = lax.optimization_barrier(jnp.mean(places, axis=2))
    separation = listeners[None, :, :] - centres[:, :, None]
    centre_reach = jnp.sqrt(lax.optimization_barrier(jnp.sum(separation * separation, axis=1)))
    phase_now = centre_reach[:, :, None] * wave_numbers[None, None, :]
    cosine = jnp.cos(phase_now)
    sine_part = jnp.sin(phase_now)
    freq_count = wave_numbers.shape[0]
    real_part = product[:, :, :freq_count] * cosine + product[:, :, freq_count:] * sine_part
    imag_part = product[:, :, freq_count:] * cosine - product[:, :, :freq_count] * sine_part
    masks = live_flags[:, None, None]
    return jnp.stack([lax.optimization_barrier(jnp.sum(masks * real_part, axis=0)), lax.optimization_barrier(jnp.sum(masks * imag_part, axis=0))])

def reference(state_old, state_section, panel_record, panel_cell, panel_angles, owned_blocks, listener_angles, listener_range):
    counts = (NX, NY, NZ)
    step_size = COURANT / max(NX, NY, NZ)
    padded_all = jnp.pad(state_section, ((0, 0), (3, 3), (3, 3), (3, 3)), mode='wrap')
    dft_rows = dft_table(SAMPLES, FREQS)
    listeners = 0.5 + listener_range[None, :] * directions(listener_angles)
    wave_numbers = WAVE_STEP * jnp.arange(1, FREQS + 1, dtype=jnp.int32).astype(jnp.float32)
    records = panel_record.reshape(DEVICES, SLOTS, BLOCK_PANELS, SAMPLES)
    cell_all = panel_cell.reshape(DEVICES, SLOTS, BLOCK_PANELS)
    angle_all = panel_angles.reshape(2, DEVICES, SLOTS, BLOCK_PANELS)

    def per_device(running, device):
        block_x = device // (N_GY * N_GZ)
        block_y = device // N_GZ % N_GY
        block_z = device % N_GZ
        corner = (jnp.int32(0), (block_x * CX).astype(jnp.int32), (block_y * CY).astype(jnp.int32), (block_z * CZ).astype(jnp.int32))
        padded = lax.dynamic_slice(padded_all, corner, (5, CX + 6, CY + 6, CZ + 6))
        old_block = lax.dynamic_slice(state_old, corner, (5, CX, CY, CZ))
        updated = section_update(padded, old_block, counts, step_size)
        density = updated[0].reshape(CX * CY * CZ)
        cell_rows = cell_all[device]
        sampled = density[cell_rows]
        sources = (records[device].astype(jnp.float32) * sampled[:, :, None]).astype(jnp.bfloat16)
        places = panel_places(cell_rows, block_x, block_y, block_z, CX, CY, CZ, counts)
        normals = jnp.transpose(directions(angle_all[:, device]), (1, 0, 2))
        live_flags = (jnp.arange(SLOTS, dtype=jnp.int32) < owned_blocks[device]).astype(jnp.float32)
        running = running + observer_terms(sources, places, normals, live_flags, dft_rows, listeners, wave_numbers)
        return (running, updated)
    running, blocks_out = lax.scan(per_device, jnp.zeros((2, OBS, FREQS), jnp.float32), jnp.arange(DEVICES, dtype=jnp.int32))
    state_next = blocks_out.reshape(N_GX, N_GY, N_GZ, 5, CX, CY, CZ).transpose(3, 0, 4, 1, 5, 2, 6).reshape(5, NX, NY, NZ)
    return (state_next, running)
```

```python
import math

import jax
import jax.numpy as jnp
import numpy as np
from jax import lax
from jax.experimental import pallas as pl
from jax.experimental.pallas import tpu as pltpu
from jax.sharding import PartitionSpec as P

FREQS = 128
NT = (((1,), (1,)), ((), ()))


GAMMA_GAS = 4.4
PRESSURE_INF = 1.0
WENO_EPS = 1e-06
WAVE_STEP = 0.25
COURANT = 0.08


def with_halo(shard, sides, width):
    for axis, dim in sides:
        size, length = (lax.axis_size(axis), shard.shape[dim])
        up = [(i, (i + 1) % size) for i in range(size)]
        down = [(j, i) for i, j in up]
        last = lax.slice_in_dim(shard, length - width, length, axis=dim)
        initial = lax.slice_in_dim(shard, 0, width, axis=dim)
        before = lax.ppermute(last, axis, up)
        after = lax.ppermute(initial, axis, down)
        shard = jnp.concatenate([before, shard, after], axis=dim)
    return shard


def weno_face(far_left, near_left, middle, near_right, far_right):
    cand_a = (2.0 * far_left - 7.0 * near_left + 11.0 * middle) / 6.0
    cand_b = (-near_left + 5.0 * middle + 2.0 * near_right) / 6.0
    cand_c = (2.0 * middle + 5.0 * near_right - far_right) / 6.0
    rough_a = (
        13.0 / 12.0 * (far_left - 2.0 * near_left + middle) ** 2
        + 0.25 * (far_left - 4.0 * near_left + 3.0 * middle) ** 2
    )
    rough_b = (
        13.0 / 12.0 * (near_left - 2.0 * middle + near_right) ** 2
        + 0.25 * (near_left - near_right) ** 2
    )
    rough_c = (
        13.0 / 12.0 * (middle - 2.0 * near_right + far_right) ** 2
        + 0.25 * (3.0 * middle - 4.0 * near_right + far_right) ** 2
    )
    weight_a = 0.1 / (WENO_EPS + rough_a) ** 2
    weight_b = 0.6 / (WENO_EPS + rough_b) ** 2
    weight_c = 0.3 / (WENO_EPS + rough_c) ** 2
    return (weight_a * cand_a + weight_b * cand_b + weight_c * cand_c) / (
        weight_a + weight_b + weight_c
    )


def euler_flux(state_slab, axis_d):
    density = state_slab[0]
    momenta = state_slab[1:4]
    energy = state_slab[4]
    velocity = momenta / density[None]
    kinetic = 0.5 * jnp.sum(momenta * velocity, axis=0)
    pressure = (GAMMA_GAS - 1.0) * (energy - kinetic) - GAMMA_GAS * PRESSURE_INF
    normal_speed = velocity[axis_d]
    sound_speed = jnp.sqrt(GAMMA_GAS * (pressure + PRESSURE_INF) / density)
    rows_out = [momenta[axis_d]]
    for component in range(3):
        carried = momenta[component] * normal_speed
        if component == axis_d:
            carried = carried + pressure
        rows_out.append(carried)
    rows_out.append((energy + pressure) * normal_speed)
    return (jnp.stack(rows_out), jnp.abs(normal_speed) + sound_speed)


def face_difference(padded, axis_d, count_d):
    array_axis = axis_d + 1
    picker = [slice(None), slice(3, -3), slice(3, -3), slice(3, -3)]
    picker[array_axis] = slice(None)
    state_slab = padded[tuple(picker)]
    fluxes, speeds = euler_flux(state_slab, axis_d)
    cell_count = state_slab.shape[array_axis] - 6

    def shifted(values, offset, along):
        return lax.slice_in_dim(values, offset, offset + cell_count + 1, axis=along)

    wave_speed = shifted(speeds, 0, axis_d)
    for offset in range(1, 6):
        wave_speed = jnp.maximum(wave_speed, shifted(speeds, offset, axis_d))
    split_up = [
        0.5
        * (
            shifted(fluxes, offset, array_axis)
            + wave_speed[None] * shifted(state_slab, offset, array_axis)
        )
        for offset in range(6)
    ]
    split_down = [
        0.5
        * (
            shifted(fluxes, offset, array_axis)
            - wave_speed[None] * shifted(state_slab, offset, array_axis)
        )
        for offset in range(6)
    ]
    face_flux = weno_face(
        split_up[0], split_up[1], split_up[2], split_up[3], split_up[4]
    ) + weno_face(split_down[5], split_down[4], split_down[3], split_down[2], split_down[1])
    after = lax.slice_in_dim(face_flux, 1, cell_count + 1, axis=array_axis)
    before = lax.slice_in_dim(face_flux, 0, cell_count, axis=array_axis)
    return (after - before) * float(count_d)


def section_update(padded, old_block, counts, step_size):
    change = (
        face_difference(padded, 0, counts[0])
        + face_difference(padded, 1, counts[1])
        + face_difference(padded, 2, counts[2])
    )
    return 0.75 * old_block + 0.25 * (padded[:, 3:-3, 3:-3, 3:-3] - step_size * change)


def directions(angles):
    polar_angle = 0.5 * angles[0]
    azimuth = angles[1]
    return jnp.stack(
        [
            jnp.cos(polar_angle) * jnp.cos(azimuth),
            jnp.cos(polar_angle) * jnp.sin(azimuth),
            jnp.sin(polar_angle),
        ]
    )


def panel_places(cell_rows, block_x, block_y, block_z, cells_x, cells_y, cells_z, counts):
    along_x = cell_rows // (cells_y * cells_z)
    along_y = cell_rows // cells_z % cells_y
    along_z = cell_rows % cells_z
    place_x = ((block_x * cells_x + along_x).astype(jnp.float32) + 0.5) / counts[0]
    place_y = ((block_y * cells_y + along_y).astype(jnp.float32) + 0.5) / counts[1]
    place_z = ((block_z * cells_z + along_z).astype(jnp.float32) + 0.5) / counts[2]
    return jnp.stack([place_x, place_y, place_z], axis=1)


def dft_table(sample_count, freq_count):
    times = np.arange(sample_count, dtype=np.int64)[None, :]
    orders = np.arange(1, freq_count + 1, dtype=np.int64)[:, None]
    phases = (np.float32(2.0 * math.pi / sample_count) * (times * orders % sample_count).astype(np.float32)).astype(np.float64)
    scaling = 1.0 / math.sqrt(sample_count)
    both = np.concatenate([np.cos(phases), -np.sin(phases)], axis=0).astype(np.float32) * np.float32(scaling)
    return jnp.asarray(both, jnp.bfloat16)


def sincos_turns(turns):
    r = turns - jnp.round(turns)
    x = r * math.pi
    x2 = x * x
    s = 1.0 / 6227020800.0
    s = s * x2 - 1.0 / 39916800.0
    s = s * x2 + 1.0 / 362880.0
    s = s * x2 - 1.0 / 5040.0
    s = s * x2 + 1.0 / 120.0
    s = s * x2 - 1.0 / 6.0
    s = (s * x2) * x + x
    c = 1.0 / 479001600.0
    c = c * x2 - 1.0 / 3628800.0
    c = c * x2 + 1.0 / 40320.0
    c = c * x2 - 1.0 / 720.0
    c = c * x2 + 1.0 / 24.0
    c = c * x2 - 0.5
    c = c * x2 + 1.0
    s2 = s + s
    return 1.0 - s2 * s, s2 * c


def recip(d):
    r = pl.reciprocal(d, approx=True)
    return r * (2.0 - d * r)


def panels_kernel(live, dens, rec, geo, cell, lis, table, out, dens3, lisb, sp, wts, prod, fine, coarse, acc):
    slots, bp = cell.shape
    rows = dens.shape[0]
    tiles = lis.shape[1]
    half = table.shape[0] // 2
    count = live[0]

    d = dens[...]
    hi = d.astype(jnp.bfloat16)
    left = d - hi.astype(jnp.float32)
    mid = left.astype(jnp.bfloat16)
    lo = (left - mid.astype(jnp.float32)).astype(jnp.bfloat16)
    dens3[:, 0:128] = hi
    dens3[:, 128:256] = mid
    dens3[:, 256:384] = lo
    for k in range(3):
        for t in range(tiles):
            row = lis[k, t : t + 1, :]
            lisb[k, t * 128 : (t + 1) * 128, :] = jnp.transpose(jnp.broadcast_to(row, (128, 128)))
    acc[...] = jnp.zeros(acc.shape, jnp.float32)
    lane = lax.broadcasted_iota(jnp.int32, (128, 128), 1).astype(jnp.float32)

    def spectrum(b, _):
        cells = cell[pl.ds(b, 1), :]
        high = (cells >> 7).astype(jnp.float32)
        low = (cells & 127).astype(jnp.float32)
        high_col = jnp.transpose(jnp.broadcast_to(high, (128, 128)))
        low_col = jnp.transpose(jnp.broadcast_to(low, (128, 128)))
        g = jnp.zeros((128, 384), jnp.float32)
        for j in range(rows // 128):
            onehot = jnp.where(high_col == lane + float(128 * j), 1.0, 0.0).astype(jnp.bfloat16)
            g = g + jnp.dot(onehot, dens3[j * 128 : (j + 1) * 128, :], preferred_element_type=jnp.float32)
        gs = (g[:, 0:128] + g[:, 128:256]) + g[:, 256:384]
        sampled = jnp.sum(jnp.where(low_col == lane, gs, 0.0), axis=1, keepdims=True)
        src = (rec[pl.ds(pl.multiple_of(b * bp, bp), bp), :].astype(jnp.float32) * sampled).astype(jnp.bfloat16)
        sp[b] = lax.dot_general(table[...], src, NT, preferred_element_type=jnp.float32).astype(jnp.bfloat16)
        return 0

    lax.fori_loop(0, count, spectrum, 0)

    sub8 = lax.broadcasted_iota(jnp.int32, (8, 128), 0).astype(jnp.float32) + 1.0
    turn = WAVE_STEP / (2.0 * math.pi)

    def block(b, _):
        px, py, pz, nx, ny, nz = [geo[k, pl.ds(b, 1), :] for k in range(6)]
        cx, cy, cz = [jnp.sum(v, axis=1, keepdims=True) * (1.0 / bp) for v in (px, py, pz)]
        sx, sy, sz = lis[0] - cx, lis[1] - cy, lis[2] - cz
        theta = jnp.sqrt(sx * sx + sy * sy + sz * sz) * turn
        c1, s1 = sincos_turns(8.0 * theta)
        cs = [None, (c1, s1)]
        for a in range(2, half // 8):
            (ca, sa), (cb, sb) = cs[a // 2], cs[a - a // 2]
            cs.append((ca * cb - sa * sb, sa * cb + ca * sb))
        for a in range(1, half // 8):
            coarse[0, a] = cs[a][0]
            coarse[1, a] = cs[a][1]
        coarse[0, 0] = theta
        for t in range(tiles):
            th = jnp.broadcast_to(coarse[0, 0, t : t + 1, :], (8, 128)) * sub8
            c, s = sincos_turns(th)
            fine[0, t] = c
            fine[1, t] = s
        for r in range(0, tiles * 128, 16):
            ox = lisb[0, r : r + 16, :] - px
            oy = lisb[1, r : r + 16, :] - py
            oz = lisb[2, r : r + 16, :] - pz
            d2 = ox * ox + oy * oy + oz * oz
            face = nx * ox + ny * oy + nz * oz
            wts[r : r + 16, :] = (face * recip(d2)).astype(jnp.bfloat16)
        for q in range(tiles // 2):
            prod[q % 2] = lax.dot_general(sp[b], wts[q * 256 : (q + 1) * 256, :], NT, preferred_element_type=jnp.float32)
            for u in range(2):
                t = 2 * q + u
                bc, bs = fine[0, t], fine[1, t]
                for a in range(half // 8):
                    if a == 0:
                        c, s = bc, bs
                    else:
                        ec = jnp.broadcast_to(coarse[0, a, t : t + 1, :], (8, 128))
                        es = jnp.broadcast_to(coarse[1, a, t : t + 1, :], (8, 128))
                        c = ec * bc - es * bs
                        s = es * bc + ec * bs
                    re = prod[q % 2, a * 8 : a * 8 + 8, u * 128 : u * 128 + 128]
                    im = prod[q % 2, half + a * 8 : half + a * 8 + 8, u * 128 : u * 128 + 128]
                    acc[0, a * 8 : a * 8 + 8, t * 128 : t * 128 + 128] += re * c + im * s
                    acc[1, a * 8 : a * 8 + 8, t * 128 : t * 128 + 128] += im * c - re * s
        return 0

    lax.fori_loop(0, count, block, 0)
    shares = out.shape[0]
    per = tiles // shares
    for g in range(shares):
        for k in range(2):
            for t in range(per):
                col = (g * per + t) * 128
                out[g, k, t * 128 : (t + 1) * 128, :] = jnp.transpose(acc[k, :, col : col + 128])


def panels(live, dens, rec, geo, cell, lis, table, shares):
    slots, bp = cell.shape
    rows = dens.shape[0]
    tiles = lis.shape[1]
    k2 = table.shape[0]
    obs = tiles * 128
    vm = pl.BlockSpec(memory_space=pltpu.VMEM)
    return pl.pallas_call(
        panels_kernel,
        out_shape=jax.ShapeDtypeStruct((shares, 2, obs // shares, k2 // 2), jnp.float32),
        in_specs=[pl.BlockSpec(memory_space=pltpu.SMEM)] + [vm] * 6,
        out_specs=vm,
        scratch_shapes=[
            pltpu.VMEM((rows, 384), jnp.bfloat16),
            pltpu.VMEM((3, obs, 128), jnp.float32),
            pltpu.VMEM((slots, k2, bp), jnp.bfloat16),
            pltpu.VMEM((obs, bp), jnp.bfloat16),
            pltpu.VMEM((2, k2, 256), jnp.float32),
            pltpu.VMEM((2, tiles, 8, 128), jnp.float32),
            pltpu.VMEM((2, k2 // 16, tiles, 128), jnp.float32),
            pltpu.VMEM((2, k2 // 2, obs), jnp.float32),
        ],
        name="panels",
        compiler_params=pltpu.CompilerParams(vmem_limit_bytes=48 * 1024 * 1024),
    )(live, dens, rec, geo, cell, lis, table)


def swap(value, axis, bit):
    size = lax.axis_size(axis)
    return lax.ppermute(value, axis, [(i, i ^ bit) for i in range(size)])


def reduce_spectra(shares):
    size = shares.shape[0]
    here = lax.axis_index("gz")
    bit = 1
    while bit < size:
        pairs = shares.reshape((shares.shape[0] // 2, 2) + shares.shape[1:])
        up = (here // bit) % 2
        mine = lax.dynamic_index_in_dim(pairs, up, 1, keepdims=False)
        theirs = lax.dynamic_index_in_dim(pairs, 1 - up, 1, keepdims=False)
        shares = mine + swap(theirs, "gz", bit)
        bit *= 2
    total = shares[0]
    for axis in ("gx", "gy"):
        bit = 1
        while bit < lax.axis_size(axis):
            total = total + swap(total, axis, bit)
            bit *= 2
    return total


def local(
    state_old,
    state_section,
    panel_record,
    panel_cell,
    panel_angles,
    owned_blocks,
    listener_angles,
    listener_range,
):
    cells_x = state_section.shape[1]
    cells_y = state_section.shape[2]
    cells_z = state_section.shape[3]
    counts = (
        cells_x * lax.axis_size("gx"),
        cells_y * lax.axis_size("gy"),
        cells_z * lax.axis_size("gz"),
    )
    step_size = COURANT / max(counts)
    padded = with_halo(state_section, (("gx", 1), ("gy", 2), ("gz", 3)), 3)
    updated = section_update(padded, state_old, counts, step_size)
    slot_count = panel_cell.shape[0]
    block_rows = panel_cell.shape[1]
    samples = panel_record.shape[1]
    density = updated[0].reshape(cells_x * cells_y, cells_z)
    places = panel_places(
        panel_cell,
        lax.axis_index("gx"),
        lax.axis_index("gy"),
        lax.axis_index("gz"),
        cells_x,
        cells_y,
        cells_z,
        counts,
    )
    normals = jnp.transpose(directions(panel_angles.reshape(2, slot_count, block_rows)), (1, 0, 2))
    geometry = jnp.transpose(
        jnp.concatenate([places, normals * (0.25 / math.pi)], axis=1), (1, 0, 2)
    )
    listeners = 0.5 + listener_range[None, :] * directions(listener_angles)
    listeners = listeners.reshape(3, -1, 128)
    shares = panels(
        owned_blocks,
        density,
        panel_record,
        geometry,
        panel_cell,
        listeners,
        dft_table(samples, FREQS),
        lax.axis_size("gz"),
    )
    spectra_out = reduce_spectra(shares)
    return (updated, spectra_out)


def solution(mesh):
    return jax.shard_map(
        local,
        mesh=mesh,
        in_specs=(
            P(None, "gx", "gy", "gz"),
            P(None, "gx", "gy", "gz"),
            P(("gx", "gy", "gz"), None),
            P(("gx", "gy", "gz"), None),
            P(None, ("gx", "gy", "gz")),
            P(("gx", "gy", "gz")),
            P(),
            P(),
        ),
        out_specs=(P(None, "gx", "gy", "gz"), P(None, "gz", None)),
        check_vma=False,
    )
```

```python
import functools
import math

import jax
import jax.numpy as jnp
import numpy as np
from jax import lax
from jax.experimental import pallas as pl
from jax.experimental.pallas import tpu as pltpu
from jax.sharding import PartitionSpec as P

FREQS = 128
NT = (((1,), (1,)), ((), ()))


GAMMA_GAS = 4.4
PRESSURE_INF = 1.0
WENO_EPS = 1e-06
WAVE_STEP = 0.25
COURANT = 0.08


def pack_kernel(state, turned, zlo, zhi, ylo, yhi, xlo, xhi, *, cx, cy, cz):
    plane = cx * cy
    groups = plane // 128
    for c in range(5):
        for g in range(groups):
            row = c * plane + g * 128
            turned[row : row + cz, :] = jnp.transpose(state[row : row + 128, :])
        for k in range(3):
            ylo[(c * 3 + k) * cx : (c * 3 + k + 1) * cx, :] = state[pl.ds(c * plane + k, cx, stride=cy), :]
            yhi[(c * 3 + k) * cx : (c * 3 + k + 1) * cx, :] = state[pl.ds(c * plane + cy - 3 + k, cx, stride=cy), :]
            zlo[(c * 3 + k) * groups : (c * 3 + k + 1) * groups, :] = turned[pl.ds(c * plane + k, groups, stride=128), :]
            zhi[(c * 3 + k) * groups : (c * 3 + k + 1) * groups, :] = turned[pl.ds(c * plane + cz - 3 + k, groups, stride=128), :]
        xlo[c * 3 * cy : (c + 1) * 3 * cy, :] = state[c * plane : c * plane + 3 * cy, :]
        xhi[c * 3 * cy : (c + 1) * 3 * cy, :] = state[c * plane + (cx - 3) * cy : (c + 1) * plane, :]


def pack(state, cx, cy, cz):
    groups = cx * cy // 128
    rows = [state.shape[0]] + [15 * groups] * 2 + [15 * cx] * 2 + [15 * cy] * 2
    vm = pl.BlockSpec(memory_space=pltpu.VMEM)
    return pl.pallas_call(
        functools.partial(pack_kernel, cx=cx, cy=cy, cz=cz),
        out_shape=[jax.ShapeDtypeStruct((r, 128), jnp.float32) for r in rows],
        in_specs=[vm],
        out_specs=[vm] * 7,
        name="pack",
    )(state)


def weno_shift(d1, d2, d3, d4):
    a0, a1, a2 = d2 - d1, d3 - d2, d4 - d3
    h2, h3 = 0.75 * d2, 0.75 * d3
    eps = 3.0 * WENO_EPS
    e0 = (a0 * a0 + eps) + h2 * (d2 + a0)
    e1 = (a1 * a1 + eps) + h2 * d3
    e2 = (a2 * a2 + eps) + h3 * (d3 - a2)
    t1 = e1 * e1
    u0 = 3.0 * (e0 * e0)
    u2 = 2.0 * (e2 * e2)
    w0, w1, w2 = t1 * u2, u0 * u2, u0 * t1
    below = 0.5 * w0 + (w1 + w2)
    above = w0 * (a1 - a0) + w2 * (a2 - a1)
    return (d2 + (d3 + d3)) - above * (1.0 / below)


def line_kernel_body(cells, flux, speed, wave, emit, *, n, width, axis):
    length = n + 6
    tiles = width // 8
    span = length * width

    def fluxes(p, _):
        for w in range(tiles):
            at = pl.multiple_of(p * width + w * 8, 8)
            rho = cells[pl.ds(at, 8), :]
            m = [cells[pl.ds((1 + k) * span + at, 8), :] for k in range(3)]
            energy = cells[pl.ds(4 * span + at, 8), :]
            inv = 1.0 / rho
            u = m[axis] * inv
            twice = (m[0] * m[0] + m[1] * m[1] + m[2] * m[2]) * inv
            pressure = (GAMMA_GAS - 1.0) * (energy - 0.5 * twice) - GAMMA_GAS * PRESSURE_INF
            sound = jnp.sqrt(GAMMA_GAS * (pressure + PRESSURE_INF) * inv)
            speed[pl.ds(at, 8), :] = jnp.abs(u) + sound
            flux[pl.ds(at, 8), :] = m[axis]
            for k in range(3):
                carried = m[k] * u
                if k == axis:
                    carried = carried + pressure
                flux[pl.ds((1 + k) * span + at, 8), :] = carried
            flux[pl.ds(4 * span + at, 8), :] = (energy + pressure) * u
        return 0

    lax.fori_loop(0, length, fluxes, 0, unroll=2)

    def waves(i, _):
        for w in range(tiles):
            at = pl.multiple_of(i * width + w * 8, 8)
            top = speed[pl.ds(at, 8), :]
            for k in range(1, 6):
                top = jnp.maximum(top, speed[pl.ds(at + k * width, 8), :])
            wave[pl.ds(at, 8), :] = top
        return 0

    lax.fori_loop(0, n + 1, waves, 0)

    def line(index, _):
        c = index // tiles
        w = index % tiles

        def load(ref, p):
            return ref[pl.ds(pl.multiple_of(c * span + p * width + w * 8, 8), 8), :]

        q = [load(cells, p) for p in range(5)]
        f = [load(flux, p) for p in range(5)]
        dq = [q[k + 1] - q[k] for k in range(4)]
        df = [f[k + 1] - f[k] for k in range(4)]
        q_last, f_last, f_mid, f_near = q[4], f[4], f[2], f[3]
        before = None
        for i in range(n + 1):
            q_new, f_new = load(cells, i + 5), load(flux, i + 5)
            dq.append(q_new - q_last)
            df.append(f_new - f_last)
            alpha = wave[pl.ds(pl.multiple_of(i * width + w * 8, 8), 8), :]
            drift = [alpha * v for v in dq]
            up = weno_shift(*[df[k] + drift[k] for k in range(4)])
            down = weno_shift(*[drift[k] - df[k] for k in (4, 3, 2, 1)])
            here = 6.0 * ((f_mid + f_near) - drift[2]) + (up + down)
            if before is not None:
                emit(c, w, i - 1, here - before)
            before = here
            dq, df = dq[1:], df[1:]
            f_mid, f_near = f_near, f_last
            q_last, f_last = q_new, f_new
        return 0

    lax.fori_loop(0, 5 * tiles, line, 0)


def z_kernel(turned, left, right, out, cells, flux, speed, wave, part, *, cx, cy, cz, scale):
    plane = cx * cy
    groups = plane // 128
    width = 2 * groups
    n = cz // 2
    length = n + 6
    for c in range(5):
        base = c * length * width
        for p in range(3):
            cells[pl.ds(base + p * width, groups, stride=2), :] = left[(c * 3 + p) * groups : (c * 3 + p + 1) * groups, :]
            cells[pl.ds(base + p * width + 1, groups, stride=2), :] = turned[pl.ds(c * plane + n - 3 + p, groups, stride=128), :]
            q = n + 3 + p
            cells[pl.ds(base + q * width, groups, stride=2), :] = turned[pl.ds(c * plane + n + p, groups, stride=128), :]
            cells[pl.ds(base + q * width + 1, groups, stride=2), :] = right[(c * 3 + p) * groups : (c * 3 + p + 1) * groups, :]
        for p in range(n):
            cells[base + (p + 3) * width : base + (p + 4) * width, :] = turned[pl.ds(c * plane + p, width, stride=n), :]

    def emit(c, w, i, value):
        part[pl.ds(c * plane + i, width, stride=n), :] = value * scale

    line_kernel_body(cells, flux, speed, wave, emit, n=n, width=width, axis=2)
    for c in range(5):
        for g in range(groups):
            row = c * plane + g * 128
            out[row : row + 128, :] = jnp.transpose(part[row : row + cz, :])


def y_kernel(state, left, right, start, out, cells, flux, speed, wave, *, cx, cy, scale):
    plane = cx * cy
    length = cy + 6
    for c in range(5):
        base = c * length * cx
        cells[base : base + 3 * cx, :] = left[c * 3 * cx : (c + 1) * 3 * cx, :]
        cells[base + (cy + 3) * cx : base + length * cx, :] = right[c * 3 * cx : (c + 1) * 3 * cx, :]
        for p in range(cy):
            for x in range(0, cx, 8):
                cells[base + (p + 3) * cx + x : base + (p + 3) * cx + x + 8, :] = state[pl.ds(c * plane + x * cy + p, 8, stride=cy), :]

    def emit(c, w, i, value):
        rows = pl.ds(c * plane + w * 8 * cy + i, 8, stride=cy)
        out[rows, :] = start[rows, :] + value * scale

    line_kernel_body(cells, flux, speed, wave, emit, n=cy, width=cx, axis=1)


def x_kernel(state, left, right, start, old, out, cells, flux, speed, wave, *, cx, cy, scale):
    plane = cx * cy
    length = cx + 6
    for c in range(5):
        base = c * length * cy
        cells[base : base + 3 * cy, :] = left[c * 3 * cy : (c + 1) * 3 * cy, :]
        cells[base + 3 * cy : base + (cx + 3) * cy, :] = state[c * plane : (c + 1) * plane, :]
        cells[base + (cx + 3) * cy : base + length * cy, :] = right[c * 3 * cy : (c + 1) * 3 * cy, :]

    def emit(c, w, i, value):
        rows = pl.ds(pl.multiple_of(c * plane + i * cy + w * 8, 8), 8)
        change = start[rows, :] + value * scale
        out[rows, :] = (0.75 * old[rows, :] + 0.25 * state[rows, :]) - change

    line_kernel_body(cells, flux, speed, wave, emit, n=cx, width=cy, axis=0)


def line_call(kernel, operands, n, width, name, more=()):
    length = n + 6
    vm = pl.BlockSpec(memory_space=pltpu.VMEM)
    return pl.pallas_call(
        kernel,
        out_shape=jax.ShapeDtypeStruct(operands[0].shape, jnp.float32),
        in_specs=[vm] * len(operands),
        out_specs=vm,
        scratch_shapes=[
            pltpu.VMEM((5 * length * width, 128), jnp.float32),
            pltpu.VMEM((5 * length * width, 128), jnp.float32),
            pltpu.VMEM((length * width, 128), jnp.float32),
            pltpu.VMEM((length * width, 128), jnp.float32),
        ]
        + list(more),
        name=name,
    )(*operands)


def neighbours(first, last, axis):
    size = lax.axis_size(axis)
    up = [(i, (i + 1) % size) for i in range(size)]
    down = [(j, i) for i, j in up]
    return lax.ppermute(last, axis, up), lax.ppermute(first, axis, down)


def flow(state_old, state_section, counts, step_size):
    shape = state_section.shape
    cx, cy, cz = shape[1:]
    state = state_section.reshape(-1, cz)
    turned, zlo, zhi, ylo, yhi, xlo, xhi = pack(state, cx, cy, cz)
    zl, zr = neighbours(zlo, zhi, "gz")
    yl, yr = neighbours(ylo, yhi, "gy")
    xl, xr = neighbours(xlo, xhi, "gx")
    scales = [0.25 * step_size * n / 12.0 for n in counts]
    plane = cx * cy
    part = line_call(
        functools.partial(z_kernel, cx=cx, cy=cy, cz=cz, scale=scales[2]),
        (turned, zl, zr), cz // 2, plane // 64, "along_z",
        (pltpu.VMEM((5 * plane, 128), jnp.float32),),
    )
    part = line_call(functools.partial(y_kernel, cx=cx, cy=cy, scale=scales[1]), (state, yl, yr, part), cy, cx, "along_y")
    updated = line_call(
        functools.partial(x_kernel, cx=cx, cy=cy, scale=scales[0]),
        (state, xl, xr, part, state_old.reshape(-1, cz)), cx, cy, "along_x",
    )
    return updated.reshape(shape)


def directions(angles):
    polar_angle = 0.5 * angles[0]
    azimuth = angles[1]
    return jnp.stack(
        [
            jnp.cos(polar_angle) * jnp.cos(azimuth),
            jnp.cos(polar_angle) * jnp.sin(azimuth),
            jnp.sin(polar_angle),
        ]
    )


def panel_places(cell_rows, block_x, block_y, block_z, cells_x, cells_y, cells_z, counts):
    along_x = cell_rows // (cells_y * cells_z)
    along_y = cell_rows // cells_z % cells_y
    along_z = cell_rows % cells_z
    place_x = ((block_x * cells_x + along_x).astype(jnp.float32) + 0.5) / counts[0]
    place_y = ((block_y * cells_y + along_y).astype(jnp.float32) + 0.5) / counts[1]
    place_z = ((block_z * cells_z + along_z).astype(jnp.float32) + 0.5) / counts[2]
    return jnp.stack([place_x, place_y, place_z], axis=1)


def dft_table(sample_count, freq_count):
    times = np.arange(sample_count, dtype=np.int64)[None, :]
    orders = np.arange(1, freq_count + 1, dtype=np.int64)[:, None]
    phases = (np.float32(2.0 * math.pi / sample_count) * (times * orders % sample_count).astype(np.float32)).astype(np.float64)
    scaling = 1.0 / math.sqrt(sample_count)
    both = np.concatenate([np.cos(phases), -np.sin(phases)], axis=0).astype(np.float32) * np.float32(scaling)
    return jnp.asarray(both, jnp.bfloat16)


def sincos_turns(turns):
    r = turns - jnp.round(turns)
    x = r * math.pi
    x2 = x * x
    s = 1.0 / 6227020800.0
    s = s * x2 - 1.0 / 39916800.0
    s = s * x2 + 1.0 / 362880.0
    s = s * x2 - 1.0 / 5040.0
    s = s * x2 + 1.0 / 120.0
    s = s * x2 - 1.0 / 6.0
    s = (s * x2) * x + x
    c = 1.0 / 479001600.0
    c = c * x2 - 1.0 / 3628800.0
    c = c * x2 + 1.0 / 40320.0
    c = c * x2 - 1.0 / 720.0
    c = c * x2 + 1.0 / 24.0
    c = c * x2 - 0.5
    c = c * x2 + 1.0
    s2 = s + s
    return 1.0 - s2 * s, s2 * c


def panels_kernel(live, dens, rec, geo, cell, lis, table, out, dens3, lisb, sp, wts, prod, fine, coarse, acc):
    slots, bp = cell.shape
    rows = dens.shape[0]
    tiles = lis.shape[1]
    half = table.shape[0] // 2
    count = live[0]

    d = dens[...]
    hi = d.astype(jnp.bfloat16)
    left = d - hi.astype(jnp.float32)
    mid = left.astype(jnp.bfloat16)
    lo = (left - mid.astype(jnp.float32)).astype(jnp.bfloat16)
    dens3[:, 0:128] = hi
    dens3[:, 128:256] = mid
    dens3[:, 256:384] = lo
    for k in range(3):
        for t in range(tiles):
            row = lis[k, t : t + 1, :]
            lisb[k, t * 128 : (t + 1) * 128, :] = jnp.transpose(jnp.broadcast_to(row, (128, 128)))
    acc[...] = jnp.zeros(acc.shape, jnp.float32)
    lane = lax.broadcasted_iota(jnp.int32, (128, 128), 1).astype(jnp.float32)

    def spectrum(b, _):
        cells = cell[pl.ds(b, 1), :]
        high = (cells >> 7).astype(jnp.float32)
        low = (cells & 127).astype(jnp.float32)
        high_col = jnp.transpose(jnp.broadcast_to(high, (128, 128)))
        low_col = jnp.transpose(jnp.broadcast_to(low, (128, 128)))
        g = jnp.zeros((128, 384), jnp.float32)
        for j in range(rows // 128):
            onehot = jnp.where(high_col == lane + float(128 * j), 1.0, 0.0).astype(jnp.bfloat16)
            g = g + jnp.dot(onehot, dens3[j * 128 : (j + 1) * 128, :], preferred_element_type=jnp.float32)
        gs = (g[:, 0:128] + g[:, 128:256]) + g[:, 256:384]
        sampled = jnp.sum(jnp.where(low_col == lane, gs, 0.0), axis=1, keepdims=True)
        src = (rec[pl.ds(pl.multiple_of(b * bp, bp), bp), :].astype(jnp.float32) * sampled).astype(jnp.bfloat16)
        sp[b] = lax.dot_general(table[...], src, NT, preferred_element_type=jnp.float32).astype(jnp.bfloat16)
        return 0

    lax.fori_loop(0, count, spectrum, 0)

    sub8 = lax.broadcasted_iota(jnp.int32, (8, 128), 0).astype(jnp.float32) + 1.0
    turn = WAVE_STEP / (2.0 * math.pi)

    def block(b, _):
        px, py, pz, nx, ny, nz = [geo[k, pl.ds(b, 1), :] for k in range(6)]
        cx, cy, cz = [jnp.sum(v, axis=1, keepdims=True) * (1.0 / bp) for v in (px, py, pz)]
        sx, sy, sz = lis[0] - cx, lis[1] - cy, lis[2] - cz
        theta = jnp.sqrt(sx * sx + sy * sy + sz * sz) * turn
        c1, s1 = sincos_turns(8.0 * theta)
        cs = [None, (c1, s1)]
        for a in range(2, half // 8):
            (ca, sa), (cb, sb) = cs[a // 2], cs[a - a // 2]
            cs.append((ca * cb - sa * sb, sa * cb + ca * sb))
        for a in range(1, half // 8):
            coarse[0, a] = cs[a][0]
            coarse[1, a] = cs[a][1]
        coarse[0, 0] = theta
        for t in range(tiles):
            th = jnp.broadcast_to(coarse[0, 0, t : t + 1, :], (8, 128)) * sub8
            c, s = sincos_turns(th)
            fine[0, t] = c
            fine[1, t] = s
        for r in range(0, tiles * 128, 16):
            ox = lisb[0, r : r + 16, :] - px
            oy = lisb[1, r : r + 16, :] - py
            oz = lisb[2, r : r + 16, :] - pz
            d2 = ox * ox + oy * oy + oz * oz
            face = nx * ox + ny * oy + nz * oz
            wts[r : r + 16, :] = (face * (1.0 / d2)).astype(jnp.bfloat16)
        for q in range(tiles // 2):
            prod[q % 2] = lax.dot_general(sp[b], wts[q * 256 : (q + 1) * 256, :], NT, preferred_element_type=jnp.float32)
            for u in range(2):
                t = 2 * q + u
                bc, bs = fine[0, t], fine[1, t]
                for a in range(half // 8):
                    if a == 0:
                        c, s = bc, bs
                    else:
                        ec = jnp.broadcast_to(coarse[0, a, t : t + 1, :], (8, 128))
                        es = jnp.broadcast_to(coarse[1, a, t : t + 1, :], (8, 128))
                        c = ec * bc - es * bs
                        s = es * bc + ec * bs
                    re = prod[q % 2, a * 8 : a * 8 + 8, u * 128 : u * 128 + 128]
                    im = prod[q % 2, half + a * 8 : half + a * 8 + 8, u * 128 : u * 128 + 128]
                    acc[0, a * 8 : a * 8 + 8, t * 128 : t * 128 + 128] += re * c + im * s
                    acc[1, a * 8 : a * 8 + 8, t * 128 : t * 128 + 128] += im * c - re * s
        return 0

    lax.fori_loop(0, count, block, 0)
    shares = out.shape[0]
    per = tiles // shares
    for g in range(shares):
        for k in range(2):
            for t in range(per):
                col = (g * per + t) * 128
                out[g, k, t * 128 : (t + 1) * 128, :] = jnp.transpose(acc[k, :, col : col + 128])


def panels(live, dens, rec, geo, cell, lis, table, shares):
    slots, bp = cell.shape
    rows = dens.shape[0]
    tiles = lis.shape[1]
    k2 = table.shape[0]
    obs = tiles * 128
    vm = pl.BlockSpec(memory_space=pltpu.VMEM)
    return pl.pallas_call(
        panels_kernel,
        out_shape=jax.ShapeDtypeStruct((shares, 2, obs // shares, k2 // 2), jnp.float32),
        in_specs=[pl.BlockSpec(memory_space=pltpu.SMEM)] + [vm] * 6,
        out_specs=vm,
        scratch_shapes=[
            pltpu.VMEM((rows, 384), jnp.bfloat16),
            pltpu.VMEM((3, obs, 128), jnp.float32),
            pltpu.VMEM((slots, k2, bp), jnp.bfloat16),
            pltpu.VMEM((obs, bp), jnp.bfloat16),
            pltpu.VMEM((2, k2, 256), jnp.float32),
            pltpu.VMEM((2, tiles, 8, 128), jnp.float32),
            pltpu.VMEM((2, k2 // 16, tiles, 128), jnp.float32),
            pltpu.VMEM((2, k2 // 2, obs), jnp.float32),
        ],
        name="panels",
        compiler_params=pltpu.CompilerParams(vmem_limit_bytes=48 * 1024 * 1024),
    )(live, dens, rec, geo, cell, lis, table)


def swap(value, axis, bit):
    size = lax.axis_size(axis)
    return lax.ppermute(value, axis, [(i, i ^ bit) for i in range(size)])


def reduce_spectra(shares):
    size = shares.shape[0]
    here = lax.axis_index("gz")
    bit = 1
    while bit < size:
        pairs = shares.reshape((shares.shape[0] // 2, 2) + shares.shape[1:])
        up = (here // bit) % 2
        mine = lax.dynamic_index_in_dim(pairs, up, 1, keepdims=False)
        theirs = lax.dynamic_index_in_dim(pairs, 1 - up, 1, keepdims=False)
        shares = mine + swap(theirs, "gz", bit)
        bit *= 2
    total = shares[0]
    for axis in ("gx", "gy"):
        bit = 1
        while bit < lax.axis_size(axis):
            total = total + swap(total, axis, bit)
            bit *= 2
    return total


def local(
    state_old,
    state_section,
    panel_record,
    panel_cell,
    panel_angles,
    owned_blocks,
    listener_angles,
    listener_range,
):
    cells_x = state_section.shape[1]
    cells_y = state_section.shape[2]
    cells_z = state_section.shape[3]
    counts = (
        cells_x * lax.axis_size("gx"),
        cells_y * lax.axis_size("gy"),
        cells_z * lax.axis_size("gz"),
    )
    step_size = COURANT / max(counts)
    updated = flow(state_old, state_section, counts, step_size)
    slot_count = panel_cell.shape[0]
    block_rows = panel_cell.shape[1]
    samples = panel_record.shape[1]
    density = updated[0].reshape(cells_x * cells_y, cells_z)
    places = panel_places(
        panel_cell,
        lax.axis_index("gx"),
        lax.axis_index("gy"),
        lax.axis_index("gz"),
        cells_x,
        cells_y,
        cells_z,
        counts,
    )
    normals = jnp.transpose(directions(panel_angles.reshape(2, slot_count, block_rows)), (1, 0, 2))
    geometry = jnp.transpose(
        jnp.concatenate([places, normals * (0.25 / math.pi)], axis=1), (1, 0, 2)
    )
    listeners = 0.5 + listener_range[None, :] * directions(listener_angles)
    listeners = listeners.reshape(3, -1, 128)
    shares = panels(
        owned_blocks,
        density,
        panel_record,
        geometry,
        panel_cell,
        listeners,
        dft_table(samples, FREQS),
        lax.axis_size("gz"),
    )
    spectra_out = reduce_spectra(shares)
    return (updated, spectra_out)


def solution(mesh):
    return jax.shard_map(
        local,
        mesh=mesh,
        in_specs=(
            P(None, "gx", "gy", "gz"),
            P(None, "gx", "gy", "gz"),
            P(("gx", "gy", "gz"), None),
            P(("gx", "gy", "gz"), None),
            P(None, ("gx", "gy", "gz")),
            P(("gx", "gy", "gz")),
            P(),
            P(),
        ),
        out_specs=(P(None, "gx", "gy", "gz"), P(None, "gz", None)),
        check_vma=False,
    )
```

```python
import functools
import math

import jax
import jax.numpy as jnp
import numpy as np
from jax import lax
from jax.experimental import pallas as pl
from jax.experimental.pallas import tpu as pltpu
from jax.sharding import PartitionSpec as P

FREQS = 128
BATCH = 4
CHUNKS = 4
NT = (((1,), (1,)), ((), ()))


GAMMA_GAS = 4.4
PRESSURE_INF = 1.0
WENO_EPS = 1e-06
WAVE_STEP = 0.25
COURANT = 0.08


def pack_kernel(state, turned, zlo, zhi, ylo, yhi, xlo, xhi, *, cx, cy, cz):
    plane = cx * cy
    groups = plane // 128
    for c in range(5):
        for g in range(groups):
            row = c * plane + g * 128
            turned[row : row + cz, :] = jnp.transpose(state[row : row + 128, :])
        for k in range(3):
            ylo[(c * 3 + k) * cx : (c * 3 + k + 1) * cx, :] = state[pl.ds(c * plane + k, cx, stride=cy), :]
            yhi[(c * 3 + k) * cx : (c * 3 + k + 1) * cx, :] = state[pl.ds(c * plane + cy - 3 + k, cx, stride=cy), :]
            zlo[(c * 3 + k) * groups : (c * 3 + k + 1) * groups, :] = turned[pl.ds(c * plane + k, groups, stride=128), :]
            zhi[(c * 3 + k) * groups : (c * 3 + k + 1) * groups, :] = turned[pl.ds(c * plane + cz - 3 + k, groups, stride=128), :]
        xlo[c * 3 * cy : (c + 1) * 3 * cy, :] = state[c * plane : c * plane + 3 * cy, :]
        xhi[c * 3 * cy : (c + 1) * 3 * cy, :] = state[c * plane + (cx - 3) * cy : (c + 1) * plane, :]


def pack(state, cx, cy, cz):
    groups = cx * cy // 128
    rows = [state.shape[0]] + [15 * groups] * 2 + [15 * cx] * 2 + [15 * cy] * 2
    vm = pl.BlockSpec(memory_space=pltpu.VMEM)
    return pl.pallas_call(
        functools.partial(pack_kernel, cx=cx, cy=cy, cz=cz),
        out_shape=[jax.ShapeDtypeStruct((r, 128), jnp.float32) for r in rows],
        in_specs=[vm],
        out_specs=[vm] * 7,
        name="pack",
        compiler_params=pltpu.CompilerParams(vmem_limit_bytes=10 * 1024 * 1024),
    )(state)


def weno_shift(d1, d2, d3, d4):
    a0, a1, a2 = d2 - d1, d3 - d2, d4 - d3
    h2, h3 = 0.75 * d2, 0.75 * d3
    eps = 3.0 * WENO_EPS
    e0 = (a0 * a0 + eps) + h2 * (d2 + a0)
    e1 = (a1 * a1 + eps) + h2 * d3
    e2 = (a2 * a2 + eps) + h3 * (d3 - a2)
    t1 = e1 * e1
    u0 = 3.0 * (e0 * e0)
    u2 = 2.0 * (e2 * e2)
    w0, w1, w2 = t1 * u2, u0 * u2, u0 * t1
    below = 0.5 * w0 + (w1 + w2)
    above = w0 * (a1 - a0) + w2 * (a2 - a1)
    return (d2 + (d3 + d3)) - above * (1.0 / below)


def line_kernel_body(cells, flux, speed, wave, emit, *, n, width, axis):
    length = n + 6
    tiles = width // 8
    span = length * width

    def fluxes(p, _):
        for w in range(tiles):
            at = pl.multiple_of(p * width + w * 8, 8)
            rho = cells[pl.ds(at, 8), :]
            m = [cells[pl.ds((1 + k) * span + at, 8), :] for k in range(3)]
            energy = cells[pl.ds(4 * span + at, 8), :]
            inv = 1.0 / rho
            u = m[axis] * inv
            twice = (m[0] * m[0] + m[1] * m[1] + m[2] * m[2]) * inv
            pressure = (GAMMA_GAS - 1.0) * (energy - 0.5 * twice) - GAMMA_GAS * PRESSURE_INF
            sound = jnp.sqrt(GAMMA_GAS * (pressure + PRESSURE_INF) * inv)
            speed[pl.ds(at, 8), :] = jnp.abs(u) + sound
            flux[pl.ds(at, 8), :] = m[axis]
            for k in range(3):
                carried = m[k] * u
                if k == axis:
                    carried = carried + pressure
                flux[pl.ds((1 + k) * span + at, 8), :] = carried
            flux[pl.ds(4 * span + at, 8), :] = (energy + pressure) * u
        return 0

    lax.fori_loop(0, length, fluxes, 0, unroll=2)

    def waves(i, _):
        for w in range(tiles):
            at = pl.multiple_of(i * width + w * 8, 8)
            top = speed[pl.ds(at, 8), :]
            for k in range(1, 6):
                top = jnp.maximum(top, speed[pl.ds(at + k * width, 8), :])
            wave[pl.ds(at, 8), :] = top
        return 0

    lax.fori_loop(0, n + 1, waves, 0)

    def line(index, _):
        c = index // tiles
        w = index % tiles

        def load(ref, p):
            return ref[pl.ds(pl.multiple_of(c * span + p * width + w * 8, 8), 8), :]

        q = [load(cells, p) for p in range(5)]
        f = [load(flux, p) for p in range(5)]
        dq = [q[k + 1] - q[k] for k in range(4)]
        df = [f[k + 1] - f[k] for k in range(4)]
        q_last, f_last, f_mid, f_near = q[4], f[4], f[2], f[3]
        before = None
        for i in range(n + 1):
            q_new, f_new = load(cells, i + 5), load(flux, i + 5)
            dq.append(q_new - q_last)
            df.append(f_new - f_last)
            alpha = wave[pl.ds(pl.multiple_of(i * width + w * 8, 8), 8), :]
            drift = [alpha * v for v in dq]
            up = weno_shift(*[df[k] + drift[k] for k in range(4)])
            down = weno_shift(*[drift[k] - df[k] for k in (4, 3, 2, 1)])
            here = 6.0 * ((f_mid + f_near) - drift[2]) + (up + down)
            if before is not None:
                emit(c, w, i - 1, here - before)
            before = here
            dq, df = dq[1:], df[1:]
            f_mid, f_near = f_near, f_last
            q_last, f_last = q_new, f_new
        return 0

    lax.fori_loop(0, 5 * tiles, line, 0)


def z_kernel(turned, left, right, out, cells, flux, speed, wave, part, *, cx, cy, cz, scale):
    plane = cx * cy
    groups = plane // 128
    width = 2 * groups
    n = cz // 2
    length = n + 6
    for c in range(5):
        base = c * length * width
        for p in range(3):
            cells[pl.ds(base + p * width, groups, stride=2), :] = left[(c * 3 + p) * groups : (c * 3 + p + 1) * groups, :]
            cells[pl.ds(base + p * width + 1, groups, stride=2), :] = turned[pl.ds(c * plane + n - 3 + p, groups, stride=128), :]
            q = n + 3 + p
            cells[pl.ds(base + q * width, groups, stride=2), :] = turned[pl.ds(c * plane + n + p, groups, stride=128), :]
            cells[pl.ds(base + q * width + 1, groups, stride=2), :] = right[(c * 3 + p) * groups : (c * 3 + p + 1) * groups, :]
        for p in range(n):
            cells[base + (p + 3) * width : base + (p + 4) * width, :] = turned[pl.ds(c * plane + p, width, stride=n), :]

    def emit(c, w, i, value):
        part[pl.ds(c * plane + i, width, stride=n), :] = value * scale

    line_kernel_body(cells, flux, speed, wave, emit, n=n, width=width, axis=2)
    for c in range(5):
        for g in range(groups):
            row = c * plane + g * 128
            out[row : row + 128, :] = jnp.transpose(part[row : row + cz, :])


def y_kernel(state, left, right, start, out, cells, flux, speed, wave, *, cx, cy, scale):
    plane = cx * cy
    length = cy + 6
    for c in range(5):
        base = c * length * cx
        cells[base : base + 3 * cx, :] = left[c * 3 * cx : (c + 1) * 3 * cx, :]
        cells[base + (cy + 3) * cx : base + length * cx, :] = right[c * 3 * cx : (c + 1) * 3 * cx, :]
        for p in range(cy):
            for x in range(0, cx, 8):
                cells[base + (p + 3) * cx + x : base + (p + 3) * cx + x + 8, :] = state[pl.ds(c * plane + x * cy + p, 8, stride=cy), :]

    def emit(c, w, i, value):
        rows = pl.ds(c * plane + w * 8 * cy + i, 8, stride=cy)
        out[rows, :] = start[rows, :] + value * scale

    line_kernel_body(cells, flux, speed, wave, emit, n=cy, width=cx, axis=1)


def x_kernel(state, left, right, start, old, out, cells, flux, speed, wave, *, cx, cy, scale):
    plane = cx * cy
    length = cx + 6
    for c in range(5):
        base = c * length * cy
        cells[base : base + 3 * cy, :] = left[c * 3 * cy : (c + 1) * 3 * cy, :]
        cells[base + 3 * cy : base + (cx + 3) * cy, :] = state[c * plane : (c + 1) * plane, :]
        cells[base + (cx + 3) * cy : base + length * cy, :] = right[c * 3 * cy : (c + 1) * 3 * cy, :]

    def emit(c, w, i, value):
        rows = pl.ds(pl.multiple_of(c * plane + i * cy + w * 8, 8), 8)
        change = start[rows, :] + value * scale
        out[rows, :] = (0.75 * old[rows, :] + 0.25 * state[rows, :]) - change

    line_kernel_body(cells, flux, speed, wave, emit, n=cx, width=cy, axis=0)


def line_call(kernel, operands, n, width, name, more=()):
    length = n + 6
    vm = pl.BlockSpec(memory_space=pltpu.VMEM)
    return pl.pallas_call(
        kernel,
        out_shape=jax.ShapeDtypeStruct(operands[0].shape, jnp.float32),
        in_specs=[vm] * len(operands),
        out_specs=vm,
        scratch_shapes=[
            pltpu.VMEM((5 * length * width, 128), jnp.float32),
            pltpu.VMEM((5 * length * width, 128), jnp.float32),
            pltpu.VMEM((length * width, 128), jnp.float32),
            pltpu.VMEM((length * width, 128), jnp.float32),
        ]
        + list(more),
        name=name,
        compiler_params=pltpu.CompilerParams(vmem_limit_bytes=14 * 1024 * 1024),
    )(*operands)


def neighbours(first, last, axis):
    size = lax.axis_size(axis)
    up = [(i, (i + 1) % size) for i in range(size)]
    down = [(j, i) for i, j in up]
    return lax.ppermute(last, axis, up), lax.ppermute(first, axis, down)


def flow(state_old, state_section, counts, step_size):
    shape = state_section.shape
    cx, cy, cz = shape[1:]
    state = state_section.reshape(-1, cz)
    turned, zlo, zhi, ylo, yhi, xlo, xhi = pack(state, cx, cy, cz)
    zl, zr = neighbours(zlo, zhi, "gz")
    yl, yr = neighbours(ylo, yhi, "gy")
    xl, xr = neighbours(xlo, xhi, "gx")
    scales = [0.25 * step_size * n / 12.0 for n in counts]
    plane = cx * cy
    part = line_call(
        functools.partial(z_kernel, cx=cx, cy=cy, cz=cz, scale=scales[2]),
        (turned, zl, zr), cz // 2, plane // 64, "along_z",
        (pltpu.VMEM((5 * plane, 128), jnp.float32),),
    )
    part = line_call(functools.partial(y_kernel, cx=cx, cy=cy, scale=scales[1]), (state, yl, yr, part), cy, cx, "along_y")
    updated = line_call(
        functools.partial(x_kernel, cx=cx, cy=cy, scale=scales[0]),
        (state, xl, xr, part, state_old.reshape(-1, cz)), cx, cy, "along_x",
    )
    return updated.reshape(shape)


def directions(angles):
    polar_angle = 0.5 * angles[0]
    azimuth = angles[1]
    return jnp.stack(
        [
            jnp.cos(polar_angle) * jnp.cos(azimuth),
            jnp.cos(polar_angle) * jnp.sin(azimuth),
            jnp.sin(polar_angle),
        ]
    )


def panel_places(cell_rows, block_x, block_y, block_z, cells_x, cells_y, cells_z, counts):
    along_x = cell_rows // (cells_y * cells_z)
    along_y = cell_rows // cells_z % cells_y
    along_z = cell_rows % cells_z
    place_x = ((block_x * cells_x + along_x).astype(jnp.float32) + 0.5) / counts[0]
    place_y = ((block_y * cells_y + along_y).astype(jnp.float32) + 0.5) / counts[1]
    place_z = ((block_z * cells_z + along_z).astype(jnp.float32) + 0.5) / counts[2]
    return jnp.stack([place_x, place_y, place_z], axis=1)


def dft_table(sample_count, freq_count):
    times = np.arange(sample_count, dtype=np.int64)[None, :]
    orders = np.arange(1, freq_count + 1, dtype=np.int64)[:, None]
    phases = (np.float32(2.0 * math.pi / sample_count) * (times * orders % sample_count).astype(np.float32)).astype(np.float64)
    scaling = 1.0 / math.sqrt(sample_count)
    both = np.concatenate([np.cos(phases), -np.sin(phases)], axis=0).astype(np.float32) * np.float32(scaling)
    return jnp.asarray(both, jnp.bfloat16)


def sincos_turns(turns):
    r = turns - jnp.round(turns)
    x = r * math.pi
    x2 = x * x
    s = 1.0 / 6227020800.0
    s = s * x2 - 1.0 / 39916800.0
    s = s * x2 + 1.0 / 362880.0
    s = s * x2 - 1.0 / 5040.0
    s = s * x2 + 1.0 / 120.0
    s = s * x2 - 1.0 / 6.0
    s = (s * x2) * x + x
    c = 1.0 / 479001600.0
    c = c * x2 - 1.0 / 3628800.0
    c = c * x2 + 1.0 / 40320.0
    c = c * x2 - 1.0 / 720.0
    c = c * x2 + 1.0 / 24.0
    c = c * x2 - 0.5
    c = c * x2 + 1.0
    s2 = s + s
    return 1.0 - s2 * s, s2 * c


def weights_kernel(live, geo, lis, *refs):
    outs, lisb = refs[:-1], refs[-1]
    tiles = lis.shape[1]
    span = tiles * 128 // len(outs)
    for k in range(3):
        for t in range(tiles):
            row = lis[k, t : t + 1, :]
            lisb[k, t * 128 : (t + 1) * 128, :] = jnp.transpose(jnp.broadcast_to(row, (128, 128)))

    def block(b, _):
        px, py, pz, nx, ny, nz = [geo[k, pl.ds(b, 1), :] for k in range(6)]
        for q, out in enumerate(outs):
            for r in range(0, span, 16):
                at = q * span + r
                ox = lisb[0, at : at + 16, :] - px
                oy = lisb[1, at : at + 16, :] - py
                oz = lisb[2, at : at + 16, :] - pz
                d2 = ox * ox + oy * oy + oz * oz
                facing = nx * ox + ny * oy + nz * oz
                out[pl.ds(pl.multiple_of(b * span + r, 16), 16), :] = (facing * (1.0 / d2)).astype(jnp.bfloat16)
        return 0

    lax.fori_loop(0, (live[0] + BATCH - 1) // BATCH * BATCH, block, 0)


def weights(live, geo, lis, chunks):
    slots, bp = geo.shape[1:]
    obs = lis.shape[1] * 128
    vm = pl.BlockSpec(memory_space=pltpu.VMEM)
    return pl.pallas_call(
        weights_kernel,
        out_shape=[jax.ShapeDtypeStruct((slots * obs // chunks, bp), jnp.bfloat16)] * chunks,
        in_specs=[pl.BlockSpec(memory_space=pltpu.SMEM), vm, vm],
        out_specs=[vm] * chunks,
        scratch_shapes=[pltpu.VMEM((3, obs, 128), jnp.float32)],
        name="weights",
        compiler_params=pltpu.CompilerParams(vmem_limit_bytes=14 * 1024 * 1024),
    )(live, geo, lis)


def spectra_kernel(live, dens, rec, cell, table, sp, dens3, held, onehot, src, sems):
    slots, bp = cell.shape
    rows = dens.shape[0] // 2
    groups = slots // BATCH
    total = (live[0] + BATCH - 1) // BATCH
    span = BATCH * bp

    def fetch(g):
        at = pl.ds(pl.multiple_of(g * span, span), span)
        return pltpu.make_async_copy(rec.at[at, :], held.at[at, :], sems.at[g])

    for g in range(groups):
        @pl.when(g < total)
        def _():
            fetch(g).start()

    for h in range(2):
        d = dens[pl.ds(h, rows, stride=2), :]
        hi = d.astype(jnp.bfloat16)
        left = d - hi.astype(jnp.float32)
        mid = left.astype(jnp.bfloat16)
        lo = (left - mid.astype(jnp.float32)).astype(jnp.bfloat16)
        for k, part in enumerate((hi, mid, lo)):
            dens3[k, :, h * 128 : (h + 1) * 128] = part
    lane = lax.broadcasted_iota(jnp.int32, (bp, 128), 1).astype(jnp.float32)

    def group(g, _):
        lows = []
        for j in range(BATCH):
            cells = cell[pl.ds(g * BATCH + j, 1), :].astype(jnp.float32)
            col = jnp.transpose(jnp.broadcast_to(cells, (128, 128)))
            high = jnp.floor(col * (1.0 / 256.0))
            low = col - 256.0 * high
            lows.append(low)
            for h in range(rows // 128):
                hit = jnp.where(high == lane + float(128 * h), 1.0, 0.0).astype(jnp.bfloat16)
                onehot[j * bp : (j + 1) * bp, h * 128 : (h + 1) * 128] = hit
        hot = onehot[...]
        picked = jnp.dot(hot, dens3[0], preferred_element_type=jnp.float32)
        picked = picked + jnp.dot(hot, dens3[1], preferred_element_type=jnp.float32)
        picked = picked + jnp.dot(hot, dens3[2], preferred_element_type=jnp.float32)
        fetch(g).wait()
        for j in range(BATCH):
            own = picked[j * bp : (j + 1) * bp, :]
            found = jnp.where(lows[j] == lane, own[:, 0:128], 0.0) + jnp.where(lows[j] == lane + 128.0, own[:, 128:256], 0.0)
            sampled = jnp.sum(found, axis=1, keepdims=True)
            record = held[pl.ds(pl.multiple_of(g * span + j * bp, bp), bp), :].astype(jnp.float32)
            src[j * bp : (j + 1) * bp, :] = (record * sampled).astype(jnp.bfloat16)
        for j in range(0, BATCH, 2):
            both = lax.dot_general(table[...], src[j * bp : (j + 2) * bp, :], NT, preferred_element_type=jnp.float32)
            both = both.astype(jnp.bfloat16)
            sp[g * BATCH + j] = both[:, 0:bp]
            sp[g * BATCH + j + 1] = both[:, bp : 2 * bp]
        return 0

    lax.fori_loop(0, total, group, 0)


def spectra(live, dens, rec, cell, table, rows):
    slots, bp = cell.shape
    samples = rec.shape[1]
    k2 = table.shape[0]
    vm = pl.BlockSpec(memory_space=pltpu.VMEM)
    return pl.pallas_call(
        spectra_kernel,
        grid=(1,),
        out_shape=jax.ShapeDtypeStruct((slots, k2, bp), jnp.bfloat16),
        in_specs=[
            pl.BlockSpec(memory_space=pltpu.SMEM),
            pl.BlockSpec((rows, 128), lambda i: (0, 0)),
            pl.BlockSpec(memory_space=pl.ANY),
            vm,
            vm,
        ],
        out_specs=vm,
        scratch_shapes=[
            pltpu.VMEM((3, rows // 2, 256), jnp.bfloat16),
            pltpu.VMEM(rec.shape, jnp.bfloat16),
            pltpu.VMEM((BATCH * bp, rows // 2), jnp.bfloat16),
            pltpu.VMEM((BATCH * bp, samples), jnp.bfloat16),
            pltpu.SemaphoreType.DMA((slots // BATCH,)),
        ],
        name="spectra",
        compiler_params=pltpu.CompilerParams(vmem_limit_bytes=12 * 1024 * 1024),
    )(live, dens, rec, cell, table)


def observe_kernel(live, centre, sp, wts, lis, out, prod, acc):
    slots, k2, bp = sp.shape
    tiles = lis.shape[1]
    half = k2 // 2
    span = tiles * 128
    total = (live[0] + BATCH - 1) // BATCH
    acc[...] = jnp.zeros(acc.shape, jnp.float32)
    orders = lax.broadcasted_iota(jnp.int32, (8, 128), 0).astype(jnp.float32) + 1.0
    orders = orders * (WAVE_STEP / (2.0 * math.pi))

    def group(g, _):
        for pair in range(0, BATCH, 2):
            waves = []
            for j in range(2):
                b = g * BATCH + pair + j
                held = wts[pl.ds(pl.multiple_of(b * span, span), span), :]
                prod[pair + j] = lax.dot_general(sp[b], held, NT, preferred_element_type=jnp.float32)
            for t in range(tiles):
                state = []
                for j in range(2):
                    b = g * BATCH + pair + j
                    away = [jnp.broadcast_to(lis[k, t : t + 1, :], (8, 128)) - centre[k, b] for k in range(3)]
                    reach = jnp.sqrt(away[0] * away[0] + away[1] * away[1] + away[2] * away[2])
                    c, s = sincos_turns(reach * orders)
                    ec = jnp.broadcast_to(c[7:8, :], (8, 128))
                    es = jnp.broadcast_to(s[7:8, :], (8, 128))
                    state.append([c, s, ec * c - es * s, es * c + ec * s, ec + ec])
                for a in range(half // 8):
                    re_sum = acc[0, a * 8 : a * 8 + 8, t * 128 : t * 128 + 128]
                    im_sum = acc[1, a * 8 : a * 8 + 8, t * 128 : t * 128 + 128]
                    for j in range(2):
                        c, s, c_next, s_next, twice = state[j]
                        re = prod[pair + j, a * 8 : a * 8 + 8, t * 128 : t * 128 + 128]
                        im = prod[pair + j, half + a * 8 : half + a * 8 + 8, t * 128 : t * 128 + 128]
                        re_sum = re_sum + (re * c + im * s)
                        im_sum = im_sum + (im * c - re * s)
                        state[j] = [c_next, s_next, twice * c_next - c, twice * s_next - s, twice]
                    acc[0, a * 8 : a * 8 + 8, t * 128 : t * 128 + 128] = re_sum
                    acc[1, a * 8 : a * 8 + 8, t * 128 : t * 128 + 128] = im_sum
        return 0

    lax.fori_loop(0, total, group, 0)
    shares, _, per, _ = out.shape
    each = 128 // per
    for k in range(2):
        for t in range(tiles):
            turned = jnp.transpose(acc[k, :, t * 128 : (t + 1) * 128])
            for e in range(each):
                out[t * each + e, k, :, :] = turned[e * per : (e + 1) * per, :]


def observe(live, centre, sp, wts, lis, shares):
    slots, k2, bp = sp.shape
    span = lis.shape[1] * 128
    vm = pl.BlockSpec(memory_space=pltpu.VMEM)
    sm = pl.BlockSpec(memory_space=pltpu.SMEM)
    return pl.pallas_call(
        observe_kernel,
        out_shape=jax.ShapeDtypeStruct((shares, 2, span // shares, k2 // 2), jnp.float32),
        in_specs=[sm, sm, vm, vm, vm],
        out_specs=vm,
        scratch_shapes=[
            pltpu.VMEM((BATCH, k2, span), jnp.float32),
            pltpu.VMEM((2, k2 // 2, span), jnp.float32),
        ],
        name="observe",
        compiler_params=pltpu.CompilerParams(vmem_limit_bytes=8 * 1024 * 1024),
    )(live, centre, sp, wts, lis)


def swap(value, axis, bit):
    size = lax.axis_size(axis)
    return lax.ppermute(value, axis, [(i, i ^ bit) for i in range(size)])


def reduce_spectra(shares):
    size = shares.shape[0]
    here = lax.axis_index("gz")
    bit = 1
    while bit < size:
        pairs = shares.reshape((shares.shape[0] // 2, 2) + shares.shape[1:])
        up = (here // bit) % 2
        mine = lax.dynamic_index_in_dim(pairs, up, 1, keepdims=False)
        theirs = lax.dynamic_index_in_dim(pairs, 1 - up, 1, keepdims=False)
        shares = mine + swap(theirs, "gz", bit)
        bit *= 2
    total = shares[0]
    for axis in ("gx", "gy"):
        bit = 1
        while bit < lax.axis_size(axis):
            total = total + swap(total, axis, bit)
            bit *= 2
    return total


def local(
    state_old,
    state_section,
    panel_record,
    panel_cell,
    panel_angles,
    owned_blocks,
    listener_angles,
    listener_range,
):
    cells_x, cells_y, cells_z = state_section.shape[1:]
    counts = (
        cells_x * lax.axis_size("gx"),
        cells_y * lax.axis_size("gy"),
        cells_z * lax.axis_size("gz"),
    )
    step_size = COURANT / max(counts)
    slot_count, block_rows = panel_cell.shape
    samples = panel_record.shape[1]
    shares = lax.axis_size("gz")
    places = panel_places(
        panel_cell,
        lax.axis_index("gx"),
        lax.axis_index("gy"),
        lax.axis_index("gz"),
        cells_x,
        cells_y,
        cells_z,
        counts,
    )
    live = jnp.arange(slot_count, dtype=jnp.int32) < owned_blocks[0]
    normals = directions(panel_angles.reshape(2, slot_count, block_rows))
    normals = jnp.where(live[None, :, None], normals * (0.25 / math.pi), 0.0)
    geometry = jnp.concatenate([jnp.transpose(places, (1, 0, 2)), normals], axis=0)
    centres = jnp.transpose(jnp.mean(places, axis=2))
    listeners = 0.5 + listener_range[None, :] * directions(listener_angles)
    listeners = jnp.transpose(listeners.reshape(3, shares, CHUNKS, -1), (0, 2, 1, 3))
    listeners = listeners.reshape(3, -1, 128)
    parts = weights(owned_blocks, geometry, listeners, CHUNKS)
    updated = flow(state_old, state_section, counts, step_size)
    heard = spectra(
        owned_blocks, updated.reshape(-1, cells_z), panel_record, panel_cell, dft_table(samples, FREQS), cells_x * cells_y
    )
    tiles = listeners.shape[1] // CHUNKS
    pieces = []
    for q in range(CHUNKS):
        own = listeners[:, q * tiles : (q + 1) * tiles]
        pieces.append(reduce_spectra(observe(owned_blocks, centres, heard, parts[q], own, shares)))
    return (updated, jnp.concatenate(pieces, axis=1))


def solution(mesh):
    return jax.shard_map(
        local,
        mesh=mesh,
        in_specs=(
            P(None, "gx", "gy", "gz"),
            P(None, "gx", "gy", "gz"),
            P(("gx", "gy", "gz"), None),
            P(("gx", "gy", "gz"), None),
            P(None, ("gx", "gy", "gz")),
            P(("gx", "gy", "gz")),
            P(),
            P(),
        ),
        out_specs=(P(None, "gx", "gy", "gz"), P(None, "gz", None)),
        check_vma=False,
    )
```

```python
import functools
import math

import jax
import jax.numpy as jnp
import numpy as np
from jax import lax
from jax.experimental import pallas as pl
from jax.experimental.pallas import tpu as pltpu
from jax.sharding import PartitionSpec as P

FREQS = 128
BATCH = 4
CHUNKS = 4
TIED = True
NT = (((1,), (1,)), ((), ()))


GAMMA_GAS = 4.4
PRESSURE_INF = 1.0
WENO_EPS = 1e-06
WAVE_STEP = 0.25
COURANT = 0.08


def pack_kernel(state, turned, zlo, zhi, ylo, yhi, xends, *, cx, cy, cz):
    plane = cx * cy
    groups = plane // 128
    for c in range(5):
        for g in range(groups):
            row = c * plane + g * 128
            turned[row : row + cz, :] = jnp.transpose(state[row : row + 128, :])
        for k in range(3):
            ylo[(c * 3 + k) * cx : (c * 3 + k + 1) * cx, :] = state[pl.ds(c * plane + k, cx, stride=cy), :]
            yhi[(c * 3 + k) * cx : (c * 3 + k + 1) * cx, :] = state[pl.ds(c * plane + cy - 3 + k, cx, stride=cy), :]
            zlo[(c * 3 + k) * groups : (c * 3 + k + 1) * groups, :] = turned[pl.ds(c * plane + k, groups, stride=128), :]
            zhi[(c * 3 + k) * groups : (c * 3 + k + 1) * groups, :] = turned[pl.ds(c * plane + cz - 3 + k, groups, stride=128), :]
        xends[c * 3 * cy : (c + 1) * 3 * cy, :] = state[c * plane : c * plane + 3 * cy, :]
        xends[(5 + c) * 3 * cy : (6 + c) * 3 * cy, :] = state[c * plane + (cx - 3) * cy : (c + 1) * plane, :]


def pack(state, cx, cy, cz):
    groups = cx * cy // 128
    rows = [state.shape[0]] + [15 * groups] * 2 + [15 * cx] * 2 + [30 * cy]
    vm = pl.BlockSpec(memory_space=pltpu.VMEM)
    return pl.pallas_call(
        functools.partial(pack_kernel, cx=cx, cy=cy, cz=cz),
        out_shape=[jax.ShapeDtypeStruct((r, 128), jnp.float32) for r in rows],
        in_specs=[vm],
        out_specs=[vm] * 6,
        name="pack",
        compiler_params=pltpu.CompilerParams(vmem_limit_bytes=2 * 1024 * 1024),
    )(state)


def weno_shift(d1, d2, d3, d4):
    a0, a1, a2 = d2 - d1, d3 - d2, d4 - d3
    h2, h3 = 0.75 * d2, 0.75 * d3
    eps = 3.0 * WENO_EPS
    e0 = (a0 * a0 + eps) + h2 * (d2 + a0)
    e1 = (a1 * a1 + eps) + h2 * d3
    e2 = (a2 * a2 + eps) + h3 * (d3 - a2)
    t1 = e1 * e1
    u0 = 3.0 * (e0 * e0)
    u2 = 2.0 * (e2 * e2)
    w0, w1, w2 = t1 * u2, u0 * u2, u0 * t1
    below = 0.5 * w0 + (w1 + w2)
    above = w0 * (a1 - a0) + w2 * (a2 - a1)
    return (d2 + (d3 + d3)) - above * (1.0 / below)


def line_kernel_body(cells, flux, speed, wave, emit, *, n, width, axis):
    length = n + 6
    tiles = width // 8
    span = length * width

    def fluxes(p, _):
        for w in range(tiles):
            at = pl.multiple_of(p * width + w * 8, 8)
            rho = cells[pl.ds(at, 8), :]
            m = [cells[pl.ds((1 + k) * span + at, 8), :] for k in range(3)]
            energy = cells[pl.ds(4 * span + at, 8), :]
            inv = 1.0 / rho
            u = m[axis] * inv
            twice = (m[0] * m[0] + m[1] * m[1] + m[2] * m[2]) * inv
            pressure = (GAMMA_GAS - 1.0) * (energy - 0.5 * twice) - GAMMA_GAS * PRESSURE_INF
            sound = jnp.sqrt(GAMMA_GAS * (pressure + PRESSURE_INF) * inv)
            speed[pl.ds(at, 8), :] = jnp.abs(u) + sound
            flux[pl.ds(at, 8), :] = m[axis]
            for k in range(3):
                carried = m[k] * u
                if k == axis:
                    carried = carried + pressure
                flux[pl.ds((1 + k) * span + at, 8), :] = carried
            flux[pl.ds(4 * span + at, 8), :] = (energy + pressure) * u
        return 0

    lax.fori_loop(0, length, fluxes, 0, unroll=5 if tiles == 1 else 2)

    def waves(i, _):
        for w in range(tiles):
            at = pl.multiple_of(i * width + w * 8, 8)
            top = speed[pl.ds(at, 8), :]
            for k in range(1, 6):
                top = jnp.maximum(top, speed[pl.ds(at + k * width, 8), :])
            wave[pl.ds(at, 8), :] = top
        return 0

    lax.fori_loop(0, n + 1, waves, 0, unroll={1: 5, 2: 3}.get(tiles, 1))

    def line(index, _):
        c = index // tiles
        w = index % tiles

        def load(ref, p):
            return ref[pl.ds(pl.multiple_of(c * span + p * width + w * 8, 8), 8), :]

        q = [load(cells, p) for p in range(5)]
        f = [load(flux, p) for p in range(5)]
        dq = [q[k + 1] - q[k] for k in range(4)]
        df = [f[k + 1] - f[k] for k in range(4)]
        q_last, f_last, f_mid, f_near = q[4], f[4], f[2], f[3]
        before = None
        for i in range(n + 1):
            q_new, f_new = load(cells, i + 5), load(flux, i + 5)
            dq.append(q_new - q_last)
            df.append(f_new - f_last)
            alpha = wave[pl.ds(pl.multiple_of(i * width + w * 8, 8), 8), :]
            drift = [alpha * v for v in dq]
            up = weno_shift(*[df[k] + drift[k] for k in range(4)])
            down = weno_shift(*[drift[k] - df[k] for k in (4, 3, 2, 1)])
            here = 6.0 * ((f_mid + f_near) - drift[2]) + (up + down)
            if before is not None:
                emit(c, w, i - 1, here - before)
            before = here
            dq, df = dq[1:], df[1:]
            f_mid, f_near = f_near, f_last
            q_last, f_last = q_new, f_new
        return 0

    lax.fori_loop(0, 5 * tiles, line, 0)


def z_kernel(turned, left, right, out, cells, flux, speed, wave, part, *, cx, cy, cz, scale):
    plane = cx * cy
    groups = plane // 128
    width = 2 * groups
    n = cz // 2
    length = n + 6
    for c in range(5):
        base = c * length * width
        for p in range(3):
            cells[pl.ds(base + p * width, groups, stride=2), :] = left[(c * 3 + p) * groups : (c * 3 + p + 1) * groups, :]
            cells[pl.ds(base + p * width + 1, groups, stride=2), :] = turned[pl.ds(c * plane + n - 3 + p, groups, stride=128), :]
            q = n + 3 + p
            cells[pl.ds(base + q * width, groups, stride=2), :] = turned[pl.ds(c * plane + n + p, groups, stride=128), :]
            cells[pl.ds(base + q * width + 1, groups, stride=2), :] = right[(c * 3 + p) * groups : (c * 3 + p + 1) * groups, :]
        for p in range(n):
            cells[base + (p + 3) * width : base + (p + 4) * width, :] = turned[pl.ds(c * plane + p, width, stride=n), :]

    def emit(c, w, i, value):
        part[pl.ds(c * plane + i, width, stride=n), :] = value * scale

    line_kernel_body(cells, flux, speed, wave, emit, n=n, width=width, axis=2)
    for c in range(5):
        for g in range(groups):
            row = c * plane + g * 128
            out[row : row + 128, :] = jnp.transpose(part[row : row + cz, :])


def y_kernel(state, left, right, start, out, cells, flux, speed, wave, *, cx, cy, scale):
    plane = cx * cy
    length = cy + 6
    for c in range(5):
        base = c * length * cx
        cells[base : base + 3 * cx, :] = left[c * 3 * cx : (c + 1) * 3 * cx, :]
        cells[base + (cy + 3) * cx : base + length * cx, :] = right[c * 3 * cx : (c + 1) * 3 * cx, :]
        for p in range(cy):
            for x in range(0, cx, 8):
                cells[base + (p + 3) * cx + x : base + (p + 3) * cx + x + 8, :] = state[pl.ds(c * plane + x * cy + p, 8, stride=cy), :]

    def emit(c, w, i, value):
        rows = pl.ds(c * plane + w * 8 * cy + i, 8, stride=cy)
        out[rows, :] = start[rows, :] + value * scale

    line_kernel_body(cells, flux, speed, wave, emit, n=cy, width=cx, axis=1)


def x_kernel(state, ends, start, old, out, density, cells, flux, speed, wave, *, cx, cy, scale):
    plane = cx * cy
    length = cx + 6
    for c in range(5):
        base = c * length * cy
        cells[base : base + 3 * cy, :] = ends[(5 + c) * 3 * cy : (6 + c) * 3 * cy, :]
        cells[base + 3 * cy : base + (cx + 3) * cy, :] = state[c * plane : (c + 1) * plane, :]
        cells[base + (cx + 3) * cy : base + length * cy, :] = ends[c * 3 * cy : (c + 1) * 3 * cy, :]

    def emit(c, w, i, value):
        rows = pl.ds(pl.multiple_of(c * plane + i * cy + w * 8, 8), 8)
        change = start[rows, :] + value * scale
        out[rows, :] = (0.75 * old[rows, :] + 0.25 * state[rows, :]) - change

    line_kernel_body(cells, flux, speed, wave, emit, n=cx, width=cy, axis=0)
    density[...] = out[0:plane, :]


def line_call(kernel, operands, n, width, name, more=(), results=()):
    length = n + 6
    vm = pl.BlockSpec(memory_space=pltpu.VMEM)
    return pl.pallas_call(
        kernel,
        out_shape=[jax.ShapeDtypeStruct(shape, jnp.float32) for shape in (operands[0].shape, *results)],
        in_specs=[vm] * len(operands),
        out_specs=[vm] * (1 + len(results)),
        scratch_shapes=[
            pltpu.VMEM((5 * length * width, 128), jnp.float32),
            pltpu.VMEM((5 * length * width, 128), jnp.float32),
            pltpu.VMEM((length * width, 128), jnp.float32),
            pltpu.VMEM((length * width, 128), jnp.float32),
        ]
        + list(more),
        name=name,
        compiler_params=pltpu.CompilerParams(vmem_limit_bytes=6 * 1024 * 1024),
    )(*operands)


def neighbours(first, last, axis):
    size = lax.axis_size(axis)
    up = [(i, (i + 1) % size) for i in range(size)]
    down = [(j, i) for i, j in up]
    return lax.ppermute(last, axis, up), lax.ppermute(first, axis, down)


def flow(state_old, state_section, counts, step_size):
    shape = state_section.shape
    cx, cy, cz = shape[1:]
    state = state_section.reshape(-1, cz)
    turned, zlo, zhi, ylo, yhi, xends = pack(state, cx, cy, cz)
    if lax.axis_size("gx") == 2:
        ends = swap(xends, "gx", 1)
    else:
        ends = jnp.concatenate(neighbours(xends[: xends.shape[0] // 2], xends[xends.shape[0] // 2 :], "gx")[::-1])
    zl, zr = neighbours(zlo, zhi, "gz")
    yl, yr = neighbours(ylo, yhi, "gy")
    scales = [0.25 * step_size * n / 12.0 for n in counts]
    plane = cx * cy
    (part,) = line_call(
        functools.partial(z_kernel, cx=cx, cy=cy, cz=cz, scale=scales[2]),
        (turned, zl, zr), cz // 2, plane // 64, "along_z",
        (pltpu.VMEM((5 * plane, 128), jnp.float32),),
    )
    (part,) = line_call(functools.partial(y_kernel, cx=cx, cy=cy, scale=scales[1]), (state, yl, yr, part), cy, cx, "along_y")
    updated, density = line_call(
        functools.partial(x_kernel, cx=cx, cy=cy, scale=scales[0]),
        (state, ends, part, state_old.reshape(-1, cz)), cx, cy, "along_x", (), ((plane, cz),),
    )
    return updated.reshape(shape), density


def dft_table(sample_count, freq_count):
    times = np.arange(sample_count, dtype=np.int64)[None, :]
    orders = np.arange(1, freq_count + 1, dtype=np.int64)[:, None]
    phases = (np.float32(2.0 * math.pi / sample_count) * (times * orders % sample_count).astype(np.float32)).astype(np.float64)
    scaling = 1.0 / math.sqrt(sample_count)
    both = np.concatenate([np.cos(phases), -np.sin(phases)], axis=0).astype(np.float32) * np.float32(scaling)
    return jnp.asarray(both, jnp.bfloat16)


def double_angle(x):
    x2 = x * x
    s = 1.0 / 6227020800.0
    s = s * x2 - 1.0 / 39916800.0
    s = s * x2 + 1.0 / 362880.0
    s = s * x2 - 1.0 / 5040.0
    s = s * x2 + 1.0 / 120.0
    s = s * x2 - 1.0 / 6.0
    s = (s * x2) * x + x
    c = 1.0 / 479001600.0
    c = c * x2 - 1.0 / 3628800.0
    c = c * x2 + 1.0 / 40320.0
    c = c * x2 - 1.0 / 720.0
    c = c * x2 + 1.0 / 24.0
    c = c * x2 - 0.5
    c = c * x2 + 1.0
    s2 = s + s
    return 1.0 - s2 * s, s2 * c


def sincos_turns(turns):
    return double_angle((turns - jnp.round(turns)) * math.pi)


def direction(polar, azimuth):
    cos_p, sin_p = double_angle(0.25 * polar)
    cos_a, sin_a = double_angle(0.5 * azimuth)
    return cos_p * cos_a, cos_p * sin_a, sin_p


def weights_kernel(live, corner, cell, angles, raw, out, centre, lis, geo, lisb, *, sizes, counts):
    slots, bp = cell.shape
    tiles = lis.shape[1]
    span = tiles * 128 // CHUNKS
    cells = cell[...].astype(jnp.float32)
    along_x = jnp.floor((cells + 0.5) * (1.0 / (sizes[1] * sizes[2])))
    rest = cells - along_x * float(sizes[1] * sizes[2])
    along_y = jnp.floor((rest + 0.5) * (1.0 / sizes[2]))
    along_z = rest - along_y * float(sizes[2])
    for k, along in enumerate((along_x, along_y, along_z)):
        place = ((along + corner[k].astype(jnp.float32)) + 0.5) / float(counts[k])
        geo[k] = place
        mean = jnp.sum(place, axis=1, keepdims=True) * (1.0 / bp)
        centre[k] = jnp.broadcast_to(mean, (slots, 128))
    shown = lax.broadcasted_iota(jnp.int32, (slots, bp), 0) < live[0]
    for k, part in enumerate(direction(angles[0], angles[1])):
        geo[3 + k] = jnp.where(shown, part * (0.25 / math.pi), 0.0)
    for k, part in enumerate(direction(raw[0], raw[1])):
        lis[k] = 0.5 + raw[2] * part
    for k in range(3):
        for t in range(tiles):
            row = lis[k, t : t + 1, :]
            lisb[k, t * 128 : (t + 1) * 128, :] = jnp.transpose(jnp.broadcast_to(row, (128, 128)))

    def block(b, _):
        px, py, pz, nx, ny, nz = [geo[k, pl.ds(b, 1), :] for k in range(6)]
        for q in range(CHUNKS):
            for r in range(0, span, 16):
                at = q * span + r
                ox = lisb[0, at : at + 16, :] - px
                oy = lisb[1, at : at + 16, :] - py
                oz = lisb[2, at : at + 16, :] - pz
                d2 = ox * ox + oy * oy + oz * oz
                facing = nx * ox + ny * oy + nz * oz
                row = pl.multiple_of(q * slots * span + b * span + r, 16)
                out[pl.ds(row, 16), :] = (facing * (1.0 / d2)).astype(jnp.bfloat16)
        return 0

    lax.fori_loop(0, (live[0] + BATCH - 1) // BATCH * BATCH, block, 0)


def weights(live, corner, cell, angles, raw, sizes, counts):
    slots, bp = cell.shape
    obs = raw.shape[1] * 128
    vm = pl.BlockSpec(memory_space=pltpu.VMEM)
    sm = pl.BlockSpec(memory_space=pltpu.SMEM)
    return pl.pallas_call(
        functools.partial(weights_kernel, sizes=sizes, counts=counts),
        out_shape=[
            jax.ShapeDtypeStruct((slots * obs, bp), jnp.bfloat16),
            jax.ShapeDtypeStruct((3, slots, 128), jnp.float32),
            jax.ShapeDtypeStruct(raw.shape, jnp.float32),
        ],
        in_specs=[sm, sm, vm, vm, vm],
        out_specs=[vm] * 3,
        scratch_shapes=[pltpu.VMEM((6, slots, bp), jnp.float32), pltpu.VMEM((3, obs, 128), jnp.float32)],
        name="weights",
        compiler_params=pltpu.CompilerParams(vmem_limit_bytes=4 * 1024 * 1024),
    )(live, corner, cell, angles, raw)


def spectra_kernel(live, dens, rec, cell, table, sp, dens3, held, onehot, src, sems):
    slots, bp = cell.shape
    rows = dens.shape[0] // 2
    groups = slots // BATCH
    total = (live[0] + BATCH - 1) // BATCH
    span = BATCH * bp

    def fetch(g):
        at = pl.ds(pl.multiple_of(g * span, span), span)
        return pltpu.make_async_copy(rec.at[at, :], held.at[at, :], sems.at[g])

    for g in range(groups):
        @pl.when(g < total)
        def _():
            fetch(g).start()

    for h in range(2):
        d = dens[pl.ds(h, rows, stride=2), :]
        hi = d.astype(jnp.bfloat16)
        left = d - hi.astype(jnp.float32)
        mid = left.astype(jnp.bfloat16)
        lo = (left - mid.astype(jnp.float32)).astype(jnp.bfloat16)
        for k, part in enumerate((hi, mid, lo)):
            dens3[k, :, h * 128 : (h + 1) * 128] = part
    lane = lax.broadcasted_iota(jnp.int32, (bp, 128), 1).astype(jnp.float32)

    def group(g, _):
        lows = []
        for j in range(BATCH):
            cells = cell[pl.ds(g * BATCH + j, 1), :].astype(jnp.float32)
            col = jnp.transpose(jnp.broadcast_to(cells, (128, 128)))
            high = jnp.floor(col * (1.0 / 256.0))
            low = col - 256.0 * high
            lows.append(low)
            for h in range(rows // 128):
                hit = jnp.where(high == lane + float(128 * h), 1.0, 0.0).astype(jnp.bfloat16)
                onehot[j * bp : (j + 1) * bp, h * 128 : (h + 1) * 128] = hit
        hot = onehot[...]
        picked = jnp.dot(hot, dens3[0], preferred_element_type=jnp.float32)
        picked = picked + jnp.dot(hot, dens3[1], preferred_element_type=jnp.float32)
        picked = picked + jnp.dot(hot, dens3[2], preferred_element_type=jnp.float32)
        fetch(g).wait()
        for j in range(BATCH):
            own = picked[j * bp : (j + 1) * bp, :]
            found = jnp.where(lows[j] == lane, own[:, 0:128], 0.0) + jnp.where(lows[j] == lane + 128.0, own[:, 128:256], 0.0)
            sampled = jnp.sum(found, axis=1, keepdims=True)
            record = held[pl.ds(pl.multiple_of(g * span + j * bp, bp), bp), :].astype(jnp.float32)
            src[j * bp : (j + 1) * bp, :] = (record * sampled).astype(jnp.bfloat16)
        for j in range(0, BATCH, 2):
            both = lax.dot_general(table[...], src[j * bp : (j + 2) * bp, :], NT, preferred_element_type=jnp.float32)
            both = both.astype(jnp.bfloat16)
            sp[g * BATCH + j] = both[:, 0:bp]
            sp[g * BATCH + j + 1] = both[:, bp : 2 * bp]
        return 0

    lax.fori_loop(0, total, group, 0)


def spectra(live, dens, rec, cell, table):
    rows = dens.shape[0]
    slots, bp = cell.shape
    samples = rec.shape[1]
    k2 = table.shape[0]
    vm = pl.BlockSpec(memory_space=pltpu.VMEM)
    return pl.pallas_call(
        spectra_kernel,
        out_shape=jax.ShapeDtypeStruct((slots, k2, bp), jnp.bfloat16),
        in_specs=[
            pl.BlockSpec(memory_space=pltpu.SMEM),
            vm,
            pl.BlockSpec(memory_space=pl.ANY),
            vm,
            vm,
        ],
        out_specs=vm,
        scratch_shapes=[
            pltpu.VMEM((3, rows // 2, 256), jnp.bfloat16),
            pltpu.VMEM(rec.shape, jnp.bfloat16),
            pltpu.VMEM((BATCH * bp, rows // 2), jnp.bfloat16),
            pltpu.VMEM((BATCH * bp, samples), jnp.bfloat16),
            pltpu.SemaphoreType.DMA((slots // BATCH,)),
        ],
        name="spectra",
        compiler_params=pltpu.CompilerParams(vmem_limit_bytes=8 * 1024 * 1024),
    )(live, dens, rec, cell, table)


def observe_kernel(live, centre, sp, wts, lis, out, prod, acc, *, chunk):
    slots, k2, bp = sp.shape
    tiles = lis.shape[1] // CHUNKS
    half = k2 // 2
    span = tiles * 128
    total = (live[0] + BATCH - 1) // BATCH
    acc[...] = jnp.zeros(acc.shape, jnp.float32)
    orders = lax.broadcasted_iota(jnp.int32, (8, 128), 0).astype(jnp.float32) + 1.0
    orders = orders * (WAVE_STEP / (2.0 * math.pi))

    def group(g, _):
        for pair in range(0, BATCH, 2):
            waves = []
            for j in range(2):
                b = g * BATCH + pair + j
                held = wts[pl.ds(pl.multiple_of(chunk * slots * span + b * span, span), span), :]
                prod[pair + j] = lax.dot_general(sp[b], held, NT, preferred_element_type=jnp.float32)
            for t in range(tiles):
                state = []
                for j in range(2):
                    b = g * BATCH + pair + j
                    u = chunk * tiles + t
                    away = [jnp.broadcast_to(lis[k, u : u + 1, :] - centre[k, pl.ds(b, 1), :], (8, 128)) for k in range(3)]
                    reach = jnp.sqrt(away[0] * away[0] + away[1] * away[1] + away[2] * away[2])
                    c, s = sincos_turns(reach * orders)
                    ec = jnp.broadcast_to(c[7:8, :], (8, 128))
                    es = jnp.broadcast_to(s[7:8, :], (8, 128))
                    state.append([c, s, ec * c - es * s, es * c + ec * s, ec + ec])
                for a in range(half // 8):
                    re_sum = acc[0, a * 8 : a * 8 + 8, t * 128 : t * 128 + 128]
                    im_sum = acc[1, a * 8 : a * 8 + 8, t * 128 : t * 128 + 128]
                    for j in range(2):
                        c, s, c_next, s_next, twice = state[j]
                        re = prod[pair + j, a * 8 : a * 8 + 8, t * 128 : t * 128 + 128]
                        im = prod[pair + j, half + a * 8 : half + a * 8 + 8, t * 128 : t * 128 + 128]
                        re_sum = re_sum + (re * c + im * s)
                        im_sum = im_sum + (im * c - re * s)
                        state[j] = [c_next, s_next, twice * c_next - c, twice * s_next - s, twice]
                    acc[0, a * 8 : a * 8 + 8, t * 128 : t * 128 + 128] = re_sum
                    acc[1, a * 8 : a * 8 + 8, t * 128 : t * 128 + 128] = im_sum
        return 0

    lax.fori_loop(0, total, group, 0)
    shares, _, per, _ = out.shape
    each = 128 // per
    for k in range(2):
        for t in range(tiles):
            turned = jnp.transpose(acc[k, :, t * 128 : (t + 1) * 128])
            for e in range(each):
                out[t * each + e, k, :, :] = turned[e * per : (e + 1) * per, :]


def observe(chunk, live, centre, sp, wts, lis, shares):
    slots, k2, bp = sp.shape
    span = lis.shape[1] * 128 // CHUNKS
    vm = pl.BlockSpec(memory_space=pltpu.VMEM)
    sm = pl.BlockSpec(memory_space=pltpu.SMEM)
    return pl.pallas_call(
        functools.partial(observe_kernel, chunk=chunk),
        out_shape=jax.ShapeDtypeStruct((shares, 2, span // shares, k2 // 2), jnp.float32),
        in_specs=[sm, vm, vm, vm, vm],
        out_specs=vm,
        scratch_shapes=[
            pltpu.VMEM((BATCH, k2, span), jnp.float32),
            pltpu.VMEM((2, k2 // 2, span), jnp.float32),
        ],
        name="observe",
        compiler_params=pltpu.CompilerParams(vmem_limit_bytes=3 * 1024 * 1024),
    )(live, centre, sp, wts, lis)


def swap(value, axis, bit):
    size = lax.axis_size(axis)
    return lax.ppermute(value, axis, [(i, i ^ bit) for i in range(size)])


def stages():
    steps = []
    for axis in ("gz", "gx", "gy"):
        bit = 1
        while bit < lax.axis_size(axis):
            steps.append((axis, bit))
            bit *= 2
    return steps


def exchange(value, axis, bit):
    if axis != "gz":
        return value + swap(value, axis, bit)
    up = (lax.axis_index("gz") // bit) % 2
    pairs = value.reshape((value.shape[0] // 2, 2) + value.shape[1:])
    mine = lax.dynamic_index_in_dim(pairs, up, 1, keepdims=False)
    theirs = lax.dynamic_index_in_dim(pairs, 1 - up, 1, keepdims=False)
    return mine + swap(theirs, "gz", bit)


def local(
    state_old,
    state_section,
    panel_record,
    panel_cell,
    panel_angles,
    owned_blocks,
    listener_angles,
    listener_range,
):
    sizes = state_section.shape[1:]
    axes = ("gx", "gy", "gz")
    counts = tuple(n * lax.axis_size(axis) for n, axis in zip(sizes, axes))
    step_size = COURANT / max(counts)
    slot_count, block_rows = panel_cell.shape
    samples = panel_record.shape[1]
    shares = lax.axis_size("gz")
    corner = jnp.stack([lax.axis_index(axis) * n for n, axis in zip(sizes, axes)]).astype(jnp.int32)
    raw = jnp.concatenate([listener_angles, listener_range[None]], axis=0)
    raw = jnp.transpose(raw.reshape(3, shares, CHUNKS, -1), (0, 2, 1, 3)).reshape(3, -1, 128)
    angles = panel_angles.reshape(2, slot_count, block_rows)
    wts, centres, listeners = weights(owned_blocks, corner, panel_cell, angles, raw, sizes, counts)
    updated, density = flow(state_old, state_section, counts, step_size)
    heard = spectra(owned_blocks, density, panel_record, panel_cell, dft_table(samples, FREQS))
    steps = stages()
    pieces = []
    live = owned_blocks
    for q in range(CHUNKS):
        if TIED and q >= 2:
            pieces = [exchange(v, *steps[n]) if n < len(steps) else v for v, n in zip(pieces, range(q - 2, -1, -1))] + pieces[q - 1 :]
            tied = lax.optimization_barrier((live, *pieces[: q - 1]))
            live, pieces = tied[0], list(tied[1:]) + pieces[q - 1 :]
        pieces.append(observe(q, live, centres, heard, wts, listeners, shares))
    for n in range(len(steps) + CHUNKS):
        for q in range(CHUNKS):
            done = max(CHUNKS - 2 - q, 0) if TIED else 0
            if done + n < len(steps):
                pieces[q] = exchange(pieces[q], *steps[done + n])
    pieces = [v.reshape((2, -1, FREQS)) for v in pieces]
    return (updated, jnp.concatenate(pieces, axis=1))


def solution(mesh):
    return jax.shard_map(
        local,
        mesh=mesh,
        in_specs=(
            P(None, "gx", "gy", "gz"),
            P(None, "gx", "gy", "gz"),
            P(("gx", "gy", "gz"), None),
            P(("gx", "gy", "gz"), None),
            P(None, ("gx", "gy", "gz")),
            P(("gx", "gy", "gz")),
            P(),
            P(),
        ),
        out_specs=(P(None, "gx", "gy", "gz"), P(None, "gz", None)),
        check_vma=False,
    )
```

```python
import functools
import math

import jax
import jax.numpy as jnp
import numpy as np
from jax import lax
from jax.experimental import pallas as pl
from jax.experimental.pallas import tpu as pltpu
from jax.sharding import PartitionSpec as P

FREQS = 128
BATCH = 4
CHUNKS = 2
PARTS = 3
NT = (((1,), (1,)), ((), ()))


GAMMA_GAS = 4.4
PRESSURE_INF = 1.0
WENO_EPS = 1e-06
WAVE_STEP = 0.25
COURANT = 0.08


def pack_kernel(state, turned, zlo, zhi, ylo, yhi, xends, *, cx, cy, cz):
    plane = cx * cy
    groups = plane // 128
    for c in range(5):
        for g in range(groups):
            row = c * plane + g * 128
            turned[row : row + cz, :] = jnp.transpose(state[row : row + 128, :])
        for k in range(3):
            ylo[(c * 3 + k) * cx : (c * 3 + k + 1) * cx, :] = state[pl.ds(c * plane + k, cx, stride=cy), :]
            yhi[(c * 3 + k) * cx : (c * 3 + k + 1) * cx, :] = state[pl.ds(c * plane + cy - 3 + k, cx, stride=cy), :]
            zlo[(c * 3 + k) * groups : (c * 3 + k + 1) * groups, :] = turned[pl.ds(c * plane + k, groups, stride=128), :]
            zhi[(c * 3 + k) * groups : (c * 3 + k + 1) * groups, :] = turned[pl.ds(c * plane + cz - 3 + k, groups, stride=128), :]
        xends[c * 3 * cy : (c + 1) * 3 * cy, :] = state[c * plane : c * plane + 3 * cy, :]
        xends[(5 + c) * 3 * cy : (6 + c) * 3 * cy, :] = state[c * plane + (cx - 3) * cy : (c + 1) * plane, :]


def pack(state, cx, cy, cz):
    groups = cx * cy // 128
    rows = [state.shape[0]] + [15 * groups] * 2 + [15 * cx] * 2 + [30 * cy]
    vm = pl.BlockSpec(memory_space=pltpu.VMEM)
    return pl.pallas_call(
        functools.partial(pack_kernel, cx=cx, cy=cy, cz=cz),
        out_shape=[jax.ShapeDtypeStruct((r, 128), jnp.float32) for r in rows],
        in_specs=[vm],
        out_specs=[vm] * 6,
        name="pack",
        compiler_params=pltpu.CompilerParams(vmem_limit_bytes=2 * 1024 * 1024),
    )(state)


def weno_shift(d1, d2, d3, d4):
    a0, a1, a2 = d2 - d1, d3 - d2, d4 - d3
    h2, h3 = 0.75 * d2, 0.75 * d3
    eps = 3.0 * WENO_EPS
    e0 = (a0 * a0 + eps) + h2 * (d2 + a0)
    e1 = (a1 * a1 + eps) + h2 * d3
    e2 = (a2 * a2 + eps) + h3 * (d3 - a2)
    t1 = e1 * e1
    u0 = 3.0 * (e0 * e0)
    u2 = 2.0 * (e2 * e2)
    w0, w1, w2 = t1 * u2, u0 * u2, u0 * t1
    below = 0.5 * w0 + (w1 + w2)
    above = w0 * (a1 - a0) + w2 * (a2 - a1)
    return (d2 + (d3 + d3)) - above * (1.0 / below)


def line_kernel_body(cells, flux, speed, wave, emit, *, n, width, axis):
    length = n + 6
    tiles = width // 8
    span = length * width

    def fluxes(p, _):
        for w in range(tiles):
            at = pl.multiple_of(p * width + w * 8, 8)
            rho = cells[pl.ds(at, 8), :]
            m = [cells[pl.ds((1 + k) * span + at, 8), :] for k in range(3)]
            energy = cells[pl.ds(4 * span + at, 8), :]
            inv = 1.0 / rho
            u = m[axis] * inv
            twice = (m[0] * m[0] + m[1] * m[1] + m[2] * m[2]) * inv
            pressure = (GAMMA_GAS - 1.0) * (energy - 0.5 * twice) - GAMMA_GAS * PRESSURE_INF
            sound = jnp.sqrt(GAMMA_GAS * (pressure + PRESSURE_INF) * inv)
            speed[pl.ds(at, 8), :] = jnp.abs(u) + sound
            flux[pl.ds(at, 8), :] = m[axis]
            for k in range(3):
                carried = m[k] * u
                if k == axis:
                    carried = carried + pressure
                flux[pl.ds((1 + k) * span + at, 8), :] = carried
            flux[pl.ds(4 * span + at, 8), :] = (energy + pressure) * u
        return 0

    lax.fori_loop(0, length, fluxes, 0, unroll=5 if tiles == 1 else 2)

    def waves(i, _):
        for w in range(tiles):
            at = pl.multiple_of(i * width + w * 8, 8)
            top = speed[pl.ds(at, 8), :]
            for k in range(1, 6):
                top = jnp.maximum(top, speed[pl.ds(at + k * width, 8), :])
            wave[pl.ds(at, 8), :] = top
        return 0

    lax.fori_loop(0, n + 1, waves, 0, unroll={1: 5, 2: 3}.get(tiles, 1))

    def line(index, _):
        c = index // tiles
        w = index % tiles

        def load(ref, p):
            return ref[pl.ds(pl.multiple_of(c * span + p * width + w * 8, 8), 8), :]

        q = [load(cells, p) for p in range(5)]
        f = [load(flux, p) for p in range(5)]
        dq = [q[k + 1] - q[k] for k in range(4)]
        df = [f[k + 1] - f[k] for k in range(4)]
        q_last, f_last, f_mid, f_near = q[4], f[4], f[2], f[3]
        before = None
        for i in range(n + 1):
            q_new, f_new = load(cells, i + 5), load(flux, i + 5)
            dq.append(q_new - q_last)
            df.append(f_new - f_last)
            alpha = wave[pl.ds(pl.multiple_of(i * width + w * 8, 8), 8), :]
            drift = [alpha * v for v in dq]
            up = weno_shift(*[df[k] + drift[k] for k in range(4)])
            down = weno_shift(*[drift[k] - df[k] for k in (4, 3, 2, 1)])
            here = 6.0 * ((f_mid + f_near) - drift[2]) + (up + down)
            if before is not None:
                emit(c, w, i - 1, here - before)
            before = here
            dq, df = dq[1:], df[1:]
            f_mid, f_near = f_near, f_last
            q_last, f_last = q_new, f_new
        return 0

    lax.fori_loop(0, 5 * tiles, line, 0)


def z_kernel(turned, left, right, out, cells, flux, speed, wave, part, *, cx, cy, cz, scale):
    plane = cx * cy
    groups = plane // 128
    width = 2 * groups
    n = cz // 2
    length = n + 6
    for c in range(5):
        base = c * length * width
        for p in range(3):
            cells[pl.ds(base + p * width, groups, stride=2), :] = left[(c * 3 + p) * groups : (c * 3 + p + 1) * groups, :]
            cells[pl.ds(base + p * width + 1, groups, stride=2), :] = turned[pl.ds(c * plane + n - 3 + p, groups, stride=128), :]
            q = n + 3 + p
            cells[pl.ds(base + q * width, groups, stride=2), :] = turned[pl.ds(c * plane + n + p, groups, stride=128), :]
            cells[pl.ds(base + q * width + 1, groups, stride=2), :] = right[(c * 3 + p) * groups : (c * 3 + p + 1) * groups, :]
        for p in range(n):
            cells[base + (p + 3) * width : base + (p + 4) * width, :] = turned[pl.ds(c * plane + p, width, stride=n), :]

    def emit(c, w, i, value):
        part[pl.ds(c * plane + i, width, stride=n), :] = value * scale

    line_kernel_body(cells, flux, speed, wave, emit, n=n, width=width, axis=2)
    for c in range(5):
        for g in range(groups):
            row = c * plane + g * 128
            out[row : row + 128, :] = jnp.transpose(part[row : row + cz, :])


def y_kernel(state, left, right, start, out, cells, flux, speed, wave, *, cx, cy, scale):
    plane = cx * cy
    length = cy + 6
    for c in range(5):
        base = c * length * cx
        cells[base : base + 3 * cx, :] = left[c * 3 * cx : (c + 1) * 3 * cx, :]
        cells[base + (cy + 3) * cx : base + length * cx, :] = right[c * 3 * cx : (c + 1) * 3 * cx, :]
        for p in range(cy):
            for x in range(0, cx, 8):
                cells[base + (p + 3) * cx + x : base + (p + 3) * cx + x + 8, :] = state[pl.ds(c * plane + x * cy + p, 8, stride=cy), :]

    def emit(c, w, i, value):
        rows = pl.ds(c * plane + w * 8 * cy + i, 8, stride=cy)
        out[rows, :] = start[rows, :] + value * scale

    line_kernel_body(cells, flux, speed, wave, emit, n=cy, width=cx, axis=1)


def x_kernel(state, ends, start, old, out, density, cells, flux, speed, wave, *, cx, cy, scale):
    plane = cx * cy
    length = cx + 6
    for c in range(5):
        base = c * length * cy
        cells[base : base + 3 * cy, :] = ends[(5 + c) * 3 * cy : (6 + c) * 3 * cy, :]
        cells[base + 3 * cy : base + (cx + 3) * cy, :] = state[c * plane : (c + 1) * plane, :]
        cells[base + (cx + 3) * cy : base + length * cy, :] = ends[c * 3 * cy : (c + 1) * 3 * cy, :]

    def emit(c, w, i, value):
        rows = pl.ds(pl.multiple_of(c * plane + i * cy + w * 8, 8), 8)
        change = start[rows, :] + value * scale
        out[rows, :] = (0.75 * old[rows, :] + 0.25 * state[rows, :]) - change

    line_kernel_body(cells, flux, speed, wave, emit, n=cx, width=cy, axis=0)
    density[...] = out[0:plane, :]


def line_call(kernel, operands, n, width, name, more=(), results=()):
    length = n + 6
    vm = pl.BlockSpec(memory_space=pltpu.VMEM)
    return pl.pallas_call(
        kernel,
        out_shape=[jax.ShapeDtypeStruct(shape, jnp.float32) for shape in (operands[0].shape, *results)],
        in_specs=[vm] * len(operands),
        out_specs=[vm] * (1 + len(results)),
        scratch_shapes=[
            pltpu.VMEM((5 * length * width, 128), jnp.float32),
            pltpu.VMEM((5 * length * width, 128), jnp.float32),
            pltpu.VMEM((length * width, 128), jnp.float32),
            pltpu.VMEM((length * width, 128), jnp.float32),
        ]
        + list(more),
        name=name,
        compiler_params=pltpu.CompilerParams(vmem_limit_bytes=6 * 1024 * 1024),
    )(*operands)


def neighbours(first, last, axis):
    size = lax.axis_size(axis)
    up = [(i, (i + 1) % size) for i in range(size)]
    down = [(j, i) for i, j in up]
    return lax.ppermute(last, axis, up), lax.ppermute(first, axis, down)


def flow(state_old, state_section, counts, step_size):
    shape = state_section.shape
    cx, cy, cz = shape[1:]
    state = state_section.reshape(-1, cz)
    turned, zlo, zhi, ylo, yhi, xends = pack(state, cx, cy, cz)
    if lax.axis_size("gx") == 2:
        ends = swap(xends, "gx", 1)
    else:
        ends = jnp.concatenate(neighbours(xends[: xends.shape[0] // 2], xends[xends.shape[0] // 2 :], "gx")[::-1])
    zl, zr = neighbours(zlo, zhi, "gz")
    yl, yr = neighbours(ylo, yhi, "gy")
    scales = [0.25 * step_size * n / 12.0 for n in counts]
    plane = cx * cy
    (part,) = line_call(
        functools.partial(z_kernel, cx=cx, cy=cy, cz=cz, scale=scales[2]),
        (turned, zl, zr), cz // 2, plane // 64, "along_z",
        (pltpu.VMEM((5 * plane, 128), jnp.float32),),
    )
    (part,) = line_call(functools.partial(y_kernel, cx=cx, cy=cy, scale=scales[1]), (state, yl, yr, part), cy, cx, "along_y")
    updated, density = line_call(
        functools.partial(x_kernel, cx=cx, cy=cy, scale=scales[0]),
        (state, ends, part, state_old.reshape(-1, cz)), cx, cy, "along_x", (), ((plane, cz),),
    )
    return updated.reshape(shape), density


def dft_table(sample_count, freq_count):
    times = np.arange(sample_count, dtype=np.int64)[None, :]
    orders = np.arange(1, freq_count + 1, dtype=np.int64)[:, None]
    phases = (np.float32(2.0 * math.pi / sample_count) * (times * orders % sample_count).astype(np.float32)).astype(np.float64)
    scaling = 1.0 / math.sqrt(sample_count)
    both = np.concatenate([np.cos(phases), -np.sin(phases)], axis=0).astype(np.float32) * np.float32(scaling)
    return jnp.asarray(both, jnp.bfloat16)


def double_angle(x):
    x2 = x * x
    s = 1.0 / 6227020800.0
    s = s * x2 - 1.0 / 39916800.0
    s = s * x2 + 1.0 / 362880.0
    s = s * x2 - 1.0 / 5040.0
    s = s * x2 + 1.0 / 120.0
    s = s * x2 - 1.0 / 6.0
    s = (s * x2) * x + x
    c = 1.0 / 479001600.0
    c = c * x2 - 1.0 / 3628800.0
    c = c * x2 + 1.0 / 40320.0
    c = c * x2 - 1.0 / 720.0
    c = c * x2 + 1.0 / 24.0
    c = c * x2 - 0.5
    c = c * x2 + 1.0
    s2 = s + s
    return 1.0 - s2 * s, s2 * c


def sincos_turns(turns):
    return double_angle((turns - jnp.round(turns)) * math.pi)


def direction(polar, azimuth):
    cos_p, sin_p = double_angle(0.25 * polar)
    cos_a, sin_a = double_angle(0.5 * azimuth)
    return cos_p * cos_a, cos_p * sin_a, sin_p


def weights_kernel(live, corner, cell, angles, raw, out, centre, lis, geo, lisb, *, sizes, counts):
    slots, bp = cell.shape
    tiles = lis.shape[1]
    span = tiles * 128 // CHUNKS
    cells = cell[...].astype(jnp.float32)
    along_x = jnp.floor((cells + 0.5) * (1.0 / (sizes[1] * sizes[2])))
    rest = cells - along_x * float(sizes[1] * sizes[2])
    along_y = jnp.floor((rest + 0.5) * (1.0 / sizes[2]))
    along_z = rest - along_y * float(sizes[2])
    for k, along in enumerate((along_x, along_y, along_z)):
        place = ((along + corner[k].astype(jnp.float32)) + 0.5) / float(counts[k])
        geo[k] = place
        mean = jnp.sum(place, axis=1, keepdims=True) * (1.0 / bp)
        centre[k] = jnp.broadcast_to(mean, (slots, 128))
    shown = lax.broadcasted_iota(jnp.int32, (slots, bp), 0) < live[0]
    for k, part in enumerate(direction(angles[0], angles[1])):
        geo[3 + k] = jnp.where(shown, part * (0.25 / math.pi), 0.0)
    for k, part in enumerate(direction(raw[0], raw[1])):
        lis[k] = 0.5 + raw[2] * part
    for k in range(3):
        for t in range(tiles):
            row = lis[k, t : t + 1, :]
            lisb[k, t * 128 : (t + 1) * 128, :] = jnp.transpose(jnp.broadcast_to(row, (128, 128)))

    def block(b, _):
        px, py, pz, nx, ny, nz = [geo[k, pl.ds(b, 1), :] for k in range(6)]
        for q in range(CHUNKS):
            for r in range(0, span, 16):
                at = q * span + r
                ox = lisb[0, at : at + 16, :] - px
                oy = lisb[1, at : at + 16, :] - py
                oz = lisb[2, at : at + 16, :] - pz
                d2 = ox * ox + oy * oy + oz * oz
                facing = nx * ox + ny * oy + nz * oz
                row = pl.multiple_of(q * slots * span + b * span + r, 16)
                out[pl.ds(row, 16), :] = (facing * (1.0 / d2)).astype(jnp.bfloat16)
        return 0

    lax.fori_loop(0, (live[0] + BATCH - 1) // BATCH * BATCH, block, 0)


def weights(live, corner, cell, angles, raw, sizes, counts):
    slots, bp = cell.shape
    obs = raw.shape[1] * 128
    vm = pl.BlockSpec(memory_space=pltpu.VMEM)
    sm = pl.BlockSpec(memory_space=pltpu.SMEM)
    return pl.pallas_call(
        functools.partial(weights_kernel, sizes=sizes, counts=counts),
        out_shape=[
            jax.ShapeDtypeStruct((slots * obs, bp), jnp.bfloat16),
            jax.ShapeDtypeStruct((3, slots, 128), jnp.float32),
            jax.ShapeDtypeStruct(raw.shape, jnp.float32),
        ],
        in_specs=[sm, sm, vm, vm, vm],
        out_specs=[vm] * 3,
        scratch_shapes=[pltpu.VMEM((6, slots, bp), jnp.float32), pltpu.VMEM((3, obs, 128), jnp.float32)],
        name="weights",
        compiler_params=pltpu.CompilerParams(vmem_limit_bytes=4 * 1024 * 1024),
    )(live, corner, cell, angles, raw)


def spectra_kernel(live, dens, rec, cell, table, sp, dens3, onehot, src):
    slots, bp = cell.shape
    rows = dens.shape[0] // 2
    total = (live[0] + BATCH - 1) // BATCH
    span = BATCH * bp

    for h in range(2):
        d = dens[pl.ds(h, rows, stride=2), :]
        hi = d.astype(jnp.bfloat16)
        left = d - hi.astype(jnp.float32)
        mid = left.astype(jnp.bfloat16)
        lo = (left - mid.astype(jnp.float32)).astype(jnp.bfloat16)
        for k, part in enumerate((hi, mid, lo)):
            dens3[k, :, h * 128 : (h + 1) * 128] = part
    lane = lax.broadcasted_iota(jnp.int32, (bp, 128), 1).astype(jnp.float32)

    def group(g, _):
        lows = []
        for j in range(BATCH):
            cells = cell[pl.ds(g * BATCH + j, 1), :].astype(jnp.float32)
            col = jnp.transpose(jnp.broadcast_to(cells, (128, 128)))
            high = jnp.floor(col * (1.0 / 256.0))
            low = col - 256.0 * high
            lows.append(low)
            for h in range(rows // 128):
                hit = jnp.where(high == lane + float(128 * h), 1.0, 0.0).astype(jnp.bfloat16)
                onehot[j * bp : (j + 1) * bp, h * 128 : (h + 1) * 128] = hit
        hot = onehot[...]
        picked = jnp.dot(hot, dens3[0], preferred_element_type=jnp.float32)
        picked = picked + jnp.dot(hot, dens3[1], preferred_element_type=jnp.float32)
        picked = picked + jnp.dot(hot, dens3[2], preferred_element_type=jnp.float32)
        for j in range(BATCH):
            own = picked[j * bp : (j + 1) * bp, :]
            found = jnp.where(lows[j] == lane, own[:, 0:128], 0.0) + jnp.where(lows[j] == lane + 128.0, own[:, 128:256], 0.0)
            sampled = jnp.sum(found, axis=1, keepdims=True)
            record = rec[pl.ds(pl.multiple_of(g * span + j * bp, bp), bp), :].astype(jnp.float32)
            src[j * bp : (j + 1) * bp, :] = (record * sampled).astype(jnp.bfloat16)
        for j in range(0, BATCH, 2):
            both = lax.dot_general(table[...], src[j * bp : (j + 2) * bp, :], NT, preferred_element_type=jnp.float32)
            both = both.astype(jnp.bfloat16)
            sp[g * BATCH + j] = both[:, 0:bp]
            sp[g * BATCH + j + 1] = both[:, bp : 2 * bp]
        return 0

    lax.fori_loop(0, total, group, 0)


def spectra(live, dens, rec, cell, table):
    rows = dens.shape[0]
    slots, bp = cell.shape
    samples = rec.shape[1]
    k2 = table.shape[0]
    vm = pl.BlockSpec(memory_space=pltpu.VMEM)
    return pl.pallas_call(
        spectra_kernel,
        out_shape=jax.ShapeDtypeStruct((slots, k2, bp), jnp.bfloat16),
        in_specs=[
            pl.BlockSpec(memory_space=pltpu.SMEM),
            vm,
            vm,
            vm,
            vm,
        ],
        out_specs=vm,
        scratch_shapes=[
            pltpu.VMEM((3, rows // 2, 256), jnp.bfloat16),
            pltpu.VMEM((BATCH * bp, rows // 2), jnp.bfloat16),
            pltpu.VMEM((BATCH * bp, samples), jnp.bfloat16),
        ],
        name="spectra",
        compiler_params=pltpu.CompilerParams(vmem_limit_bytes=3 * 1024 * 1024),
    )(live, dens, rec, cell, table)


def observe_kernel(live, centre, sp, wts, lis, *refs, chunk, part, parts, ties):
    slots, k2, bp = sp.shape
    tiles = lis.shape[1] // CHUNKS
    half = k2 // 2
    span = tiles * 128
    before, refs = (refs[0], refs[1 + ties :]) if part > 0 else (None, refs[ties:])
    out, prod, acc = refs if part == parts - 1 else (None, refs[1], refs[0])
    total = (live[0] + BATCH - 1) // BATCH
    turns = (total - part + parts - 1) // parts
    if before is None:
        acc[...] = jnp.zeros(acc.shape, jnp.float32)
    else:
        acc[...] = before[...]
    orders = lax.broadcasted_iota(jnp.int32, (8, 128), 0).astype(jnp.float32) + 1.0
    orders = orders * (WAVE_STEP / (2.0 * math.pi))

    def group(turn, _):
        g = turn * parts + part
        for pair in range(0, BATCH, 2):
            for j in range(2):
                b = g * BATCH + pair + j
                held = wts[pl.ds(pl.multiple_of(chunk * slots * span + b * span, span), span), :]
                prod[pair + j] = lax.dot_general(sp[b], held, NT, preferred_element_type=jnp.float32)
            for t in range(tiles):
                state = []
                for j in range(2):
                    b = g * BATCH + pair + j
                    u = chunk * tiles + t
                    away = [jnp.broadcast_to(lis[k, u : u + 1, :] - centre[k, pl.ds(b, 1), :], (8, 128)) for k in range(3)]
                    reach = jnp.sqrt(away[0] * away[0] + away[1] * away[1] + away[2] * away[2])
                    c, s = sincos_turns(reach * orders)
                    ec = jnp.broadcast_to(c[7:8, :], (8, 128))
                    es = jnp.broadcast_to(s[7:8, :], (8, 128))
                    state.append([c, s, ec * c - es * s, es * c + ec * s, ec + ec])
                for a in range(half // 8):
                    re_sum = acc[0, a * 8 : a * 8 + 8, t * 128 : t * 128 + 128]
                    im_sum = acc[1, a * 8 : a * 8 + 8, t * 128 : t * 128 + 128]
                    for j in range(2):
                        c, s, c_next, s_next, twice = state[j]
                        re = prod[pair + j, a * 8 : a * 8 + 8, t * 128 : t * 128 + 128]
                        im = prod[pair + j, half + a * 8 : half + a * 8 + 8, t * 128 : t * 128 + 128]
                        re_sum = re_sum + (re * c + im * s)
                        im_sum = im_sum + (im * c - re * s)
                        state[j] = [c_next, s_next, twice * c_next - c, twice * s_next - s, twice]
                    acc[0, a * 8 : a * 8 + 8, t * 128 : t * 128 + 128] = re_sum
                    acc[1, a * 8 : a * 8 + 8, t * 128 : t * 128 + 128] = im_sum
        return 0

    lax.fori_loop(0, turns, group, 0)
    if out is None:
        return
    shares, _, per, _ = out.shape
    each = 128 // per
    for k in range(2):
        for t in range(tiles):
            turned = jnp.transpose(acc[k, :, t * 128 : (t + 1) * 128])
            for e in range(each):
                out[t * each + e, k, :, :] = turned[e * per : (e + 1) * per, :]


def observe(chunk, part, parts, live, centre, sp, wts, lis, shares, before=None, ties=()):
    slots, k2, bp = sp.shape
    span = lis.shape[1] * 128 // CHUNKS
    vm = pl.BlockSpec(memory_space=pltpu.VMEM)
    sm = pl.BlockSpec(memory_space=pltpu.SMEM)
    sums = (2, k2 // 2, span)
    last = part == parts - 1
    scratch = [pltpu.VMEM((BATCH, k2, span), jnp.float32)]
    return pl.pallas_call(
        functools.partial(observe_kernel, chunk=chunk, part=part, parts=parts, ties=len(ties)),
        out_shape=jax.ShapeDtypeStruct((shares, 2, span // shares, k2 // 2) if last else sums, jnp.float32),
        in_specs=[sm, vm, vm, vm, vm] + [vm] * (part > 0) + [pl.BlockSpec(memory_space=pl.ANY)] * len(ties),
        out_specs=vm,
        scratch_shapes=scratch + [pltpu.VMEM(sums, jnp.float32)] * last,
        name="observe",
        cost_estimate=pl.CostEstimate(flops=4_000_000_000, transcendentals=0, bytes_accessed=1_000_000),
        compiler_params=pltpu.CompilerParams(vmem_limit_bytes=4 * 1024 * 1024),
    )(live, centre, sp, wts, lis, *([before] if part > 0 else []), *ties)


def swap(value, axis, bit):
    size = lax.axis_size(axis)
    return lax.ppermute(value, axis, [(i, i ^ bit) for i in range(size)])


def stages():
    def bits(axis):
        return [1 << k for k in range(lax.axis_size(axis).bit_length() - 1)]

    steps = [("halve", axis, bit) for axis in ("gz", "gx") for bit in bits(axis)]
    steps += [("sum", "gy", bit) for bit in bits("gy")]
    return steps + [("gather", "gx", bit) for bit in bits("gx")[::-1]]


def exchange(value, kind, axis, bit):
    if kind == "sum":
        return value + swap(value, axis, bit)
    up = (lax.axis_index(axis) // bit) % 2
    if kind == "gather":
        theirs = swap(value, axis, bit)
        first = jnp.where(up == 0, value, theirs)
        return jnp.concatenate([first, jnp.where(up == 0, theirs, value)], axis=2)
    if axis == "gz":
        pairs, dim = value.reshape((value.shape[0] // 2, 2) + value.shape[1:]), 1
    else:
        pairs, dim = value.reshape(value.shape[:2] + (2, value.shape[2] // 2) + value.shape[3:]), 2
    mine = lax.dynamic_index_in_dim(pairs, up, dim, keepdims=False)
    theirs = lax.dynamic_index_in_dim(pairs, 1 - up, dim, keepdims=False)
    return mine + swap(theirs, axis, bit)


def local(
    state_old,
    state_section,
    panel_record,
    panel_cell,
    panel_angles,
    owned_blocks,
    listener_angles,
    listener_range,
):
    sizes = state_section.shape[1:]
    axes = ("gx", "gy", "gz")
    counts = tuple(n * lax.axis_size(axis) for n, axis in zip(sizes, axes))
    step_size = COURANT / max(counts)
    slot_count, block_rows = panel_cell.shape
    samples = panel_record.shape[1]
    shares = lax.axis_size("gz")
    corner = jnp.stack([lax.axis_index(axis) * n for n, axis in zip(sizes, axes)]).astype(jnp.int32)
    raw = jnp.concatenate([listener_angles, listener_range[None]], axis=0)
    raw = jnp.transpose(raw.reshape(3, shares, CHUNKS, -1), (0, 2, 1, 3)).reshape(3, -1, 128)
    angles = panel_angles.reshape(2, slot_count, block_rows)
    wts, centres, listeners = weights(owned_blocks, corner, panel_cell, angles, raw, sizes, counts)
    updated, density = flow(state_old, state_section, counts, step_size)
    heard = spectra(owned_blocks, density, panel_record, panel_cell, dft_table(samples, FREQS))
    steps = stages()
    known = (owned_blocks, centres, heard, wts, listeners, shares)
    pieces, done = [], []
    for q in range(CHUNKS):
        parts = 1 if q == 0 else PARTS
        sums = None
        for part in range(parts):
            ties = []
            if part > 0:
                for k in range(len(pieces)):
                    if done[k] < len(steps):
                        pieces[k] = exchange(pieces[k], *steps[done[k]])
                        done[k] += 1
                        ties.append(pieces[k])
            sums = observe(q, part, parts, *known, sums, ties)
        pieces.append(sums)
        done.append(0)
    while min(done) < len(steps):
        for k in range(len(pieces)):
            if done[k] < len(steps):
                pieces[k] = exchange(pieces[k], *steps[done[k]])
                done[k] += 1
    pieces = [v.reshape((2, -1, FREQS)) for v in pieces]
    return (updated, jnp.concatenate(pieces, axis=1))


def solution(mesh):
    return jax.shard_map(
        local,
        mesh=mesh,
        in_specs=(
            P(None, "gx", "gy", "gz"),
            P(None, "gx", "gy", "gz"),
            P(("gx", "gy", "gz"), None),
            P(("gx", "gy", "gz"), None),
            P(None, ("gx", "gy", "gz")),
            P(("gx", "gy", "gz")),
            P(),
            P(),
        ),
        out_specs=(P(None, "gx", "gy", "gz"), P(None, "gz", None)),
        check_vma=False,
    )
```

```python
import functools
import math

import jax
import jax.numpy as jnp
import numpy as np
from jax import lax
from jax.experimental import pallas as pl
from jax.experimental.pallas import tpu as pltpu
from jax.sharding import PartitionSpec as P

FREQS = 128
BATCH = 4
CHUNKS = 2
PARTS = 3
NT = (((1,), (1,)), ((), ()))


GAMMA_GAS = 4.4
PRESSURE_INF = 1.0
WENO_EPS = 1e-06
WAVE_STEP = 0.25
COURANT = 0.08


def pack_kernel(state, turned, zlo, zhi, ylo, yhi, xends, *, cx, cy, cz):
    plane = cx * cy
    groups = plane // 128
    for c in range(5):
        for g in range(groups):
            row = c * plane + g * 128
            turned[row : row + cz, :] = jnp.transpose(state[row : row + 128, :])
        for k in range(3):
            ylo[(c * 3 + k) * cx : (c * 3 + k + 1) * cx, :] = state[pl.ds(c * plane + k, cx, stride=cy), :]
            yhi[(c * 3 + k) * cx : (c * 3 + k + 1) * cx, :] = state[pl.ds(c * plane + cy - 3 + k, cx, stride=cy), :]
            zlo[(c * 3 + k) * groups : (c * 3 + k + 1) * groups, :] = turned[pl.ds(c * plane + k, groups, stride=128), :]
            zhi[(c * 3 + k) * groups : (c * 3 + k + 1) * groups, :] = turned[pl.ds(c * plane + cz - 3 + k, groups, stride=128), :]
        xends[c * 3 * cy : (c + 1) * 3 * cy, :] = state[c * plane : c * plane + 3 * cy, :]
        xends[(5 + c) * 3 * cy : (6 + c) * 3 * cy, :] = state[c * plane + (cx - 3) * cy : (c + 1) * plane, :]


def pack(state, cx, cy, cz):
    groups = cx * cy // 128
    rows = [state.shape[0]] + [15 * groups] * 2 + [15 * cx] * 2 + [30 * cy]
    vm = pl.BlockSpec(memory_space=pltpu.VMEM)
    return pl.pallas_call(
        functools.partial(pack_kernel, cx=cx, cy=cy, cz=cz),
        out_shape=[jax.ShapeDtypeStruct((r, 128), jnp.float32) for r in rows],
        in_specs=[vm],
        out_specs=[vm] * 6,
        name="pack",
        compiler_params=pltpu.CompilerParams(vmem_limit_bytes=2 * 1024 * 1024),
    )(state)


def weno_shift(d1, d2, d3, d4):
    a0, a1, a2 = d2 - d1, d3 - d2, d4 - d3
    h2, h3 = 0.75 * d2, 0.75 * d3
    eps = 3.0 * WENO_EPS
    e0 = (a0 * a0 + eps) + h2 * (d2 + a0)
    e1 = (a1 * a1 + eps) + h2 * d3
    e2 = (a2 * a2 + eps) + h3 * (d3 - a2)
    t1 = e1 * e1
    u0 = 3.0 * (e0 * e0)
    u2 = 2.0 * (e2 * e2)
    w0, w1, w2 = t1 * u2, u0 * u2, u0 * t1
    below = 0.5 * w0 + (w1 + w2)
    above = w0 * (a1 - a0) + w2 * (a2 - a1)
    return (d2 + (d3 + d3)) - above * (1.0 / below)


def line_kernel_body(cells, flux, speed, wave, emit, *, n, width, axis):
    length = n + 6
    tiles = width // 8
    span = length * width

    def fluxes(p, _):
        for w in range(tiles):
            at = pl.multiple_of(p * width + w * 8, 8)
            rho = cells[pl.ds(at, 8), :]
            m = [cells[pl.ds((1 + k) * span + at, 8), :] for k in range(3)]
            energy = cells[pl.ds(4 * span + at, 8), :]
            inv = 1.0 / rho
            u = m[axis] * inv
            twice = (m[0] * m[0] + m[1] * m[1] + m[2] * m[2]) * inv
            pressure = (GAMMA_GAS - 1.0) * (energy - 0.5 * twice) - GAMMA_GAS * PRESSURE_INF
            sound = jnp.sqrt(GAMMA_GAS * (pressure + PRESSURE_INF) * inv)
            speed[pl.ds(at, 8), :] = jnp.abs(u) + sound
            flux[pl.ds(at, 8), :] = m[axis]
            for k in range(3):
                carried = m[k] * u
                if k == axis:
                    carried = carried + pressure
                flux[pl.ds((1 + k) * span + at, 8), :] = carried
            flux[pl.ds(4 * span + at, 8), :] = (energy + pressure) * u
        return 0

    lax.fori_loop(0, length, fluxes, 0, unroll=5 if tiles == 1 else 2)

    def waves(i, _):
        for w in range(tiles):
            at = pl.multiple_of(i * width + w * 8, 8)
            top = speed[pl.ds(at, 8), :]
            for k in range(1, 6):
                top = jnp.maximum(top, speed[pl.ds(at + k * width, 8), :])
            wave[pl.ds(at, 8), :] = top
        return 0

    lax.fori_loop(0, n + 1, waves, 0, unroll={1: 5, 2: 3}.get(tiles, 1))

    def line(index, _):
        c = index // tiles
        w = index % tiles

        def load(ref, p):
            return ref[pl.ds(pl.multiple_of(c * span + p * width + w * 8, 8), 8), :]

        q = [load(cells, p) for p in range(5)]
        f = [load(flux, p) for p in range(5)]
        dq = [q[k + 1] - q[k] for k in range(4)]
        df = [f[k + 1] - f[k] for k in range(4)]
        q_last, f_last, f_mid, f_near = q[4], f[4], f[2], f[3]
        before = None
        for i in range(n + 1):
            q_new, f_new = load(cells, i + 5), load(flux, i + 5)
            dq.append(q_new - q_last)
            df.append(f_new - f_last)
            alpha = wave[pl.ds(pl.multiple_of(i * width + w * 8, 8), 8), :]
            drift = [alpha * v for v in dq]
            up = weno_shift(*[df[k] + drift[k] for k in range(4)])
            down = weno_shift(*[drift[k] - df[k] for k in (4, 3, 2, 1)])
            here = 6.0 * ((f_mid + f_near) - drift[2]) + (up + down)
            if before is not None:
                emit(c, w, i - 1, here - before)
            before = here
            dq, df = dq[1:], df[1:]
            f_mid, f_near = f_near, f_last
            q_last, f_last = q_new, f_new
        return 0

    lax.fori_loop(0, 5 * tiles, line, 0)


def z_kernel(turned, left, right, out, cells, flux, speed, wave, part, *, cx, cy, cz, scale):
    plane = cx * cy
    groups = plane // 128
    width = 2 * groups
    n = cz // 2
    length = n + 6
    for c in range(5):
        base = c * length * width
        for p in range(3):
            cells[pl.ds(base + p * width, groups, stride=2), :] = left[(c * 3 + p) * groups : (c * 3 + p + 1) * groups, :]
            cells[pl.ds(base + p * width + 1, groups, stride=2), :] = turned[pl.ds(c * plane + n - 3 + p, groups, stride=128), :]
            q = n + 3 + p
            cells[pl.ds(base + q * width, groups, stride=2), :] = turned[pl.ds(c * plane + n + p, groups, stride=128), :]
            cells[pl.ds(base + q * width + 1, groups, stride=2), :] = right[(c * 3 + p) * groups : (c * 3 + p + 1) * groups, :]
        for p in range(n):
            cells[base + (p + 3) * width : base + (p + 4) * width, :] = turned[pl.ds(c * plane + p, width, stride=n), :]

    def emit(c, w, i, value):
        part[pl.ds(c * plane + i, width, stride=n), :] = value * scale

    line_kernel_body(cells, flux, speed, wave, emit, n=n, width=width, axis=2)
    for c in range(5):
        for g in range(groups):
            row = c * plane + g * 128
            out[row : row + 128, :] = jnp.transpose(part[row : row + cz, :])


def y_kernel(state, left, right, start, out, cells, flux, speed, wave, *, cx, cy, scale):
    plane = cx * cy
    length = cy + 6
    for c in range(5):
        base = c * length * cx
        cells[base : base + 3 * cx, :] = left[c * 3 * cx : (c + 1) * 3 * cx, :]
        cells[base + (cy + 3) * cx : base + length * cx, :] = right[c * 3 * cx : (c + 1) * 3 * cx, :]
        for p in range(cy):
            for x in range(0, cx, 8):
                cells[base + (p + 3) * cx + x : base + (p + 3) * cx + x + 8, :] = state[pl.ds(c * plane + x * cy + p, 8, stride=cy), :]

    def emit(c, w, i, value):
        rows = pl.ds(c * plane + w * 8 * cy + i, 8, stride=cy)
        out[rows, :] = start[rows, :] + value * scale

    line_kernel_body(cells, flux, speed, wave, emit, n=cy, width=cx, axis=1)


def x_kernel(state, ends, start, old, out, density, cells, flux, speed, wave, *, cx, cy, scale):
    plane = cx * cy
    length = cx + 6
    for c in range(5):
        base = c * length * cy
        cells[base : base + 3 * cy, :] = ends[(5 + c) * 3 * cy : (6 + c) * 3 * cy, :]
        cells[base + 3 * cy : base + (cx + 3) * cy, :] = state[c * plane : (c + 1) * plane, :]
        cells[base + (cx + 3) * cy : base + length * cy, :] = ends[c * 3 * cy : (c + 1) * 3 * cy, :]

    def emit(c, w, i, value):
        rows = pl.ds(pl.multiple_of(c * plane + i * cy + w * 8, 8), 8)
        change = start[rows, :] + value * scale
        out[rows, :] = (0.75 * old[rows, :] + 0.25 * state[rows, :]) - change

    line_kernel_body(cells, flux, speed, wave, emit, n=cx, width=cy, axis=0)
    density[...] = out[0:plane, :]


def line_call(kernel, operands, n, width, name, more=(), results=()):
    length = n + 6
    vm = pl.BlockSpec(memory_space=pltpu.VMEM)
    return pl.pallas_call(
        kernel,
        out_shape=[jax.ShapeDtypeStruct(shape, jnp.float32) for shape in (operands[0].shape, *results)],
        in_specs=[vm] * len(operands),
        out_specs=[vm] * (1 + len(results)),
        scratch_shapes=[
            pltpu.VMEM((5 * length * width, 128), jnp.float32),
            pltpu.VMEM((5 * length * width, 128), jnp.float32),
            pltpu.VMEM((length * width, 128), jnp.float32),
            pltpu.VMEM((length * width, 128), jnp.float32),
        ]
        + list(more),
        name=name,
        compiler_params=pltpu.CompilerParams(vmem_limit_bytes=6 * 1024 * 1024),
    )(*operands)


def neighbours(first, last, axis):
    size = lax.axis_size(axis)
    up = [(i, (i + 1) % size) for i in range(size)]
    down = [(j, i) for i, j in up]
    return lax.ppermute(last, axis, up), lax.ppermute(first, axis, down)


def flow(state_old, state_section, counts, step_size):
    shape = state_section.shape
    cx, cy, cz = shape[1:]
    state = state_section.reshape(-1, cz)
    turned, zlo, zhi, ylo, yhi, xends = pack(state, cx, cy, cz)
    if lax.axis_size("gx") == 2:
        ends = swap(xends, "gx", 1)
    else:
        ends = jnp.concatenate(neighbours(xends[: xends.shape[0] // 2], xends[xends.shape[0] // 2 :], "gx")[::-1])
    zl, zr = neighbours(zlo, zhi, "gz")
    yl, yr = neighbours(ylo, yhi, "gy")
    scales = [0.25 * step_size * n / 12.0 for n in counts]
    plane = cx * cy
    (part,) = line_call(
        functools.partial(z_kernel, cx=cx, cy=cy, cz=cz, scale=scales[2]),
        (turned, zl, zr), cz // 2, plane // 64, "along_z",
        (pltpu.VMEM((5 * plane, 128), jnp.float32),),
    )
    (part,) = line_call(functools.partial(y_kernel, cx=cx, cy=cy, scale=scales[1]), (state, yl, yr, part), cy, cx, "along_y")
    updated, density = line_call(
        functools.partial(x_kernel, cx=cx, cy=cy, scale=scales[0]),
        (state, ends, part, state_old.reshape(-1, cz)), cx, cy, "along_x", (), ((plane, cz),),
    )
    return updated.reshape(shape), density


def dft_table(sample_count, freq_count):
    times = np.arange(sample_count, dtype=np.int64)[None, :]
    orders = np.arange(1, freq_count + 1, dtype=np.int64)[:, None]
    phases = (np.float32(2.0 * math.pi / sample_count) * (times * orders % sample_count).astype(np.float32)).astype(np.float64)
    scaling = 1.0 / math.sqrt(sample_count)
    both = np.concatenate([np.cos(phases), -np.sin(phases)], axis=0).astype(np.float32) * np.float32(scaling)
    return jnp.asarray(both, jnp.bfloat16)


def double_angle(x):
    x2 = x * x
    s = 1.0 / 6227020800.0
    s = s * x2 - 1.0 / 39916800.0
    s = s * x2 + 1.0 / 362880.0
    s = s * x2 - 1.0 / 5040.0
    s = s * x2 + 1.0 / 120.0
    s = s * x2 - 1.0 / 6.0
    s = (s * x2) * x + x
    c = 1.0 / 479001600.0
    c = c * x2 - 1.0 / 3628800.0
    c = c * x2 + 1.0 / 40320.0
    c = c * x2 - 1.0 / 720.0
    c = c * x2 + 1.0 / 24.0
    c = c * x2 - 0.5
    c = c * x2 + 1.0
    s2 = s + s
    return 1.0 - s2 * s, s2 * c


def sincos_turns(turns):
    return double_angle((turns - jnp.round(turns)) * math.pi)


def direction(polar, azimuth):
    cos_p, sin_p = double_angle(0.25 * polar)
    cos_a, sin_a = double_angle(0.5 * azimuth)
    return cos_p * cos_a, cos_p * sin_a, sin_p


def three(value):
    high = value.astype(jnp.bfloat16).astype(jnp.float32)
    middle = (value - high).astype(jnp.bfloat16).astype(jnp.float32)
    return high, middle, ((value - high) - middle).astype(jnp.bfloat16).astype(jnp.float32)


def weights_kernel(
    live, corner, cell, angles, raw, out, centre, lis, geo, lisb, pan, row_side, sides, col_side, cols, *, sizes, counts
):
    slots, bp = cell.shape
    tiles = lis.shape[1]
    span = tiles * 128 // CHUNKS
    cells = cell[...].astype(jnp.float32)
    along_x = jnp.floor((cells + 0.5) * (1.0 / (sizes[1] * sizes[2])))
    rest = cells - along_x * float(sizes[1] * sizes[2])
    along_y = jnp.floor((rest + 0.5) * (1.0 / sizes[2]))
    along_z = rest - along_y * float(sizes[2])
    offsets = []
    for k, along in enumerate((along_x, along_y, along_z)):
        place = ((along + corner[k].astype(jnp.float32)) + 0.5) / float(counts[k])
        mean = jnp.sum(place, axis=1, keepdims=True) * (1.0 / bp)
        centre[k] = jnp.broadcast_to(mean, (slots, 128))
        offsets.append(place - 0.5)
    shown = lax.broadcasted_iota(jnp.int32, (slots, bp), 0) < live[0]
    along_normal = 0.0
    for k, part in enumerate(direction(angles[0], angles[1])):
        geo[k] = jnp.where(shown, part * (0.25 / math.pi), 0.0)
        along_normal = along_normal + geo[k] * offsets[k]
    geo[3] = along_normal
    shifts = []
    for k, part in enumerate(direction(raw[0], raw[1])):
        shift = raw[2] * part
        lis[k] = 0.5 + shift
        shifts.append(shift)
        for t in range(tiles):
            lisb[k, t * 128 : (t + 1) * 128, :] = jnp.transpose(jnp.broadcast_to(shift[t : t + 1, :], (128, 128)))
    one = jnp.ones((tiles, 128), jnp.float32)
    left, right = [], []
    for k in range(3):
        for n, part in enumerate(three(-2.0 * offsets[k])):
            pan[3 * k + n] = part
        high, middle, low = three(shifts[k])
        left += [high, high, high, middle, middle, low]
        right += [3 * k, 3 * k + 1, 3 * k + 2, 3 * k, 3 * k + 1, 3 * k]
    for n, part in enumerate(three(offsets[0] * offsets[0] + offsets[1] * offsets[1] + offsets[2] * offsets[2])):
        pan[9 + n] = part
    pan[12] = jnp.ones((slots, bp), jnp.float32)
    left += [*three(shifts[0] * shifts[0] + shifts[1] * shifts[1] + shifts[2] * shifts[2]), one, one, one]
    right += [12, 12, 12, 9, 10, 11]
    row_side[...] = jnp.zeros(row_side.shape, jnp.float32)
    col_side[...] = jnp.zeros(col_side.shape, jnp.float32)
    cols[...] = jnp.zeros(cols.shape, jnp.bfloat16)
    for n, part in enumerate(left):
        for t in range(tiles):
            row_side[n : n + 1, t * 128 : (t + 1) * 128] = part[t : t + 1, :]
    for t in range(tiles):
        sides[t * 128 : (t + 1) * 128, :] = jnp.transpose(row_side[:, t * 128 : (t + 1) * 128]).astype(jnp.bfloat16)

    def pair(turn, _):
        first = turn * 2
        for j in range(2):
            for n, source in enumerate(right):
                col_side[n : n + 1, j * bp : (j + 1) * bp] = pan[source, pl.ds(first + j, 1), :]
        cols[0:32, :] = col_side[...].astype(jnp.bfloat16)
        parts = [[geo[k, pl.ds(first + j, 1), :] for k in range(4)] for j in range(2)]
        for q in range(CHUNKS):
            for r in range(0, span, 128):
                at = q * span + r
                d2 = jnp.dot(sides[at : at + 128, :], cols[...], preferred_element_type=jnp.float32)
                for w in range(0, 128, 16):
                    lx, ly, lz = [lisb[k, at + w : at + w + 16, :] for k in range(3)]
                    for j in range(2):
                        nx, ny, nz, shift = parts[j]
                        facing = (nx * lx + ny * ly) + (nz * lz - shift)
                        row = pl.multiple_of(q * slots * span + (first + j) * span + r + w, 16)
                        value = facing * (1.0 / d2[w : w + 16, j * bp : (j + 1) * bp])
                        out[pl.ds(row, 16), :] = value.astype(jnp.bfloat16)
        return 0

    lax.fori_loop(0, (live[0] + BATCH - 1) // BATCH * (BATCH // 2), pair, 0)


def weights(live, corner, cell, angles, raw, sizes, counts):
    slots, bp = cell.shape
    obs = raw.shape[1] * 128
    vm = pl.BlockSpec(memory_space=pltpu.VMEM)
    sm = pl.BlockSpec(memory_space=pltpu.SMEM)
    return pl.pallas_call(
        functools.partial(weights_kernel, sizes=sizes, counts=counts),
        out_shape=[
            jax.ShapeDtypeStruct((slots * obs, bp), jnp.bfloat16),
            jax.ShapeDtypeStruct((3, slots, 128), jnp.float32),
            jax.ShapeDtypeStruct(raw.shape, jnp.float32),
        ],
        in_specs=[sm, sm, vm, vm, vm],
        out_specs=[vm] * 3,
        scratch_shapes=[
            pltpu.VMEM((4, slots, bp), jnp.float32),
            pltpu.VMEM((3, obs, 128), jnp.float32),
            pltpu.VMEM((13, slots, bp), jnp.float32),
            pltpu.VMEM((128, obs), jnp.float32),
            pltpu.VMEM((obs, 128), jnp.bfloat16),
            pltpu.VMEM((32, 2 * bp), jnp.float32),
            pltpu.VMEM((128, 2 * bp), jnp.bfloat16),
        ],
        name="weights",
        compiler_params=pltpu.CompilerParams(vmem_limit_bytes=4 * 1024 * 1024),
    )(live, corner, cell, angles, raw)


def spectra_kernel(live, dens, rec, cell, table, sp, dens3, onehot, src):
    slots, bp = cell.shape
    rows = dens.shape[0] // 2
    total = (live[0] + BATCH - 1) // BATCH
    span = BATCH * bp

    for h in range(2):
        d = dens[pl.ds(h, rows, stride=2), :]
        hi = d.astype(jnp.bfloat16)
        left = d - hi.astype(jnp.float32)
        mid = left.astype(jnp.bfloat16)
        lo = (left - mid.astype(jnp.float32)).astype(jnp.bfloat16)
        for k, part in enumerate((hi, mid, lo)):
            dens3[k, :, h * 128 : (h + 1) * 128] = part
    lane = lax.broadcasted_iota(jnp.int32, (bp, 128), 1).astype(jnp.float32)

    def group(g, _):
        lows = []
        for j in range(BATCH):
            cells = cell[pl.ds(g * BATCH + j, 1), :].astype(jnp.float32)
            col = jnp.transpose(jnp.broadcast_to(cells, (128, 128)))
            high = jnp.floor(col * (1.0 / 256.0))
            low = col - 256.0 * high
            lows.append(low)
            for h in range(rows // 128):
                hit = jnp.where(high == lane + float(128 * h), 1.0, 0.0).astype(jnp.bfloat16)
                onehot[j * bp : (j + 1) * bp, h * 128 : (h + 1) * 128] = hit
        hot = onehot[...]
        picked = jnp.dot(hot, dens3[0], preferred_element_type=jnp.float32)
        picked = picked + jnp.dot(hot, dens3[1], preferred_element_type=jnp.float32)
        picked = picked + jnp.dot(hot, dens3[2], preferred_element_type=jnp.float32)
        for j in range(BATCH):
            own = picked[j * bp : (j + 1) * bp, :]
            found = jnp.where(lows[j] == lane, own[:, 0:128], 0.0) + jnp.where(lows[j] == lane + 128.0, own[:, 128:256], 0.0)
            sampled = jnp.sum(found, axis=1, keepdims=True)
            record = rec[pl.ds(pl.multiple_of(g * span + j * bp, bp), bp), :].astype(jnp.float32)
            src[j * bp : (j + 1) * bp, :] = (record * sampled).astype(jnp.bfloat16)
        for j in range(0, BATCH, 2):
            both = lax.dot_general(table[...], src[j * bp : (j + 2) * bp, :], NT, preferred_element_type=jnp.float32)
            both = both.astype(jnp.bfloat16)
            sp[g * BATCH + j] = both[:, 0:bp]
            sp[g * BATCH + j + 1] = both[:, bp : 2 * bp]
        return 0

    lax.fori_loop(0, total, group, 0)


def spectra(live, dens, rec, cell, table):
    rows = dens.shape[0]
    slots, bp = cell.shape
    samples = rec.shape[1]
    k2 = table.shape[0]
    vm = pl.BlockSpec(memory_space=pltpu.VMEM)
    return pl.pallas_call(
        spectra_kernel,
        out_shape=jax.ShapeDtypeStruct((slots, k2, bp), jnp.bfloat16),
        in_specs=[
            pl.BlockSpec(memory_space=pltpu.SMEM),
            vm,
            vm,
            vm,
            vm,
        ],
        out_specs=vm,
        scratch_shapes=[
            pltpu.VMEM((3, rows // 2, 256), jnp.bfloat16),
            pltpu.VMEM((BATCH * bp, rows // 2), jnp.bfloat16),
            pltpu.VMEM((BATCH * bp, samples), jnp.bfloat16),
        ],
        name="spectra",
        compiler_params=pltpu.CompilerParams(vmem_limit_bytes=3 * 1024 * 1024),
    )(live, dens, rec, cell, table)


def observe_kernel(live, centre, sp, wts, lis, *refs, chunk, part, parts, ties):
    slots, k2, bp = sp.shape
    tiles = lis.shape[1] // CHUNKS
    half = k2 // 2
    span = tiles * 128
    before, refs = (refs[0], refs[1 + ties :]) if part > 0 else (None, refs[ties:])
    out, prod, acc = refs if part == parts - 1 else (None, refs[1], refs[0])
    total = (live[0] + BATCH - 1) // BATCH
    turns = (total - part + parts - 1) // parts
    if before is None:
        acc[...] = jnp.zeros(acc.shape, jnp.float32)
    else:
        acc[...] = before[...]
    orders = lax.broadcasted_iota(jnp.int32, (8, 128), 0).astype(jnp.float32) + 1.0
    orders = orders * (WAVE_STEP / (2.0 * math.pi))

    def group(turn, _):
        g = turn * parts + part
        for h, pair in [(h, pair) for h in range(0, span, 256) for pair in range(0, BATCH, 2)]:
            for j in range(2):
                b = g * BATCH + pair + j
                held = wts[pl.ds(pl.multiple_of(chunk * slots * span + b * span + h, 256), 256), :]
                prod[pair + j, :, h : h + 256] = lax.dot_general(sp[b], held, NT, preferred_element_type=jnp.float32)
            for t in range(h // 128, h // 128 + 2):
                state = []
                for j in range(2):
                    b = g * BATCH + pair + j
                    u = chunk * tiles + t
                    away = [jnp.broadcast_to(lis[k, u : u + 1, :] - centre[k, pl.ds(b, 1), :], (8, 128)) for k in range(3)]
                    reach = jnp.sqrt(away[0] * away[0] + away[1] * away[1] + away[2] * away[2])
                    c, s = sincos_turns(reach * orders)
                    ec = jnp.broadcast_to(c[7:8, :], (8, 128))
                    es = jnp.broadcast_to(s[7:8, :], (8, 128))
                    state.append([c, s, ec * c - es * s, es * c + ec * s, ec + ec])
                for a in range(half // 8):
                    re_sum = acc[0, a * 8 : a * 8 + 8, t * 128 : t * 128 + 128]
                    im_sum = acc[1, a * 8 : a * 8 + 8, t * 128 : t * 128 + 128]
                    for j in range(2):
                        c, s, c_next, s_next, twice = state[j]
                        re = prod[pair + j, a * 8 : a * 8 + 8, t * 128 : t * 128 + 128]
                        im = prod[pair + j, half + a * 8 : half + a * 8 + 8, t * 128 : t * 128 + 128]
                        re_sum = re_sum + (re * c + im * s)
                        im_sum = im_sum + (im * c - re * s)
                        state[j] = [c_next, s_next, twice * c_next - c, twice * s_next - s, twice]
                    acc[0, a * 8 : a * 8 + 8, t * 128 : t * 128 + 128] = re_sum
                    acc[1, a * 8 : a * 8 + 8, t * 128 : t * 128 + 128] = im_sum
        return 0

    lax.fori_loop(0, turns, group, 0)
    if out is None:
        return
    shares, _, per, _ = out.shape
    each = 128 // per
    for k in range(2):
        for t in range(tiles):
            turned = jnp.transpose(acc[k, :, t * 128 : (t + 1) * 128])
            for e in range(each):
                out[t * each + e, k, :, :] = turned[e * per : (e + 1) * per, :]


def observe(chunk, part, parts, live, centre, sp, wts, lis, shares, before=None, ties=()):
    slots, k2, bp = sp.shape
    span = lis.shape[1] * 128 // CHUNKS
    vm = pl.BlockSpec(memory_space=pltpu.VMEM)
    sm = pl.BlockSpec(memory_space=pltpu.SMEM)
    sums = (2, k2 // 2, span)
    last = part == parts - 1
    scratch = [pltpu.VMEM((BATCH, k2, span), jnp.float32)]
    return pl.pallas_call(
        functools.partial(observe_kernel, chunk=chunk, part=part, parts=parts, ties=len(ties)),
        out_shape=jax.ShapeDtypeStruct((shares, 2, span // shares, k2 // 2) if last else sums, jnp.float32),
        in_specs=[sm, vm, vm, vm, vm] + [vm] * (part > 0) + [pl.BlockSpec(memory_space=pl.ANY)] * len(ties),
        out_specs=vm,
        scratch_shapes=scratch + [pltpu.VMEM(sums, jnp.float32)] * last,
        name="observe",
        cost_estimate=pl.CostEstimate(flops=4_000_000_000, transcendentals=0, bytes_accessed=1_000_000),
        compiler_params=pltpu.CompilerParams(vmem_limit_bytes=4 * 1024 * 1024),
    )(live, centre, sp, wts, lis, *([before] if part > 0 else []), *ties)


def swap(value, axis, bit):
    size = lax.axis_size(axis)
    return lax.ppermute(value, axis, [(i, i ^ bit) for i in range(size)])


def stages():
    def bits(axis):
        return [1 << k for k in range(lax.axis_size(axis).bit_length() - 1)]

    steps = [("halve", axis, bit) for axis in ("gz", "gx") for bit in bits(axis)]
    steps += [("sum", "gy", bit) for bit in bits("gy")]
    return steps + [("gather", "gx", bit) for bit in bits("gx")[::-1]]


def exchange(value, kind, axis, bit):
    if kind == "sum":
        return value + swap(value, axis, bit)
    up = (lax.axis_index(axis) // bit) % 2
    if kind == "gather":
        theirs = swap(value, axis, bit)
        first = jnp.where(up == 0, value, theirs)
        return jnp.concatenate([first, jnp.where(up == 0, theirs, value)], axis=2)
    if axis == "gz":
        pairs, dim = value.reshape((value.shape[0] // 2, 2) + value.shape[1:]), 1
    else:
        pairs, dim = value.reshape(value.shape[:2] + (2, value.shape[2] // 2) + value.shape[3:]), 2
    mine = lax.dynamic_index_in_dim(pairs, up, dim, keepdims=False)
    theirs = lax.dynamic_index_in_dim(pairs, 1 - up, dim, keepdims=False)
    return mine + swap(theirs, axis, bit)


def local(
    state_old,
    state_section,
    panel_record,
    panel_cell,
    panel_angles,
    owned_blocks,
    listener_angles,
    listener_range,
):
    sizes = state_section.shape[1:]
    axes = ("gx", "gy", "gz")
    counts = tuple(n * lax.axis_size(axis) for n, axis in zip(sizes, axes))
    step_size = COURANT / max(counts)
    slot_count, block_rows = panel_cell.shape
    samples = panel_record.shape[1]
    shares = lax.axis_size("gz")
    corner = jnp.stack([lax.axis_index(axis) * n for n, axis in zip(sizes, axes)]).astype(jnp.int32)
    raw = jnp.concatenate([listener_angles, listener_range[None]], axis=0)
    raw = jnp.transpose(raw.reshape(3, shares, CHUNKS, -1), (0, 2, 1, 3)).reshape(3, -1, 128)
    angles = panel_angles.reshape(2, slot_count, block_rows)
    wts, centres, listeners = weights(owned_blocks, corner, panel_cell, angles, raw, sizes, counts)
    updated, density = flow(state_old, state_section, counts, step_size)
    heard = spectra(owned_blocks, density, panel_record, panel_cell, dft_table(samples, FREQS))
    steps = stages()
    known = (owned_blocks, centres, heard, wts, listeners, shares)
    pieces, done = [], []
    for q in range(CHUNKS):
        parts = 1 if q == 0 else PARTS
        sums = None
        for part in range(parts):
            ties = []
            if part > 0:
                for k in range(len(pieces)):
                    if done[k] < len(steps):
                        pieces[k] = exchange(pieces[k], *steps[done[k]])
                        done[k] += 1
                        ties.append(pieces[k])
            sums = observe(q, part, parts, *known, sums, ties)
        pieces.append(sums)
        done.append(0)
    while min(done) < len(steps):
        for k in range(len(pieces)):
            if done[k] < len(steps):
                pieces[k] = exchange(pieces[k], *steps[done[k]])
                done[k] += 1
    pieces = [v.reshape((2, -1, FREQS)) for v in pieces]
    return (updated, jnp.concatenate(pieces, axis=1))


def solution(mesh):
    return jax.shard_map(
        local,
        mesh=mesh,
        in_specs=(
            P(None, "gx", "gy", "gz"),
            P(None, "gx", "gy", "gz"),
            P(("gx", "gy", "gz"), None),
            P(("gx", "gy", "gz"), None),
            P(None, ("gx", "gy", "gz")),
            P(("gx", "gy", "gz")),
            P(),
            P(),
        ),
        out_specs=(P(None, "gx", "gy", "gz"), P(None, "gz", None)),
        check_vma=False,
    )
```

```python
import functools
import math

import jax
import jax.numpy as jnp
import numpy as np
from jax import lax
from jax.experimental import pallas as pl
from jax.experimental.pallas import tpu as pltpu
from jax.sharding import PartitionSpec as P

FREQS = 128
BATCH = 4
WIDE = 8
CHUNKS = 2
PARTS = 3
NT = (((1,), (1,)), ((), ()))


GAMMA_GAS = 4.4
PRESSURE_INF = 1.0
WENO_EPS = 1e-06
WAVE_STEP = 0.25
COURANT = 0.08


def pack_kernel(state, turned, zlo, zhi, ylo, yhi, xends, *, cx, cy, cz):
    plane = cx * cy
    groups = plane // 128
    for c in range(5):
        for g in range(groups):
            row = c * plane + g * 128
            turned[row : row + cz, :] = jnp.transpose(state[row : row + 128, :])
        for k in range(3):
            ylo[(c * 3 + k) * cx : (c * 3 + k + 1) * cx, :] = state[pl.ds(c * plane + k, cx, stride=cy), :]
            yhi[(c * 3 + k) * cx : (c * 3 + k + 1) * cx, :] = state[pl.ds(c * plane + cy - 3 + k, cx, stride=cy), :]
            zlo[(c * 3 + k) * groups : (c * 3 + k + 1) * groups, :] = turned[pl.ds(c * plane + k, groups, stride=128), :]
            zhi[(c * 3 + k) * groups : (c * 3 + k + 1) * groups, :] = turned[pl.ds(c * plane + cz - 3 + k, groups, stride=128), :]
        xends[c * 3 * cy : (c + 1) * 3 * cy, :] = state[c * plane : c * plane + 3 * cy, :]
        xends[(5 + c) * 3 * cy : (6 + c) * 3 * cy, :] = state[c * plane + (cx - 3) * cy : (c + 1) * plane, :]


def pack(state, cx, cy, cz):
    groups = cx * cy // 128
    rows = [state.shape[0]] + [15 * groups] * 2 + [15 * cx] * 2 + [30 * cy]
    vm = pl.BlockSpec(memory_space=pltpu.VMEM)
    return pl.pallas_call(
        functools.partial(pack_kernel, cx=cx, cy=cy, cz=cz),
        out_shape=[jax.ShapeDtypeStruct((r, 128), jnp.float32) for r in rows],
        in_specs=[vm],
        out_specs=[vm] * 6,
        name="pack",
        compiler_params=pltpu.CompilerParams(vmem_limit_bytes=2 * 1024 * 1024),
    )(state)


def weno_shift(d1, d2, d3, d4):
    a0, a1, a2 = d2 - d1, d3 - d2, d4 - d3
    h2, h3 = 0.75 * d2, 0.75 * d3
    eps = 3.0 * WENO_EPS
    e0 = (a0 * a0 + eps) + h2 * (d2 + a0)
    e1 = (a1 * a1 + eps) + h2 * d3
    e2 = (a2 * a2 + eps) + h3 * (d3 - a2)
    t1 = e1 * e1
    u0 = 3.0 * (e0 * e0)
    u2 = 2.0 * (e2 * e2)
    w0, w1, w2 = t1 * u2, u0 * u2, u0 * t1
    below = 0.5 * w0 + (w1 + w2)
    above = w0 * (a1 - a0) + w2 * (a2 - a1)
    return (d2 + (d3 + d3)) - above * (1.0 / below)


def line_kernel_body(cells, flux, speed, wave, emit, *, n, width, axis):
    length = n + 6
    tiles = width // 8
    span = length * width

    def fluxes(p, _):
        for w in range(tiles):
            at = pl.multiple_of(p * width + w * 8, 8)
            rho = cells[pl.ds(at, 8), :]
            m = [cells[pl.ds((1 + k) * span + at, 8), :] for k in range(3)]
            energy = cells[pl.ds(4 * span + at, 8), :]
            inv = 1.0 / rho
            u = m[axis] * inv
            twice = (m[0] * m[0] + m[1] * m[1] + m[2] * m[2]) * inv
            pressure = (GAMMA_GAS - 1.0) * (energy - 0.5 * twice) - GAMMA_GAS * PRESSURE_INF
            sound = jnp.sqrt(GAMMA_GAS * (pressure + PRESSURE_INF) * inv)
            speed[pl.ds(at, 8), :] = jnp.abs(u) + sound
            flux[pl.ds(at, 8), :] = m[axis]
            for k in range(3):
                carried = m[k] * u
                if k == axis:
                    carried = carried + pressure
                flux[pl.ds((1 + k) * span + at, 8), :] = carried
            flux[pl.ds(4 * span + at, 8), :] = (energy + pressure) * u
        return 0

    lax.fori_loop(0, length, fluxes, 0, unroll=5 if tiles == 1 else 2)

    def waves(i, _):
        for w in range(tiles):
            at = pl.multiple_of(i * width + w * 8, 8)
            top = speed[pl.ds(at, 8), :]
            for k in range(1, 6):
                top = jnp.maximum(top, speed[pl.ds(at + k * width, 8), :])
            wave[pl.ds(at, 8), :] = top
        return 0

    lax.fori_loop(0, n + 1, waves, 0, unroll={1: 5, 2: 3}.get(tiles, 1))

    def line(index, _):
        c = index // tiles
        w = index % tiles

        def load(ref, p):
            return ref[pl.ds(pl.multiple_of(c * span + p * width + w * 8, 8), 8), :]

        q = [load(cells, p) for p in range(5)]
        f = [load(flux, p) for p in range(5)]
        dq = [q[k + 1] - q[k] for k in range(4)]
        df = [f[k + 1] - f[k] for k in range(4)]
        q_last, f_last, f_mid, f_near = q[4], f[4], f[2], f[3]
        before = None
        for i in range(n + 1):
            q_new, f_new = load(cells, i + 5), load(flux, i + 5)
            dq.append(q_new - q_last)
            df.append(f_new - f_last)
            alpha = wave[pl.ds(pl.multiple_of(i * width + w * 8, 8), 8), :]
            drift = [alpha * v for v in dq]
            up = weno_shift(*[df[k] + drift[k] for k in range(4)])
            down = weno_shift(*[drift[k] - df[k] for k in (4, 3, 2, 1)])
            here = 6.0 * ((f_mid + f_near) - drift[2]) + (up + down)
            if before is not None:
                emit(c, w, i - 1, here - before)
            before = here
            dq, df = dq[1:], df[1:]
            f_mid, f_near = f_near, f_last
            q_last, f_last = q_new, f_new
        return 0

    lax.fori_loop(0, 5 * tiles, line, 0)


def z_kernel(turned, left, right, out, cells, flux, speed, wave, part, *, cx, cy, cz, scale):
    plane = cx * cy
    groups = plane // 128
    width = 2 * groups
    n = cz // 2
    length = n + 6
    for c in range(5):
        base = c * length * width
        for p in range(3):
            cells[pl.ds(base + p * width, groups, stride=2), :] = left[(c * 3 + p) * groups : (c * 3 + p + 1) * groups, :]
            cells[pl.ds(base + p * width + 1, groups, stride=2), :] = turned[pl.ds(c * plane + n - 3 + p, groups, stride=128), :]
            q = n + 3 + p
            cells[pl.ds(base + q * width, groups, stride=2), :] = turned[pl.ds(c * plane + n + p, groups, stride=128), :]
            cells[pl.ds(base + q * width + 1, groups, stride=2), :] = right[(c * 3 + p) * groups : (c * 3 + p + 1) * groups, :]
        for p in range(n):
            cells[base + (p + 3) * width : base + (p + 4) * width, :] = turned[pl.ds(c * plane + p, width, stride=n), :]

    def emit(c, w, i, value):
        part[pl.ds(c * plane + i, width, stride=n), :] = value * scale

    line_kernel_body(cells, flux, speed, wave, emit, n=n, width=width, axis=2)
    for c in range(5):
        for g in range(groups):
            row = c * plane + g * 128
            out[row : row + 128, :] = jnp.transpose(part[row : row + cz, :])


def y_kernel(state, left, right, start, out, cells, flux, speed, wave, *, cx, cy, scale):
    plane = cx * cy
    length = cy + 6
    for c in range(5):
        base = c * length * cx
        cells[base : base + 3 * cx, :] = left[c * 3 * cx : (c + 1) * 3 * cx, :]
        cells[base + (cy + 3) * cx : base + length * cx, :] = right[c * 3 * cx : (c + 1) * 3 * cx, :]
        for p in range(cy):
            for x in range(0, cx, 8):
                cells[base + (p + 3) * cx + x : base + (p + 3) * cx + x + 8, :] = state[pl.ds(c * plane + x * cy + p, 8, stride=cy), :]

    def emit(c, w, i, value):
        rows = pl.ds(c * plane + w * 8 * cy + i, 8, stride=cy)
        out[rows, :] = start[rows, :] + value * scale

    line_kernel_body(cells, flux, speed, wave, emit, n=cy, width=cx, axis=1)


def x_kernel(state, ends, start, old, out, density, cells, flux, speed, wave, *, cx, cy, scale):
    plane = cx * cy
    length = cx + 6
    for c in range(5):
        base = c * length * cy
        cells[base : base + 3 * cy, :] = ends[(5 + c) * 3 * cy : (6 + c) * 3 * cy, :]
        cells[base + 3 * cy : base + (cx + 3) * cy, :] = state[c * plane : (c + 1) * plane, :]
        cells[base + (cx + 3) * cy : base + length * cy, :] = ends[c * 3 * cy : (c + 1) * 3 * cy, :]

    def emit(c, w, i, value):
        rows = pl.ds(pl.multiple_of(c * plane + i * cy + w * 8, 8), 8)
        change = start[rows, :] + value * scale
        out[rows, :] = (0.75 * old[rows, :] + 0.25 * state[rows, :]) - change

    line_kernel_body(cells, flux, speed, wave, emit, n=cx, width=cy, axis=0)
    density[...] = out[0:plane, :]


def line_call(kernel, operands, n, width, name, more=(), results=()):
    length = n + 6
    vm = pl.BlockSpec(memory_space=pltpu.VMEM)
    return pl.pallas_call(
        kernel,
        out_shape=[jax.ShapeDtypeStruct(shape, jnp.float32) for shape in (operands[0].shape, *results)],
        in_specs=[vm] * len(operands),
        out_specs=[vm] * (1 + len(results)),
        scratch_shapes=[
            pltpu.VMEM((5 * length * width, 128), jnp.float32),
            pltpu.VMEM((5 * length * width, 128), jnp.float32),
            pltpu.VMEM((length * width, 128), jnp.float32),
            pltpu.VMEM((length * width, 128), jnp.float32),
        ]
        + list(more),
        name=name,
        compiler_params=pltpu.CompilerParams(vmem_limit_bytes=6 * 1024 * 1024),
    )(*operands)


def neighbours(first, last, axis):
    size = lax.axis_size(axis)
    up = [(i, (i + 1) % size) for i in range(size)]
    down = [(j, i) for i, j in up]
    return lax.ppermute(last, axis, up), lax.ppermute(first, axis, down)


def flow(state_old, state_section, counts, step_size):
    shape = state_section.shape
    cx, cy, cz = shape[1:]
    state = state_section.reshape(-1, cz)
    turned, zlo, zhi, ylo, yhi, xends = pack(state, cx, cy, cz)
    if lax.axis_size("gx") == 2:
        ends = swap(xends, "gx", 1)
    else:
        ends = jnp.concatenate(neighbours(xends[: xends.shape[0] // 2], xends[xends.shape[0] // 2 :], "gx")[::-1])
    zl, zr = neighbours(zlo, zhi, "gz")
    yl, yr = neighbours(ylo, yhi, "gy")
    scales = [0.25 * step_size * n / 12.0 for n in counts]
    plane = cx * cy
    (part,) = line_call(
        functools.partial(z_kernel, cx=cx, cy=cy, cz=cz, scale=scales[2]),
        (turned, zl, zr), cz // 2, plane // 64, "along_z",
        (pltpu.VMEM((5 * plane, 128), jnp.float32),),
    )
    (part,) = line_call(functools.partial(y_kernel, cx=cx, cy=cy, scale=scales[1]), (state, yl, yr, part), cy, cx, "along_y")
    updated, density = line_call(
        functools.partial(x_kernel, cx=cx, cy=cy, scale=scales[0]),
        (state, ends, part, state_old.reshape(-1, cz)), cx, cy, "along_x", (), ((plane, cz),),
    )
    return updated.reshape(shape), density


def dft_table(sample_count, freq_count):
    times = np.arange(sample_count, dtype=np.int64)[None, :]
    orders = np.arange(1, freq_count + 1, dtype=np.int64)[:, None]
    phases = (np.float32(2.0 * math.pi / sample_count) * (times * orders % sample_count).astype(np.float32)).astype(np.float64)
    scaling = 1.0 / math.sqrt(sample_count)
    both = np.concatenate([np.cos(phases), -np.sin(phases)], axis=0).astype(np.float32) * np.float32(scaling)
    return jnp.asarray(both, jnp.bfloat16)


def double_angle(x):
    x2 = x * x
    s = 1.0 / 6227020800.0
    s = s * x2 - 1.0 / 39916800.0
    s = s * x2 + 1.0 / 362880.0
    s = s * x2 - 1.0 / 5040.0
    s = s * x2 + 1.0 / 120.0
    s = s * x2 - 1.0 / 6.0
    s = (s * x2) * x + x
    c = 1.0 / 479001600.0
    c = c * x2 - 1.0 / 3628800.0
    c = c * x2 + 1.0 / 40320.0
    c = c * x2 - 1.0 / 720.0
    c = c * x2 + 1.0 / 24.0
    c = c * x2 - 0.5
    c = c * x2 + 1.0
    s2 = s + s
    return 1.0 - s2 * s, s2 * c


def sincos_turns(turns):
    return double_angle((turns - jnp.round(turns)) * math.pi)


def direction(polar, azimuth):
    cos_p, sin_p = double_angle(0.25 * polar)
    cos_a, sin_a = double_angle(0.5 * azimuth)
    return cos_p * cos_a, cos_p * sin_a, sin_p


def three(value):
    high = value.astype(jnp.bfloat16).astype(jnp.float32)
    middle = (value - high).astype(jnp.bfloat16).astype(jnp.float32)
    return high, middle, ((value - high) - middle).astype(jnp.bfloat16).astype(jnp.float32)


def weights_kernel(
    live, corner, cell, angles, raw, out, centre, lis, geo, lisb, pan, row_side, sides, col_side, cols, *, sizes, counts
):
    slots, bp = cell.shape
    tiles = lis.shape[1]
    span = tiles * 128 // CHUNKS
    cells = cell[...].astype(jnp.float32)
    along_x = jnp.floor((cells + 0.5) * (1.0 / (sizes[1] * sizes[2])))
    rest = cells - along_x * float(sizes[1] * sizes[2])
    along_y = jnp.floor((rest + 0.5) * (1.0 / sizes[2]))
    along_z = rest - along_y * float(sizes[2])
    offsets = []
    for k, along in enumerate((along_x, along_y, along_z)):
        place = ((along + corner[k].astype(jnp.float32)) + 0.5) / float(counts[k])
        mean = jnp.sum(place, axis=1, keepdims=True) * (1.0 / bp)
        centre[k] = jnp.broadcast_to(mean, (slots, 128))
        offsets.append(place - 0.5)
    shown = lax.broadcasted_iota(jnp.int32, (slots, bp), 0) < live[0]
    along_normal = 0.0
    for k, part in enumerate(direction(angles[0], angles[1])):
        geo[k] = jnp.where(shown, part * (0.25 / math.pi), 0.0)
        along_normal = along_normal + geo[k] * offsets[k]
    geo[3] = along_normal
    shifts = []
    for k, part in enumerate(direction(raw[0], raw[1])):
        shift = raw[2] * part
        lis[k] = 0.5 + shift
        shifts.append(shift)
        for t in range(tiles):
            lisb[k, t * 128 : (t + 1) * 128, :] = jnp.transpose(jnp.broadcast_to(shift[t : t + 1, :], (128, 128)))
    one = jnp.ones((tiles, 128), jnp.float32)
    left, right = [], []
    for k in range(3):
        for n, part in enumerate(three(-2.0 * offsets[k])):
            pan[3 * k + n] = part
        high, middle, low = three(shifts[k])
        left += [high, high, high, middle, middle, low]
        right += [3 * k, 3 * k + 1, 3 * k + 2, 3 * k, 3 * k + 1, 3 * k]
    for n, part in enumerate(three(offsets[0] * offsets[0] + offsets[1] * offsets[1] + offsets[2] * offsets[2])):
        pan[9 + n] = part
    pan[12] = jnp.ones((slots, bp), jnp.float32)
    left += [*three(shifts[0] * shifts[0] + shifts[1] * shifts[1] + shifts[2] * shifts[2]), one, one, one]
    right += [12, 12, 12, 9, 10, 11]
    row_side[...] = jnp.zeros(row_side.shape, jnp.float32)
    col_side[...] = jnp.zeros(col_side.shape, jnp.float32)
    cols[...] = jnp.zeros(cols.shape, jnp.bfloat16)
    for n, part in enumerate(left):
        for t in range(tiles):
            row_side[n : n + 1, t * 128 : (t + 1) * 128] = part[t : t + 1, :]
    for t in range(tiles):
        sides[t * 128 : (t + 1) * 128, :] = jnp.transpose(row_side[:, t * 128 : (t + 1) * 128]).astype(jnp.bfloat16)

    def pair(turn, _):
        first = turn * 2
        for j in range(2):
            for n, source in enumerate(right):
                col_side[n : n + 1, j * bp : (j + 1) * bp] = pan[source, pl.ds(first + j, 1), :]
        cols[0:32, :] = col_side[...].astype(jnp.bfloat16)
        parts = [[geo[k, pl.ds(first + j, 1), :] for k in range(4)] for j in range(2)]
        for q in range(CHUNKS):
            for r in range(0, span, 128):
                at = q * span + r
                d2 = jnp.dot(sides[at : at + 128, :], cols[...], preferred_element_type=jnp.float32)
                for w in range(0, 128, 16):
                    lx, ly, lz = [lisb[k, at + w : at + w + 16, :] for k in range(3)]
                    for j in range(2):
                        nx, ny, nz, shift = parts[j]
                        facing = (nx * lx + ny * ly) + (nz * lz - shift)
                        row = pl.multiple_of(q * slots * span + (first + j) * span + r + w, 16)
                        value = facing * (1.0 / d2[w : w + 16, j * bp : (j + 1) * bp])
                        out[pl.ds(row, 16), :] = value.astype(jnp.bfloat16)
        return 0

    lax.fori_loop(0, (live[0] + BATCH - 1) // BATCH * (BATCH // 2), pair, 0)


def weights(live, corner, cell, angles, raw, sizes, counts):
    slots, bp = cell.shape
    obs = raw.shape[1] * 128
    vm = pl.BlockSpec(memory_space=pltpu.VMEM)
    sm = pl.BlockSpec(memory_space=pltpu.SMEM)
    return pl.pallas_call(
        functools.partial(weights_kernel, sizes=sizes, counts=counts),
        out_shape=[
            jax.ShapeDtypeStruct((slots * obs, bp), jnp.bfloat16),
            jax.ShapeDtypeStruct((3, slots, 128), jnp.float32),
            jax.ShapeDtypeStruct(raw.shape, jnp.float32),
        ],
        in_specs=[sm, sm, vm, vm, vm],
        out_specs=[vm] * 3,
        scratch_shapes=[
            pltpu.VMEM((4, slots, bp), jnp.float32),
            pltpu.VMEM((3, obs, 128), jnp.float32),
            pltpu.VMEM((13, slots, bp), jnp.float32),
            pltpu.VMEM((128, obs), jnp.float32),
            pltpu.VMEM((obs, 128), jnp.bfloat16),
            pltpu.VMEM((32, 2 * bp), jnp.float32),
            pltpu.VMEM((128, 2 * bp), jnp.bfloat16),
        ],
        name="weights",
        compiler_params=pltpu.CompilerParams(vmem_limit_bytes=4 * 1024 * 1024),
    )(live, corner, cell, angles, raw)


def spectra_kernel(live, dens, rec, cell, table, sp, dens3, onehot, src):
    slots, bp = cell.shape
    rows = dens.shape[0] // 2
    total = (live[0] + WIDE - 1) // WIDE
    span = WIDE * bp

    for h in range(2):
        d = dens[pl.ds(h, rows, stride=2), :]
        hi = d.astype(jnp.bfloat16)
        left = d - hi.astype(jnp.float32)
        mid = left.astype(jnp.bfloat16)
        lo = (left - mid.astype(jnp.float32)).astype(jnp.bfloat16)
        for k, part in enumerate((hi, mid, lo)):
            dens3[k, :, h * 128 : (h + 1) * 128] = part
    lane = lax.broadcasted_iota(jnp.int32, (bp, 128), 1).astype(jnp.float32)

    def group(g, _):
        lows = []
        for j in range(WIDE):
            cells = cell[pl.ds(g * WIDE + j, 1), :].astype(jnp.float32)
            col = jnp.transpose(jnp.broadcast_to(cells, (128, 128)))
            high = jnp.floor(col * (1.0 / 256.0))
            low = col - 256.0 * high
            lows.append(low)
            for h in range(rows // 128):
                hit = jnp.where(high == lane + float(128 * h), 1.0, 0.0).astype(jnp.bfloat16)
                onehot[j * bp : (j + 1) * bp, h * 128 : (h + 1) * 128] = hit
        for j in range(WIDE):
            if j % 2 == 0:
                hot = onehot[j * bp : (j + 2) * bp, :]
                picked = jnp.dot(hot, dens3[0], preferred_element_type=jnp.float32)
                picked = picked + jnp.dot(hot, dens3[1], preferred_element_type=jnp.float32)
                picked = picked + jnp.dot(hot, dens3[2], preferred_element_type=jnp.float32)
            own = picked[j % 2 * bp : (j % 2 + 1) * bp, :]
            found = jnp.where(lows[j] == lane, own[:, 0:128], 0.0) + jnp.where(lows[j] == lane + 128.0, own[:, 128:256], 0.0)
            sampled = jnp.sum(found, axis=1, keepdims=True)
            record = rec[pl.ds(pl.multiple_of(g * span + j * bp, bp), bp), :].astype(jnp.float32)
            src[j * bp : (j + 1) * bp, :] = (record * sampled).astype(jnp.bfloat16)
        for j in range(0, WIDE, 2):
            both = lax.dot_general(table[...], src[j * bp : (j + 2) * bp, :], NT, preferred_element_type=jnp.float32)
            both = both.astype(jnp.bfloat16)
            sp[g * WIDE + j] = both[:, 0:bp]
            sp[g * WIDE + j + 1] = both[:, bp : 2 * bp]
        return 0

    lax.fori_loop(0, total, group, 0)


def spectra(live, dens, rec, cell, table):
    rows = dens.shape[0]
    slots, bp = cell.shape
    samples = rec.shape[1]
    k2 = table.shape[0]
    vm = pl.BlockSpec(memory_space=pltpu.VMEM)
    return pl.pallas_call(
        spectra_kernel,
        out_shape=jax.ShapeDtypeStruct((slots, k2, bp), jnp.bfloat16),
        in_specs=[
            pl.BlockSpec(memory_space=pltpu.SMEM),
            vm,
            vm,
            vm,
            vm,
        ],
        out_specs=vm,
        scratch_shapes=[
            pltpu.VMEM((3, rows // 2, 256), jnp.bfloat16),
            pltpu.VMEM((WIDE * bp, rows // 2), jnp.bfloat16),
            pltpu.VMEM((WIDE * bp, samples), jnp.bfloat16),
        ],
        name="spectra",
        compiler_params=pltpu.CompilerParams(vmem_limit_bytes=7 * 1024 * 1024),
    )(live, dens, rec, cell, table)


def observe_kernel(live, centre, sp, wts, lis, *refs, chunk, part, parts, ties):
    slots, k2, bp = sp.shape
    tiles = lis.shape[1] // CHUNKS
    half = k2 // 2
    span = tiles * 128
    before, refs = (refs[0], refs[1 + ties :]) if part > 0 else (None, refs[ties:])
    out, prod, acc = refs if part == parts - 1 else (None, refs[1], refs[0])
    total = (live[0] + BATCH - 1) // BATCH
    turns = (total - part + parts - 1) // parts
    if before is None:
        acc[...] = jnp.zeros(acc.shape, jnp.float32)
    else:
        acc[...] = before[...]
    orders = lax.broadcasted_iota(jnp.int32, (8, 128), 0).astype(jnp.float32) + 1.0
    orders = orders * (WAVE_STEP / (2.0 * math.pi))

    def group(turn, _):
        g = turn * parts + part
        for h, pair in [(h, pair) for h in range(0, span, 256) for pair in range(0, BATCH, 2)]:
            for j in range(2):
                b = g * BATCH + pair + j
                held = wts[pl.ds(pl.multiple_of(chunk * slots * span + b * span + h, 256), 256), :]
                prod[pair + j, :, h : h + 256] = lax.dot_general(sp[b], held, NT, preferred_element_type=jnp.float32)
            for t in range(h // 128, h // 128 + 2):
                state = []
                for j in range(2):
                    b = g * BATCH + pair + j
                    u = chunk * tiles + t
                    away = [jnp.broadcast_to(lis[k, u : u + 1, :] - centre[k, pl.ds(b, 1), :], (8, 128)) for k in range(3)]
                    reach = jnp.sqrt(away[0] * away[0] + away[1] * away[1] + away[2] * away[2])
                    c, s = sincos_turns(reach * orders)
                    ec = jnp.broadcast_to(c[7:8, :], (8, 128))
                    es = jnp.broadcast_to(s[7:8, :], (8, 128))
                    state.append([c, s, ec * c - es * s, es * c + ec * s, ec + ec])
                for a in range(half // 8):
                    re_sum = acc[0, a * 8 : a * 8 + 8, t * 128 : t * 128 + 128]
                    im_sum = acc[1, a * 8 : a * 8 + 8, t * 128 : t * 128 + 128]
                    for j in range(2):
                        c, s, c_next, s_next, twice = state[j]
                        re = prod[pair + j, a * 8 : a * 8 + 8, t * 128 : t * 128 + 128]
                        im = prod[pair + j, half + a * 8 : half + a * 8 + 8, t * 128 : t * 128 + 128]
                        re_sum = re_sum + (re * c + im * s)
                        im_sum = im_sum + (im * c - re * s)
                        state[j] = [c_next, s_next, twice * c_next - c, twice * s_next - s, twice]
                    acc[0, a * 8 : a * 8 + 8, t * 128 : t * 128 + 128] = re_sum
                    acc[1, a * 8 : a * 8 + 8, t * 128 : t * 128 + 128] = im_sum
        return 0

    lax.fori_loop(0, turns, group, 0)
    if out is None:
        return
    shares, _, per, _ = out.shape
    each = 128 // per
    for k in range(2):
        for t in range(tiles):
            turned = jnp.transpose(acc[k, :, t * 128 : (t + 1) * 128])
            for e in range(each):
                out[t * each + e, k, :, :] = turned[e * per : (e + 1) * per, :]


def observe(chunk, part, parts, live, centre, sp, wts, lis, shares, before=None, ties=()):
    slots, k2, bp = sp.shape
    span = lis.shape[1] * 128 // CHUNKS
    vm = pl.BlockSpec(memory_space=pltpu.VMEM)
    sm = pl.BlockSpec(memory_space=pltpu.SMEM)
    sums = (2, k2 // 2, span)
    last = part == parts - 1
    scratch = [pltpu.VMEM((BATCH, k2, span), jnp.float32)]
    return pl.pallas_call(
        functools.partial(observe_kernel, chunk=chunk, part=part, parts=parts, ties=len(ties)),
        out_shape=jax.ShapeDtypeStruct((shares, 2, span // shares, k2 // 2) if last else sums, jnp.float32),
        in_specs=[sm, vm, vm, vm, vm] + [vm] * (part > 0) + [pl.BlockSpec(memory_space=pl.ANY)] * len(ties),
        out_specs=vm,
        scratch_shapes=scratch + [pltpu.VMEM(sums, jnp.float32)] * last,
        name="observe",
        cost_estimate=pl.CostEstimate(flops=4_000_000_000, transcendentals=0, bytes_accessed=1_000_000),
        compiler_params=pltpu.CompilerParams(vmem_limit_bytes=4 * 1024 * 1024),
    )(live, centre, sp, wts, lis, *([before] if part > 0 else []), *ties)


def swap(value, axis, bit):
    size = lax.axis_size(axis)
    return lax.ppermute(value, axis, [(i, i ^ bit) for i in range(size)])


def stages():
    def bits(axis):
        return [1 << k for k in range(lax.axis_size(axis).bit_length() - 1)]

    steps = [("halve", axis, bit) for axis in ("gz", "gx") for bit in bits(axis)]
    steps += [("sum", "gy", bit) for bit in bits("gy")]
    return steps + [("gather", "gx", bit) for bit in bits("gx")[::-1]]


def exchange(value, kind, axis, bit):
    if kind == "sum":
        return value + swap(value, axis, bit)
    up = (lax.axis_index(axis) // bit) % 2
    if kind == "gather":
        theirs = swap(value, axis, bit)
        first = jnp.where(up == 0, value, theirs)
        return jnp.concatenate([first, jnp.where(up == 0, theirs, value)], axis=2)
    if axis == "gz":
        pairs, dim = value.reshape((value.shape[0] // 2, 2) + value.shape[1:]), 1
    else:
        pairs, dim = value.reshape(value.shape[:2] + (2, value.shape[2] // 2) + value.shape[3:]), 2
    mine = lax.dynamic_index_in_dim(pairs, up, dim, keepdims=False)
    theirs = lax.dynamic_index_in_dim(pairs, 1 - up, dim, keepdims=False)
    return mine + swap(theirs, axis, bit)


def local(
    state_old,
    state_section,
    panel_record,
    panel_cell,
    panel_angles,
    owned_blocks,
    listener_angles,
    listener_range,
):
    sizes = state_section.shape[1:]
    axes = ("gx", "gy", "gz")
    counts = tuple(n * lax.axis_size(axis) for n, axis in zip(sizes, axes))
    step_size = COURANT / max(counts)
    slot_count, block_rows = panel_cell.shape
    samples = panel_record.shape[1]
    shares = lax.axis_size("gz")
    corner = jnp.stack([lax.axis_index(axis) * n for n, axis in zip(sizes, axes)]).astype(jnp.int32)
    raw = jnp.concatenate([listener_angles, listener_range[None]], axis=0)
    raw = jnp.transpose(raw.reshape(3, shares, CHUNKS, -1), (0, 2, 1, 3)).reshape(3, -1, 128)
    angles = panel_angles.reshape(2, slot_count, block_rows)
    wts, centres, listeners = weights(owned_blocks, corner, panel_cell, angles, raw, sizes, counts)
    updated, density = flow(state_old, state_section, counts, step_size)
    heard = spectra(owned_blocks, density, panel_record, panel_cell, dft_table(samples, FREQS))
    steps = stages()
    known = (owned_blocks, centres, heard, wts, listeners, shares)
    pieces, done = [], []
    for q in range(CHUNKS):
        parts = 1 if q == 0 else PARTS
        sums = None
        for part in range(parts):
            ties = []
            if part > 0:
                for k in range(len(pieces)):
                    if done[k] < len(steps):
                        pieces[k] = exchange(pieces[k], *steps[done[k]])
                        done[k] += 1
                        ties.append(pieces[k])
            sums = observe(q, part, parts, *known, sums, ties)
        pieces.append(sums)
        done.append(0)
    while min(done) < len(steps):
        for k in range(len(pieces)):
            if done[k] < len(steps):
                pieces[k] = exchange(pieces[k], *steps[done[k]])
                done[k] += 1
    pieces = [v.reshape((2, -1, FREQS)) for v in pieces]
    return (updated, jnp.concatenate(pieces, axis=1))


def solution(mesh):
    return jax.shard_map(
        local,
        mesh=mesh,
        in_specs=(
            P(None, "gx", "gy", "gz"),
            P(None, "gx", "gy", "gz"),
            P(("gx", "gy", "gz"), None),
            P(("gx", "gy", "gz"), None),
            P(None, ("gx", "gy", "gz")),
            P(("gx", "gy", "gz")),
            P(),
            P(),
        ),
        out_specs=(P(None, "gx", "gy", "gz"), P(None, "gz", None)),
        check_vma=False,
    )
```

```python
import functools
import math

import jax
import jax.numpy as jnp
import numpy as np
from jax import lax
from jax.experimental import pallas as pl
from jax.experimental.pallas import tpu as pltpu
from jax.sharding import PartitionSpec as P

FREQS = 128
BATCH = 4
WIDE = 8
CHUNKS = 2
PARTS = 2
NT = (((1,), (1,)), ((), ()))


GAMMA_GAS = 4.4
PRESSURE_INF = 1.0
WENO_EPS = 1e-06
WAVE_STEP = 0.25
COURANT = 0.08


def pack_kernel(state, turned, zlo, zhi, ylo, yhi, xends, *, cx, cy, cz):
    plane = cx * cy
    groups = plane // 128
    for c in range(5):
        for g in range(groups):
            row = c * plane + g * 128
            turned[row : row + cz, :] = jnp.transpose(state[row : row + 128, :])
        for k in range(3):
            ylo[(c * 3 + k) * cx : (c * 3 + k + 1) * cx, :] = state[pl.ds(c * plane + k, cx, stride=cy), :]
            yhi[(c * 3 + k) * cx : (c * 3 + k + 1) * cx, :] = state[pl.ds(c * plane + cy - 3 + k, cx, stride=cy), :]
            zlo[(c * 3 + k) * groups : (c * 3 + k + 1) * groups, :] = turned[pl.ds(c * plane + k, groups, stride=128), :]
            zhi[(c * 3 + k) * groups : (c * 3 + k + 1) * groups, :] = turned[pl.ds(c * plane + cz - 3 + k, groups, stride=128), :]
        xends[c * 3 * cy : (c + 1) * 3 * cy, :] = state[c * plane : c * plane + 3 * cy, :]
        xends[(5 + c) * 3 * cy : (6 + c) * 3 * cy, :] = state[c * plane + (cx - 3) * cy : (c + 1) * plane, :]


def pack(state, cx, cy, cz):
    groups = cx * cy // 128
    rows = [state.shape[0]] + [15 * groups] * 2 + [15 * cx] * 2 + [30 * cy]
    vm = pl.BlockSpec(memory_space=pltpu.VMEM)
    return pl.pallas_call(
        functools.partial(pack_kernel, cx=cx, cy=cy, cz=cz),
        out_shape=[jax.ShapeDtypeStruct((r, 128), jnp.float32) for r in rows],
        in_specs=[vm],
        out_specs=[vm] * 6,
        name="pack",
        compiler_params=pltpu.CompilerParams(vmem_limit_bytes=2 * 1024 * 1024),
    )(state)


def weno_shift(d1, d2, d3, d4):
    a0, a1, a2 = d2 - d1, d3 - d2, d4 - d3
    h2, h3 = 0.75 * d2, 0.75 * d3
    eps = 3.0 * WENO_EPS
    e0 = (a0 * a0 + eps) + h2 * (d2 + a0)
    e1 = (a1 * a1 + eps) + h2 * d3
    e2 = (a2 * a2 + eps) + h3 * (d3 - a2)
    t1 = e1 * e1
    u0 = 3.0 * (e0 * e0)
    u2 = 2.0 * (e2 * e2)
    w0, w1, w2 = t1 * u2, u0 * u2, u0 * t1
    below = 0.5 * w0 + (w1 + w2)
    above = w0 * (a1 - a0) + w2 * (a2 - a1)
    return (d2 + (d3 + d3)) - above * (1.0 / below)


def line_kernel_body(cells, flux, speed, wave, emit, *, n, width, axis):
    length = n + 6
    tiles = width // 8
    span = length * width

    def fluxes(p, _):
        for w in range(tiles):
            at = pl.multiple_of(p * width + w * 8, 8)
            rho = cells[pl.ds(at, 8), :]
            m = [cells[pl.ds((1 + k) * span + at, 8), :] for k in range(3)]
            energy = cells[pl.ds(4 * span + at, 8), :]
            inv = 1.0 / rho
            u = m[axis] * inv
            twice = (m[0] * m[0] + m[1] * m[1] + m[2] * m[2]) * inv
            pressure = (GAMMA_GAS - 1.0) * (energy - 0.5 * twice) - GAMMA_GAS * PRESSURE_INF
            sound = jnp.sqrt(GAMMA_GAS * (pressure + PRESSURE_INF) * inv)
            speed[pl.ds(at, 8), :] = jnp.abs(u) + sound
            flux[pl.ds(at, 8), :] = m[axis]
            for k in range(3):
                carried = m[k] * u
                if k == axis:
                    carried = carried + pressure
                flux[pl.ds((1 + k) * span + at, 8), :] = carried
            flux[pl.ds(4 * span + at, 8), :] = (energy + pressure) * u
        return 0

    lax.fori_loop(0, length, fluxes, 0, unroll=5 if tiles == 1 else 2)

    def waves(i, _):
        for w in range(tiles):
            at = pl.multiple_of(i * width + w * 8, 8)
            top = speed[pl.ds(at, 8), :]
            for k in range(1, 6):
                top = jnp.maximum(top, speed[pl.ds(at + k * width, 8), :])
            wave[pl.ds(at, 8), :] = top
        return 0

    lax.fori_loop(0, n + 1, waves, 0, unroll={1: 5, 2: 3}.get(tiles, 1))

    def line(index, _):
        c = index // tiles
        w = index % tiles

        def load(ref, p):
            return ref[pl.ds(pl.multiple_of(c * span + p * width + w * 8, 8), 8), :]

        q = [load(cells, p) for p in range(5)]
        f = [load(flux, p) for p in range(5)]
        dq = [q[k + 1] - q[k] for k in range(4)]
        df = [f[k + 1] - f[k] for k in range(4)]
        q_last, f_last, f_mid, f_near = q[4], f[4], f[2], f[3]
        before = None
        for i in range(n + 1):
            q_new, f_new = load(cells, i + 5), load(flux, i + 5)
            dq.append(q_new - q_last)
            df.append(f_new - f_last)
            alpha = wave[pl.ds(pl.multiple_of(i * width + w * 8, 8), 8), :]
            drift = [alpha * v for v in dq]
            up = weno_shift(*[df[k] + drift[k] for k in range(4)])
            down = weno_shift(*[drift[k] - df[k] for k in (4, 3, 2, 1)])
            here = 6.0 * ((f_mid + f_near) - drift[2]) + (up + down)
            if before is not None:
                emit(c, w, i - 1, here - before)
            before = here
            dq, df = dq[1:], df[1:]
            f_mid, f_near = f_near, f_last
            q_last, f_last = q_new, f_new
        return 0

    lax.fori_loop(0, 5 * tiles, line, 0)


def z_kernel(turned, left, right, out, cells, flux, speed, wave, part, *, cx, cy, cz, scale):
    plane = cx * cy
    groups = plane // 128
    width = 2 * groups
    n = cz // 2
    length = n + 6
    for c in range(5):
        base = c * length * width
        for p in range(3):
            cells[pl.ds(base + p * width, groups, stride=2), :] = left[(c * 3 + p) * groups : (c * 3 + p + 1) * groups, :]
            cells[pl.ds(base + p * width + 1, groups, stride=2), :] = turned[pl.ds(c * plane + n - 3 + p, groups, stride=128), :]
            q = n + 3 + p
            cells[pl.ds(base + q * width, groups, stride=2), :] = turned[pl.ds(c * plane + n + p, groups, stride=128), :]
            cells[pl.ds(base + q * width + 1, groups, stride=2), :] = right[(c * 3 + p) * groups : (c * 3 + p + 1) * groups, :]
        for p in range(n):
            cells[base + (p + 3) * width : base + (p + 4) * width, :] = turned[pl.ds(c * plane + p, width, stride=n), :]

    def emit(c, w, i, value):
        part[pl.ds(c * plane + i, width, stride=n), :] = value * scale

    line_kernel_body(cells, flux, speed, wave, emit, n=n, width=width, axis=2)
    for c in range(5):
        for g in range(groups):
            row = c * plane + g * 128
            out[row : row + 128, :] = jnp.transpose(part[row : row + cz, :])


def y_kernel(state, left, right, start, out, cells, flux, speed, wave, *, cx, cy, scale):
    plane = cx * cy
    length = cy + 6
    for c in range(5):
        base = c * length * cx
        cells[base : base + 3 * cx, :] = left[c * 3 * cx : (c + 1) * 3 * cx, :]
        cells[base + (cy + 3) * cx : base + length * cx, :] = right[c * 3 * cx : (c + 1) * 3 * cx, :]
        for p in range(cy):
            for x in range(0, cx, 8):
                cells[base + (p + 3) * cx + x : base + (p + 3) * cx + x + 8, :] = state[pl.ds(c * plane + x * cy + p, 8, stride=cy), :]

    def emit(c, w, i, value):
        rows = pl.ds(c * plane + w * 8 * cy + i, 8, stride=cy)
        out[rows, :] = start[rows, :] + value * scale

    line_kernel_body(cells, flux, speed, wave, emit, n=cy, width=cx, axis=1)


def x_kernel(state, ends, start, old, out, density, cells, flux, speed, wave, *, cx, cy, scale):
    plane = cx * cy
    length = cx + 6
    for c in range(5):
        base = c * length * cy
        cells[base : base + 3 * cy, :] = ends[(5 + c) * 3 * cy : (6 + c) * 3 * cy, :]
        cells[base + 3 * cy : base + (cx + 3) * cy, :] = state[c * plane : (c + 1) * plane, :]
        cells[base + (cx + 3) * cy : base + length * cy, :] = ends[c * 3 * cy : (c + 1) * 3 * cy, :]

    def emit(c, w, i, value):
        rows = pl.ds(pl.multiple_of(c * plane + i * cy + w * 8, 8), 8)
        change = start[rows, :] + value * scale
        out[rows, :] = (0.75 * old[rows, :] + 0.25 * state[rows, :]) - change

    line_kernel_body(cells, flux, speed, wave, emit, n=cx, width=cy, axis=0)
    density[...] = out[0:plane, :]


def line_call(kernel, operands, n, width, name, more=(), results=()):
    length = n + 6
    vm = pl.BlockSpec(memory_space=pltpu.VMEM)
    return pl.pallas_call(
        kernel,
        out_shape=[jax.ShapeDtypeStruct(shape, jnp.float32) for shape in (operands[0].shape, *results)],
        in_specs=[vm] * len(operands),
        out_specs=[vm] * (1 + len(results)),
        scratch_shapes=[
            pltpu.VMEM((5 * length * width, 128), jnp.float32),
            pltpu.VMEM((5 * length * width, 128), jnp.float32),
            pltpu.VMEM((length * width, 128), jnp.float32),
            pltpu.VMEM((length * width, 128), jnp.float32),
        ]
        + list(more),
        name=name,
        compiler_params=pltpu.CompilerParams(vmem_limit_bytes=6 * 1024 * 1024),
    )(*operands)


def neighbours(first, last, axis):
    size = lax.axis_size(axis)
    up = [(i, (i + 1) % size) for i in range(size)]
    down = [(j, i) for i, j in up]
    return lax.ppermute(last, axis, up), lax.ppermute(first, axis, down)


def flow(state_old, state_section, counts, step_size):
    shape = state_section.shape
    cx, cy, cz = shape[1:]
    state = state_section.reshape(-1, cz)
    turned, zlo, zhi, ylo, yhi, xends = pack(state, cx, cy, cz)
    if lax.axis_size("gx") == 2:
        ends = swap(xends, "gx", 1)
    else:
        ends = jnp.concatenate(neighbours(xends[: xends.shape[0] // 2], xends[xends.shape[0] // 2 :], "gx")[::-1])
    zl, zr = neighbours(zlo, zhi, "gz")
    yl, yr = neighbours(ylo, yhi, "gy")
    scales = [0.25 * step_size * n / 12.0 for n in counts]
    plane = cx * cy
    (part,) = line_call(
        functools.partial(z_kernel, cx=cx, cy=cy, cz=cz, scale=scales[2]),
        (turned, zl, zr), cz // 2, plane // 64, "along_z",
        (pltpu.VMEM((5 * plane, 128), jnp.float32),),
    )
    (part,) = line_call(functools.partial(y_kernel, cx=cx, cy=cy, scale=scales[1]), (state, yl, yr, part), cy, cx, "along_y")
    updated, density = line_call(
        functools.partial(x_kernel, cx=cx, cy=cy, scale=scales[0]),
        (state, ends, part, state_old.reshape(-1, cz)), cx, cy, "along_x", (), ((plane, cz),),
    )
    return updated.reshape(shape), density


def dft_table(sample_count, freq_count):
    times = np.arange(sample_count, dtype=np.int64)[None, :]
    orders = np.arange(1, freq_count + 1, dtype=np.int64)[:, None]
    phases = (np.float32(2.0 * math.pi / sample_count) * (times * orders % sample_count).astype(np.float32)).astype(np.float64)
    scaling = 1.0 / math.sqrt(sample_count)
    both = np.concatenate([np.cos(phases), -np.sin(phases)], axis=0).astype(np.float32) * np.float32(scaling)
    return jnp.asarray(both, jnp.bfloat16)


def double_angle(x):
    x2 = x * x
    s = 1.0 / 6227020800.0
    s = s * x2 - 1.0 / 39916800.0
    s = s * x2 + 1.0 / 362880.0
    s = s * x2 - 1.0 / 5040.0
    s = s * x2 + 1.0 / 120.0
    s = s * x2 - 1.0 / 6.0
    s = (s * x2) * x + x
    c = 1.0 / 479001600.0
    c = c * x2 - 1.0 / 3628800.0
    c = c * x2 + 1.0 / 40320.0
    c = c * x2 - 1.0 / 720.0
    c = c * x2 + 1.0 / 24.0
    c = c * x2 - 0.5
    c = c * x2 + 1.0
    s2 = s + s
    return 1.0 - s2 * s, s2 * c


def sincos_turns(turns):
    return double_angle((turns - jnp.round(turns)) * math.pi)


def direction(polar, azimuth):
    cos_p, sin_p = double_angle(0.25 * polar)
    cos_a, sin_a = double_angle(0.5 * azimuth)
    return cos_p * cos_a, cos_p * sin_a, sin_p


def three(value):
    high = value.astype(jnp.bfloat16).astype(jnp.float32)
    middle = (value - high).astype(jnp.bfloat16).astype(jnp.float32)
    return high, middle, ((value - high) - middle).astype(jnp.bfloat16).astype(jnp.float32)


def weights_kernel(
    live, corner, cell, angles, raw, out, centre, lis, geo, lisb, pan, row_side, sides, col_side, cols, *, sizes, counts
):
    slots, bp = cell.shape
    tiles = lis.shape[1]
    span = tiles * 128 // CHUNKS
    cells = cell[...].astype(jnp.float32)
    along_x = jnp.floor((cells + 0.5) * (1.0 / (sizes[1] * sizes[2])))
    rest = cells - along_x * float(sizes[1] * sizes[2])
    along_y = jnp.floor((rest + 0.5) * (1.0 / sizes[2]))
    along_z = rest - along_y * float(sizes[2])
    offsets = []
    for k, along in enumerate((along_x, along_y, along_z)):
        place = ((along + corner[k].astype(jnp.float32)) + 0.5) / float(counts[k])
        mean = jnp.sum(place, axis=1, keepdims=True) * (1.0 / bp)
        centre[k] = jnp.broadcast_to(mean, (slots, 128))
        offsets.append(place - 0.5)
    shown = lax.broadcasted_iota(jnp.int32, (slots, bp), 0) < live[0]
    along_normal = 0.0
    for k, part in enumerate(direction(angles[0], angles[1])):
        geo[k] = jnp.where(shown, part * (0.25 / math.pi), 0.0)
        along_normal = along_normal + geo[k] * offsets[k]
    geo[3] = along_normal
    shifts = []
    for k, part in enumerate(direction(raw[0], raw[1])):
        shift = raw[2] * part
        lis[k] = 0.5 + shift
        shifts.append(shift)
        for t in range(tiles):
            lisb[k, t * 128 : (t + 1) * 128, :] = jnp.transpose(jnp.broadcast_to(shift[t : t + 1, :], (128, 128)))
    one = jnp.ones((tiles, 128), jnp.float32)
    left, right = [], []
    for k in range(3):
        for n, part in enumerate(three(-2.0 * offsets[k])):
            pan[3 * k + n] = part
        high, middle, low = three(shifts[k])
        left += [high, high, high, middle, middle, low]
        right += [3 * k, 3 * k + 1, 3 * k + 2, 3 * k, 3 * k + 1, 3 * k]
    for n, part in enumerate(three(offsets[0] * offsets[0] + offsets[1] * offsets[1] + offsets[2] * offsets[2])):
        pan[9 + n] = part
    pan[12] = jnp.ones((slots, bp), jnp.float32)
    left += [*three(shifts[0] * shifts[0] + shifts[1] * shifts[1] + shifts[2] * shifts[2]), one, one, one]
    right += [12, 12, 12, 9, 10, 11]
    row_side[...] = jnp.zeros(row_side.shape, jnp.float32)
    col_side[...] = jnp.zeros(col_side.shape, jnp.float32)
    cols[...] = jnp.zeros(cols.shape, jnp.bfloat16)
    for n, part in enumerate(left):
        for t in range(tiles):
            row_side[n : n + 1, t * 128 : (t + 1) * 128] = part[t : t + 1, :]
    for t in range(tiles):
        sides[t * 128 : (t + 1) * 128, :] = jnp.transpose(row_side[:, t * 128 : (t + 1) * 128]).astype(jnp.bfloat16)

    def pair(turn, _):
        first = turn * 2
        for j in range(2):
            for n, source in enumerate(right):
                col_side[n : n + 1, j * bp : (j + 1) * bp] = pan[source, pl.ds(first + j, 1), :]
        cols[0:32, :] = col_side[...].astype(jnp.bfloat16)
        parts = [[geo[k, pl.ds(first + j, 1), :] for k in range(4)] for j in range(2)]
        for q in range(CHUNKS):
            for r in range(0, span, 128):
                at = q * span + r
                d2 = jnp.dot(sides[at : at + 128, :], cols[...], preferred_element_type=jnp.float32)
                for w in range(0, 128, 16):
                    lx, ly, lz = [lisb[k, at + w : at + w + 16, :] for k in range(3)]
                    for j in range(2):
                        nx, ny, nz, shift = parts[j]
                        facing = (nx * lx + ny * ly) + (nz * lz - shift)
                        row = pl.multiple_of(q * slots * span + (first + j) * span + r + w, 16)
                        value = facing * (1.0 / d2[w : w + 16, j * bp : (j + 1) * bp])
                        out[pl.ds(row, 16), :] = value.astype(jnp.bfloat16)
        return 0

    lax.fori_loop(0, (live[0] + BATCH - 1) // BATCH * (BATCH // 2), pair, 0)


def weights(live, corner, cell, angles, raw, sizes, counts):
    slots, bp = cell.shape
    obs = raw.shape[1] * 128
    vm = pl.BlockSpec(memory_space=pltpu.VMEM)
    sm = pl.BlockSpec(memory_space=pltpu.SMEM)
    return pl.pallas_call(
        functools.partial(weights_kernel, sizes=sizes, counts=counts),
        out_shape=[
            jax.ShapeDtypeStruct((slots * obs, bp), jnp.bfloat16),
            jax.ShapeDtypeStruct((3, slots, 128), jnp.float32),
            jax.ShapeDtypeStruct(raw.shape, jnp.float32),
        ],
        in_specs=[sm, sm, vm, vm, vm],
        out_specs=[vm] * 3,
        scratch_shapes=[
            pltpu.VMEM((4, slots, bp), jnp.float32),
            pltpu.VMEM((3, obs, 128), jnp.float32),
            pltpu.VMEM((13, slots, bp), jnp.float32),
            pltpu.VMEM((128, obs), jnp.float32),
            pltpu.VMEM((obs, 128), jnp.bfloat16),
            pltpu.VMEM((32, 2 * bp), jnp.float32),
            pltpu.VMEM((128, 2 * bp), jnp.bfloat16),
        ],
        name="weights",
        compiler_params=pltpu.CompilerParams(vmem_limit_bytes=4 * 1024 * 1024),
    )(live, corner, cell, angles, raw)


def spectra_kernel(live, dens, rec, cell, table, sp, dens3, onehot, src):
    slots, bp = cell.shape
    rows = dens.shape[0] // 2
    total = (live[0] + WIDE - 1) // WIDE
    span = WIDE * bp

    for h in range(2):
        d = dens[pl.ds(h, rows, stride=2), :]
        hi = d.astype(jnp.bfloat16)
        left = d - hi.astype(jnp.float32)
        mid = left.astype(jnp.bfloat16)
        lo = (left - mid.astype(jnp.float32)).astype(jnp.bfloat16)
        for k, part in enumerate((hi, mid, lo)):
            dens3[k, :, h * 128 : (h + 1) * 128] = part
    lane = lax.broadcasted_iota(jnp.int32, (bp, 128), 1).astype(jnp.float32)

    def group(g, _):
        lows = []
        for j in range(WIDE):
            cells = cell[pl.ds(g * WIDE + j, 1), :].astype(jnp.float32)
            col = jnp.transpose(jnp.broadcast_to(cells, (128, 128)))
            high = jnp.floor(col * (1.0 / 256.0))
            low = col - 256.0 * high
            lows.append(low)
            for h in range(rows // 128):
                hit = jnp.where(high == lane + float(128 * h), 1.0, 0.0).astype(jnp.bfloat16)
                onehot[j * bp : (j + 1) * bp, h * 128 : (h + 1) * 128] = hit
        for j in range(WIDE):
            if j % 2 == 0:
                hot = onehot[j * bp : (j + 2) * bp, :]
                picked = jnp.dot(hot, dens3[0], preferred_element_type=jnp.float32)
                picked = picked + jnp.dot(hot, dens3[1], preferred_element_type=jnp.float32)
                picked = picked + jnp.dot(hot, dens3[2], preferred_element_type=jnp.float32)
            own = picked[j % 2 * bp : (j % 2 + 1) * bp, :]
            found = jnp.where(lows[j] == lane, own[:, 0:128], 0.0) + jnp.where(lows[j] == lane + 128.0, own[:, 128:256], 0.0)
            sampled = jnp.sum(found, axis=1, keepdims=True)
            record = rec[pl.ds(pl.multiple_of(g * span + j * bp, bp), bp), :].astype(jnp.float32)
            src[j * bp : (j + 1) * bp, :] = (record * sampled).astype(jnp.bfloat16)
        for j in range(0, WIDE, 2):
            both = lax.dot_general(table[...], src[j * bp : (j + 2) * bp, :], NT, preferred_element_type=jnp.float32)
            both = both.astype(jnp.bfloat16)
            sp[g * WIDE + j] = both[:, 0:bp]
            sp[g * WIDE + j + 1] = both[:, bp : 2 * bp]
        return 0

    lax.fori_loop(0, total, group, 0)


def spectra(live, dens, rec, cell, table):
    rows = dens.shape[0]
    slots, bp = cell.shape
    samples = rec.shape[1]
    k2 = table.shape[0]
    vm = pl.BlockSpec(memory_space=pltpu.VMEM)
    return pl.pallas_call(
        spectra_kernel,
        out_shape=jax.ShapeDtypeStruct((slots, k2, bp), jnp.bfloat16),
        in_specs=[
            pl.BlockSpec(memory_space=pltpu.SMEM),
            vm,
            vm,
            vm,
            vm,
        ],
        out_specs=vm,
        scratch_shapes=[
            pltpu.VMEM((3, rows // 2, 256), jnp.bfloat16),
            pltpu.VMEM((WIDE * bp, rows // 2), jnp.bfloat16),
            pltpu.VMEM((WIDE * bp, samples), jnp.bfloat16),
        ],
        name="spectra",
        compiler_params=pltpu.CompilerParams(vmem_limit_bytes=7 * 1024 * 1024),
    )(live, dens, rec, cell, table)


def observe_kernel(live, centre, sp, wts, lis, *refs, chunk, part, parts, ties):
    slots, k2, bp = sp.shape
    tiles = lis.shape[1] // CHUNKS
    half = k2 // 2
    span = tiles * 128
    before, refs = (refs[0], refs[1 + ties :]) if part > 0 else (None, refs[ties:])
    out, prod, acc = refs if part == parts - 1 else (None, refs[1], refs[0])
    total = (live[0] + BATCH - 1) // BATCH
    turns = (total - part + parts - 1) // parts
    if before is None:
        acc[...] = jnp.zeros(acc.shape, jnp.float32)
    else:
        acc[...] = before[...]
    orders = lax.broadcasted_iota(jnp.int32, (8, 128), 0).astype(jnp.float32) + 1.0
    orders = orders * (WAVE_STEP / (2.0 * math.pi))

    def group(turn, _):
        g = turn * parts + part
        for h, pair in [(h, pair) for h in range(0, span, 256) for pair in range(0, BATCH, 2)]:
            for j in range(2):
                b = g * BATCH + pair + j
                held = wts[pl.ds(pl.multiple_of(chunk * slots * span + b * span + h, 256), 256), :]
                prod[pair + j, :, h : h + 256] = lax.dot_general(sp[b], held, NT, preferred_element_type=jnp.float32)
            for t in range(h // 128, h // 128 + 2):
                state = []
                for j in range(2):
                    b = g * BATCH + pair + j
                    u = chunk * tiles + t
                    away = [jnp.broadcast_to(lis[k, u : u + 1, :] - centre[k, pl.ds(b, 1), :], (8, 128)) for k in range(3)]
                    reach = jnp.sqrt(away[0] * away[0] + away[1] * away[1] + away[2] * away[2])
                    c, s = sincos_turns(reach * orders)
                    ec = jnp.broadcast_to(c[7:8, :], (8, 128))
                    es = jnp.broadcast_to(s[7:8, :], (8, 128))
                    state.append([c, s, ec * c - es * s, es * c + ec * s, ec + ec])
                for a in range(half // 8):
                    re_sum = acc[0, a * 8 : a * 8 + 8, t * 128 : t * 128 + 128]
                    im_sum = acc[1, a * 8 : a * 8 + 8, t * 128 : t * 128 + 128]
                    for j in range(2):
                        c, s, c_next, s_next, twice = state[j]
                        re = prod[pair + j, a * 8 : a * 8 + 8, t * 128 : t * 128 + 128]
                        im = prod[pair + j, half + a * 8 : half + a * 8 + 8, t * 128 : t * 128 + 128]
                        re_sum = re_sum + (re * c + im * s)
                        im_sum = im_sum + (im * c - re * s)
                        state[j] = [c_next, s_next, twice * c_next - c, twice * s_next - s, twice]
                    acc[0, a * 8 : a * 8 + 8, t * 128 : t * 128 + 128] = re_sum
                    acc[1, a * 8 : a * 8 + 8, t * 128 : t * 128 + 128] = im_sum
        return 0

    lax.fori_loop(0, turns, group, 0)
    if out is None:
        return
    shares, _, per, _ = out.shape
    each = 128 // per
    for k in range(2):
        for t in range(tiles):
            turned = jnp.transpose(acc[k, :, t * 128 : (t + 1) * 128])
            for e in range(each):
                out[t * each + e, k, :, :] = turned[e * per : (e + 1) * per, :]


def observe(chunk, part, parts, live, centre, sp, wts, lis, shares, before=None, ties=()):
    slots, k2, bp = sp.shape
    span = lis.shape[1] * 128 // CHUNKS
    vm = pl.BlockSpec(memory_space=pltpu.VMEM)
    sm = pl.BlockSpec(memory_space=pltpu.SMEM)
    sums = (2, k2 // 2, span)
    last = part == parts - 1
    scratch = [pltpu.VMEM((BATCH, k2, span), jnp.float32)]
    return pl.pallas_call(
        functools.partial(observe_kernel, chunk=chunk, part=part, parts=parts, ties=len(ties)),
        out_shape=jax.ShapeDtypeStruct((shares, 2, span // shares, k2 // 2) if last else sums, jnp.float32),
        in_specs=[sm, vm, vm, vm, vm] + [vm] * (part > 0) + [pl.BlockSpec(memory_space=pl.ANY)] * len(ties),
        out_specs=vm,
        scratch_shapes=scratch + [pltpu.VMEM(sums, jnp.float32)] * last,
        name="observe",
        cost_estimate=pl.CostEstimate(flops=4_000_000_000, transcendentals=0, bytes_accessed=1_000_000),
        compiler_params=pltpu.CompilerParams(vmem_limit_bytes=4 * 1024 * 1024),
    )(live, centre, sp, wts, lis, *([before] if part > 0 else []), *ties)


def swap(value, axis, bit):
    size = lax.axis_size(axis)
    return lax.ppermute(value, axis, [(i, i ^ bit) for i in range(size)])


def stages():
    def bits(axis):
        return [1 << k for k in range(lax.axis_size(axis).bit_length() - 1)]

    steps = [("halve", axis, bit) for axis in ("gz", "gx") for bit in bits(axis)]
    steps += [("sum", "gy", bit) for bit in bits("gy")]
    return steps + [("gather", "gx", bit) for bit in bits("gx")[::-1]]


def exchange(value, kind, axis, bit):
    if kind == "sum":
        return value + swap(value, axis, bit)
    up = (lax.axis_index(axis) // bit) % 2
    if kind == "gather":
        theirs = swap(value, axis, bit)
        first = jnp.where(up == 0, value, theirs)
        return jnp.concatenate([first, jnp.where(up == 0, theirs, value)], axis=2)
    if axis == "gz":
        pairs, dim = value.reshape((value.shape[0] // 2, 2) + value.shape[1:]), 1
    else:
        pairs, dim = value.reshape(value.shape[:2] + (2, value.shape[2] // 2) + value.shape[3:]), 2
    mine = lax.dynamic_index_in_dim(pairs, up, dim, keepdims=False)
    theirs = lax.dynamic_index_in_dim(pairs, 1 - up, dim, keepdims=False)
    return mine + swap(theirs, axis, bit)


def local(
    state_old,
    state_section,
    panel_record,
    panel_cell,
    panel_angles,
    owned_blocks,
    listener_angles,
    listener_range,
):
    sizes = state_section.shape[1:]
    axes = ("gx", "gy", "gz")
    counts = tuple(n * lax.axis_size(axis) for n, axis in zip(sizes, axes))
    step_size = COURANT / max(counts)
    slot_count, block_rows = panel_cell.shape
    samples = panel_record.shape[1]
    shares = lax.axis_size("gz")
    corner = jnp.stack([lax.axis_index(axis) * n for n, axis in zip(sizes, axes)]).astype(jnp.int32)
    raw = jnp.concatenate([listener_angles, listener_range[None]], axis=0)
    raw = jnp.transpose(raw.reshape(3, shares, CHUNKS, -1), (0, 2, 1, 3)).reshape(3, -1, 128)
    angles = panel_angles.reshape(2, slot_count, block_rows)
    wts, centres, listeners = weights(owned_blocks, corner, panel_cell, angles, raw, sizes, counts)
    updated, density = flow(state_old, state_section, counts, step_size)
    heard = spectra(owned_blocks, density, panel_record, panel_cell, dft_table(samples, FREQS))
    steps = stages()
    known = (owned_blocks, centres, heard, wts, listeners, shares)
    pieces, done = [], []
    for q in range(CHUNKS):
        parts = 1 if q == 0 else PARTS
        sums = None
        for part in range(parts):
            ties = []
            if part > 0:
                for k in range(len(pieces)):
                    if done[k] < len(steps):
                        pieces[k] = exchange(pieces[k], *steps[done[k]])
                        done[k] += 1
                        ties.append(pieces[k])
            sums = observe(q, part, parts, *known, sums, ties)
        pieces.append(sums)
        done.append(0)
    while min(done) < len(steps):
        for k in range(len(pieces)):
            if done[k] < len(steps):
                pieces[k] = exchange(pieces[k], *steps[done[k]])
                done[k] += 1
    pieces = [v.reshape((2, -1, FREQS)) for v in pieces]
    return (updated, jnp.concatenate(pieces, axis=1))


def solution(mesh):
    return jax.shard_map(
        local,
        mesh=mesh,
        in_specs=(
            P(None, "gx", "gy", "gz"),
            P(None, "gx", "gy", "gz"),
            P(("gx", "gy", "gz"), None),
            P(("gx", "gy", "gz"), None),
            P(None, ("gx", "gy", "gz")),
            P(("gx", "gy", "gz")),
            P(),
            P(),
        ),
        out_specs=(P(None, "gx", "gy", "gz"), P(None, "gz", None)),
        check_vma=False,
    )
```

```python
import functools
import math

import jax
import jax.numpy as jnp
import numpy as np
from jax import lax
from jax.experimental import pallas as pl
from jax.experimental.pallas import tpu as pltpu
from jax.sharding import PartitionSpec as P

FREQS = 128
BATCH = 4
WIDE = 8
CHUNKS = 2
PARTS = 1
NT = (((1,), (1,)), ((), ()))


GAMMA_GAS = 4.4
PRESSURE_INF = 1.0
WENO_EPS = 1e-06
WAVE_STEP = 0.25
COURANT = 0.08


def pack_kernel(state, turned, zlo, zhi, ylo, yhi, xends, *, cx, cy, cz):
    plane = cx * cy
    groups = plane // 128
    for c in range(5):
        for g in range(groups):
            row = c * plane + g * 128
            turned[row : row + cz, :] = jnp.transpose(state[row : row + 128, :])
        for k in range(3):
            ylo[(c * 3 + k) * cx : (c * 3 + k + 1) * cx, :] = state[pl.ds(c * plane + k, cx, stride=cy), :]
            yhi[(c * 3 + k) * cx : (c * 3 + k + 1) * cx, :] = state[pl.ds(c * plane + cy - 3 + k, cx, stride=cy), :]
            zlo[(c * 3 + k) * groups : (c * 3 + k + 1) * groups, :] = turned[pl.ds(c * plane + k, groups, stride=128), :]
            zhi[(c * 3 + k) * groups : (c * 3 + k + 1) * groups, :] = turned[pl.ds(c * plane + cz - 3 + k, groups, stride=128), :]
        xends[c * 3 * cy : (c + 1) * 3 * cy, :] = state[c * plane : c * plane + 3 * cy, :]
        xends[(5 + c) * 3 * cy : (6 + c) * 3 * cy, :] = state[c * plane + (cx - 3) * cy : (c + 1) * plane, :]


def pack(state, cx, cy, cz):
    groups = cx * cy // 128
    rows = [state.shape[0]] + [15 * groups] * 2 + [15 * cx] * 2 + [30 * cy]
    vm = pl.BlockSpec(memory_space=pltpu.VMEM)
    return pl.pallas_call(
        functools.partial(pack_kernel, cx=cx, cy=cy, cz=cz),
        out_shape=[jax.ShapeDtypeStruct((r, 128), jnp.float32) for r in rows],
        in_specs=[vm],
        out_specs=[vm] * 6,
        name="pack",
        compiler_params=pltpu.CompilerParams(vmem_limit_bytes=2 * 1024 * 1024),
    )(state)


def weno_shift(d1, d2, d3, d4):
    a0, a1, a2 = d2 - d1, d3 - d2, d4 - d3
    h2, h3 = 0.75 * d2, 0.75 * d3
    eps = 3.0 * WENO_EPS
    e0 = (a0 * a0 + eps) + h2 * (d2 + a0)
    e1 = (a1 * a1 + eps) + h2 * d3
    e2 = (a2 * a2 + eps) + h3 * (d3 - a2)
    t1 = e1 * e1
    u0 = 3.0 * (e0 * e0)
    u2 = 2.0 * (e2 * e2)
    w0, w1, w2 = t1 * u2, u0 * u2, u0 * t1
    below = 0.5 * w0 + (w1 + w2)
    above = w0 * (a1 - a0) + w2 * (a2 - a1)
    return (d2 + (d3 + d3)) - above * (1.0 / below)


def line_kernel_body(cells, flux, speed, wave, emit, *, n, width, axis):
    length = n + 6
    tiles = width // 8
    span = length * width

    def fluxes(p, _):
        for w in range(tiles):
            at = pl.multiple_of(p * width + w * 8, 8)
            rho = cells[pl.ds(at, 8), :]
            m = [cells[pl.ds((1 + k) * span + at, 8), :] for k in range(3)]
            energy = cells[pl.ds(4 * span + at, 8), :]
            inv = 1.0 / rho
            u = m[axis] * inv
            twice = (m[0] * m[0] + m[1] * m[1] + m[2] * m[2]) * inv
            pressure = (GAMMA_GAS - 1.0) * (energy - 0.5 * twice) - GAMMA_GAS * PRESSURE_INF
            sound = jnp.sqrt(GAMMA_GAS * (pressure + PRESSURE_INF) * inv)
            speed[pl.ds(at, 8), :] = jnp.abs(u) + sound
            flux[pl.ds(at, 8), :] = m[axis]
            for k in range(3):
                carried = m[k] * u
                if k == axis:
                    carried = carried + pressure
                flux[pl.ds((1 + k) * span + at, 8), :] = carried
            flux[pl.ds(4 * span + at, 8), :] = (energy + pressure) * u
        return 0

    lax.fori_loop(0, length, fluxes, 0, unroll=5 if tiles == 1 else 2)

    def waves(i, _):
        for w in range(tiles):
            at = pl.multiple_of(i * width + w * 8, 8)
            top = speed[pl.ds(at, 8), :]
            for k in range(1, 6):
                top = jnp.maximum(top, speed[pl.ds(at + k * width, 8), :])
            wave[pl.ds(at, 8), :] = top
        return 0

    lax.fori_loop(0, n + 1, waves, 0, unroll={1: 5, 2: 3}.get(tiles, 1))

    def line(index, _):
        c = index // tiles
        w = index % tiles

        def load(ref, p):
            return ref[pl.ds(pl.multiple_of(c * span + p * width + w * 8, 8), 8), :]

        q = [load(cells, p) for p in range(5)]
        f = [load(flux, p) for p in range(5)]
        dq = [q[k + 1] - q[k] for k in range(4)]
        df = [f[k + 1] - f[k] for k in range(4)]
        q_last, f_last, f_mid, f_near = q[4], f[4], f[2], f[3]
        before = None
        for i in range(n + 1):
            q_new, f_new = load(cells, i + 5), load(flux, i + 5)
            dq.append(q_new - q_last)
            df.append(f_new - f_last)
            alpha = wave[pl.ds(pl.multiple_of(i * width + w * 8, 8), 8), :]
            drift = [alpha * v for v in dq]
            up = weno_shift(*[df[k] + drift[k] for k in range(4)])
            down = weno_shift(*[drift[k] - df[k] for k in (4, 3, 2, 1)])
            here = 6.0 * ((f_mid + f_near) - drift[2]) + (up + down)
            if before is not None:
                emit(c, w, i - 1, here - before)
            before = here
            dq, df = dq[1:], df[1:]
            f_mid, f_near = f_near, f_last
            q_last, f_last = q_new, f_new
        return 0

    lax.fori_loop(0, 5 * tiles, line, 0)


def z_kernel(turned, left, right, out, cells, flux, speed, wave, part, *, cx, cy, cz, scale):
    plane = cx * cy
    groups = plane // 128
    width = 2 * groups
    n = cz // 2
    length = n + 6
    for c in range(5):
        base = c * length * width
        for p in range(3):
            cells[pl.ds(base + p * width, groups, stride=2), :] = left[(c * 3 + p) * groups : (c * 3 + p + 1) * groups, :]
            cells[pl.ds(base + p * width + 1, groups, stride=2), :] = turned[pl.ds(c * plane + n - 3 + p, groups, stride=128), :]
            q = n + 3 + p
            cells[pl.ds(base + q * width, groups, stride=2), :] = turned[pl.ds(c * plane + n + p, groups, stride=128), :]
            cells[pl.ds(base + q * width + 1, groups, stride=2), :] = right[(c * 3 + p) * groups : (c * 3 + p + 1) * groups, :]
        for p in range(n):
            cells[base + (p + 3) * width : base + (p + 4) * width, :] = turned[pl.ds(c * plane + p, width, stride=n), :]

    def emit(c, w, i, value):
        part[pl.ds(c * plane + i, width, stride=n), :] = value * scale

    line_kernel_body(cells, flux, speed, wave, emit, n=n, width=width, axis=2)
    for c in range(5):
        for g in range(groups):
            row = c * plane + g * 128
            out[row : row + 128, :] = jnp.transpose(part[row : row + cz, :])


def y_kernel(state, left, right, start, out, cells, flux, speed, wave, *, cx, cy, scale):
    plane = cx * cy
    length = cy + 6
    for c in range(5):
        base = c * length * cx
        cells[base : base + 3 * cx, :] = left[c * 3 * cx : (c + 1) * 3 * cx, :]
        cells[base + (cy + 3) * cx : base + length * cx, :] = right[c * 3 * cx : (c + 1) * 3 * cx, :]
        for p in range(cy):
            for x in range(0, cx, 8):
                cells[base + (p + 3) * cx + x : base + (p + 3) * cx + x + 8, :] = state[pl.ds(c * plane + x * cy + p, 8, stride=cy), :]

    def emit(c, w, i, value):
        rows = pl.ds(c * plane + w * 8 * cy + i, 8, stride=cy)
        out[rows, :] = start[rows, :] + value * scale

    line_kernel_body(cells, flux, speed, wave, emit, n=cy, width=cx, axis=1)


def x_kernel(state, ends, start, old, out, density, cells, flux, speed, wave, *, cx, cy, scale):
    plane = cx * cy
    length = cx + 6
    for c in range(5):
        base = c * length * cy
        cells[base : base + 3 * cy, :] = ends[(5 + c) * 3 * cy : (6 + c) * 3 * cy, :]
        cells[base + 3 * cy : base + (cx + 3) * cy, :] = state[c * plane : (c + 1) * plane, :]
        cells[base + (cx + 3) * cy : base + length * cy, :] = ends[c * 3 * cy : (c + 1) * 3 * cy, :]

    def emit(c, w, i, value):
        rows = pl.ds(pl.multiple_of(c * plane + i * cy + w * 8, 8), 8)
        change = start[rows, :] + value * scale
        out[rows, :] = (0.75 * old[rows, :] + 0.25 * state[rows, :]) - change

    line_kernel_body(cells, flux, speed, wave, emit, n=cx, width=cy, axis=0)
    density[...] = out[0:plane, :]


def line_call(kernel, operands, n, width, name, more=(), results=()):
    length = n + 6
    vm = pl.BlockSpec(memory_space=pltpu.VMEM)
    return pl.pallas_call(
        kernel,
        out_shape=[jax.ShapeDtypeStruct(shape, jnp.float32) for shape in (operands[0].shape, *results)],
        in_specs=[vm] * len(operands),
        out_specs=[vm] * (1 + len(results)),
        scratch_shapes=[
            pltpu.VMEM((5 * length * width, 128), jnp.float32),
            pltpu.VMEM((5 * length * width, 128), jnp.float32),
            pltpu.VMEM((length * width, 128), jnp.float32),
            pltpu.VMEM((length * width, 128), jnp.float32),
        ]
        + list(more),
        name=name,
        compiler_params=pltpu.CompilerParams(vmem_limit_bytes=6 * 1024 * 1024),
    )(*operands)


def neighbours(first, last, axis):
    size = lax.axis_size(axis)
    up = [(i, (i + 1) % size) for i in range(size)]
    down = [(j, i) for i, j in up]
    return lax.ppermute(last, axis, up), lax.ppermute(first, axis, down)


def flow(state_old, state_section, counts, step_size):
    shape = state_section.shape
    cx, cy, cz = shape[1:]
    state = state_section.reshape(-1, cz)
    turned, zlo, zhi, ylo, yhi, xends = pack(state, cx, cy, cz)
    if lax.axis_size("gx") == 2:
        ends = swap(xends, "gx", 1)
    else:
        ends = jnp.concatenate(neighbours(xends[: xends.shape[0] // 2], xends[xends.shape[0] // 2 :], "gx")[::-1])
    zl, zr = neighbours(zlo, zhi, "gz")
    yl, yr = neighbours(ylo, yhi, "gy")
    scales = [0.25 * step_size * n / 12.0 for n in counts]
    plane = cx * cy
    (part,) = line_call(
        functools.partial(z_kernel, cx=cx, cy=cy, cz=cz, scale=scales[2]),
        (turned, zl, zr), cz // 2, plane // 64, "along_z",
        (pltpu.VMEM((5 * plane, 128), jnp.float32),),
    )
    (part,) = line_call(functools.partial(y_kernel, cx=cx, cy=cy, scale=scales[1]), (state, yl, yr, part), cy, cx, "along_y")
    updated, density = line_call(
        functools.partial(x_kernel, cx=cx, cy=cy, scale=scales[0]),
        (state, ends, part, state_old.reshape(-1, cz)), cx, cy, "along_x", (), ((plane, cz),),
    )
    return updated.reshape(shape), density


def dft_table(sample_count, freq_count):
    times = np.arange(sample_count, dtype=np.int64)[None, :]
    orders = np.arange(1, freq_count + 1, dtype=np.int64)[:, None]
    phases = (np.float32(2.0 * math.pi / sample_count) * (times * orders % sample_count).astype(np.float32)).astype(np.float64)
    scaling = 1.0 / math.sqrt(sample_count)
    both = np.concatenate([np.cos(phases), -np.sin(phases)], axis=0).astype(np.float32) * np.float32(scaling)
    return jnp.asarray(both, jnp.bfloat16)


def double_angle(x):
    x2 = x * x
    s = 1.0 / 6227020800.0
    s = s * x2 - 1.0 / 39916800.0
    s = s * x2 + 1.0 / 362880.0
    s = s * x2 - 1.0 / 5040.0
    s = s * x2 + 1.0 / 120.0
    s = s * x2 - 1.0 / 6.0
    s = (s * x2) * x + x
    c = 1.0 / 479001600.0
    c = c * x2 - 1.0 / 3628800.0
    c = c * x2 + 1.0 / 40320.0
    c = c * x2 - 1.0 / 720.0
    c = c * x2 + 1.0 / 24.0
    c = c * x2 - 0.5
    c = c * x2 + 1.0
    s2 = s + s
    return 1.0 - s2 * s, s2 * c


def sincos_turns(turns):
    return double_angle((turns - jnp.round(turns)) * math.pi)


def direction(polar, azimuth):
    cos_p, sin_p = double_angle(0.25 * polar)
    cos_a, sin_a = double_angle(0.5 * azimuth)
    return cos_p * cos_a, cos_p * sin_a, sin_p


def three(value):
    high = value.astype(jnp.bfloat16).astype(jnp.float32)
    middle = (value - high).astype(jnp.bfloat16).astype(jnp.float32)
    return high, middle, ((value - high) - middle).astype(jnp.bfloat16).astype(jnp.float32)


def weights_kernel(
    live, corner, cell, angles, raw, out, centre, lis, geo, lisb, pan, row_side, sides, col_side, cols, *, sizes, counts
):
    slots, bp = cell.shape
    tiles = lis.shape[1]
    span = tiles * 128 // CHUNKS
    cells = cell[...].astype(jnp.float32)
    along_x = jnp.floor((cells + 0.5) * (1.0 / (sizes[1] * sizes[2])))
    rest = cells - along_x * float(sizes[1] * sizes[2])
    along_y = jnp.floor((rest + 0.5) * (1.0 / sizes[2]))
    along_z = rest - along_y * float(sizes[2])
    offsets = []
    for k, along in enumerate((along_x, along_y, along_z)):
        place = ((along + corner[k].astype(jnp.float32)) + 0.5) / float(counts[k])
        mean = jnp.sum(place, axis=1, keepdims=True) * (1.0 / bp)
        centre[k] = jnp.broadcast_to(mean, (slots, 128))
        offsets.append(place - 0.5)
    shown = lax.broadcasted_iota(jnp.int32, (slots, bp), 0) < live[0]
    along_normal = 0.0
    for k, part in enumerate(direction(angles[0], angles[1])):
        geo[k] = jnp.where(shown, part * (0.25 / math.pi), 0.0)
        along_normal = along_normal + geo[k] * offsets[k]
    geo[3] = along_normal
    shifts = []
    for k, part in enumerate(direction(raw[0], raw[1])):
        shift = raw[2] * part
        lis[k] = 0.5 + shift
        shifts.append(shift)
        for t in range(tiles):
            lisb[k, t * 128 : (t + 1) * 128, :] = jnp.transpose(jnp.broadcast_to(shift[t : t + 1, :], (128, 128)))
    one = jnp.ones((tiles, 128), jnp.float32)
    left, right = [], []
    for k in range(3):
        for n, part in enumerate(three(-2.0 * offsets[k])):
            pan[3 * k + n] = part
        high, middle, low = three(shifts[k])
        left += [high, high, high, middle, middle, low]
        right += [3 * k, 3 * k + 1, 3 * k + 2, 3 * k, 3 * k + 1, 3 * k]
    for n, part in enumerate(three(offsets[0] * offsets[0] + offsets[1] * offsets[1] + offsets[2] * offsets[2])):
        pan[9 + n] = part
    pan[12] = jnp.ones((slots, bp), jnp.float32)
    left += [*three(shifts[0] * shifts[0] + shifts[1] * shifts[1] + shifts[2] * shifts[2]), one, one, one]
    right += [12, 12, 12, 9, 10, 11]
    row_side[...] = jnp.zeros(row_side.shape, jnp.float32)
    col_side[...] = jnp.zeros(col_side.shape, jnp.float32)
    cols[...] = jnp.zeros(cols.shape, jnp.bfloat16)
    for n, part in enumerate(left):
        for t in range(tiles):
            row_side[n : n + 1, t * 128 : (t + 1) * 128] = part[t : t + 1, :]
    for t in range(tiles):
        sides[t * 128 : (t + 1) * 128, :] = jnp.transpose(row_side[:, t * 128 : (t + 1) * 128]).astype(jnp.bfloat16)

    def pair(turn, _):
        first = turn * 2
        for j in range(2):
            for n, source in enumerate(right):
                col_side[n : n + 1, j * bp : (j + 1) * bp] = pan[source, pl.ds(first + j, 1), :]
        cols[0:32, :] = col_side[...].astype(jnp.bfloat16)
        parts = [[geo[k, pl.ds(first + j, 1), :] for k in range(4)] for j in range(2)]
        for q in range(CHUNKS):
            for r in range(0, span, 128):
                at = q * span + r
                d2 = jnp.dot(sides[at : at + 128, :], cols[...], preferred_element_type=jnp.float32)
                for w in range(0, 128, 16):
                    lx, ly, lz = [lisb[k, at + w : at + w + 16, :] for k in range(3)]
                    for j in range(2):
                        nx, ny, nz, shift = parts[j]
                        facing = (nx * lx + ny * ly) + (nz * lz - shift)
                        row = pl.multiple_of(q * slots * span + (first + j) * span + r + w, 16)
                        value = facing * (1.0 / d2[w : w + 16, j * bp : (j + 1) * bp])
                        out[pl.ds(row, 16), :] = value.astype(jnp.bfloat16)
        return 0

    lax.fori_loop(0, (live[0] + BATCH - 1) // BATCH * (BATCH // 2), pair, 0)


def weights(live, corner, cell, angles, raw, sizes, counts):
    slots, bp = cell.shape
    obs = raw.shape[1] * 128
    vm = pl.BlockSpec(memory_space=pltpu.VMEM)
    sm = pl.BlockSpec(memory_space=pltpu.SMEM)
    return pl.pallas_call(
        functools.partial(weights_kernel, sizes=sizes, counts=counts),
        out_shape=[
            jax.ShapeDtypeStruct((slots * obs, bp), jnp.bfloat16),
            jax.ShapeDtypeStruct((3, slots, 128), jnp.float32),
            jax.ShapeDtypeStruct(raw.shape, jnp.float32),
        ],
        in_specs=[sm, sm, vm, vm, vm],
        out_specs=[vm] * 3,
        scratch_shapes=[
            pltpu.VMEM((4, slots, bp), jnp.float32),
            pltpu.VMEM((3, obs, 128), jnp.float32),
            pltpu.VMEM((13, slots, bp), jnp.float32),
            pltpu.VMEM((128, obs), jnp.float32),
            pltpu.VMEM((obs, 128), jnp.bfloat16),
            pltpu.VMEM((32, 2 * bp), jnp.float32),
            pltpu.VMEM((128, 2 * bp), jnp.bfloat16),
        ],
        name="weights",
        compiler_params=pltpu.CompilerParams(vmem_limit_bytes=4 * 1024 * 1024),
    )(live, corner, cell, angles, raw)


def spectra_kernel(live, dens, rec, cell, table, sp, dens3, onehot, src):
    slots, bp = cell.shape
    rows = dens.shape[0] // 2
    total = (live[0] + WIDE - 1) // WIDE
    span = WIDE * bp

    for h in range(2):
        d = dens[pl.ds(h, rows, stride=2), :]
        hi = d.astype(jnp.bfloat16)
        left = d - hi.astype(jnp.float32)
        mid = left.astype(jnp.bfloat16)
        lo = (left - mid.astype(jnp.float32)).astype(jnp.bfloat16)
        for k, part in enumerate((hi, mid, lo)):
            dens3[k, :, h * 128 : (h + 1) * 128] = part
    lane = lax.broadcasted_iota(jnp.int32, (bp, 128), 1).astype(jnp.float32)

    def group(g, _):
        lows = []
        for j in range(WIDE):
            cells = cell[pl.ds(g * WIDE + j, 1), :].astype(jnp.float32)
            col = jnp.transpose(jnp.broadcast_to(cells, (128, 128)))
            high = jnp.floor(col * (1.0 / 256.0))
            low = col - 256.0 * high
            lows.append(low)
            for h in range(rows // 128):
                hit = jnp.where(high == lane + float(128 * h), 1.0, 0.0).astype(jnp.bfloat16)
                onehot[j * bp : (j + 1) * bp, h * 128 : (h + 1) * 128] = hit
        for j in range(WIDE):
            if j % 2 == 0:
                hot = onehot[j * bp : (j + 2) * bp, :]
                picked = jnp.dot(hot, dens3[0], preferred_element_type=jnp.float32)
                picked = picked + jnp.dot(hot, dens3[1], preferred_element_type=jnp.float32)
                picked = picked + jnp.dot(hot, dens3[2], preferred_element_type=jnp.float32)
            own = picked[j % 2 * bp : (j % 2 + 1) * bp, :]
            found = jnp.where(lows[j] == lane, own[:, 0:128], 0.0) + jnp.where(lows[j] == lane + 128.0, own[:, 128:256], 0.0)
            sampled = jnp.sum(found, axis=1, keepdims=True)
            record = rec[pl.ds(pl.multiple_of(g * span + j * bp, bp), bp), :].astype(jnp.float32)
            src[j * bp : (j + 1) * bp, :] = (record * sampled).astype(jnp.bfloat16)
        for j in range(0, WIDE, 2):
            both = lax.dot_general(table[...], src[j * bp : (j + 2) * bp, :], NT, preferred_element_type=jnp.float32)
            both = both.astype(jnp.bfloat16)
            sp[g * WIDE + j] = both[:, 0:bp]
            sp[g * WIDE + j + 1] = both[:, bp : 2 * bp]
        return 0

    lax.fori_loop(0, total, group, 0)


def spectra(live, dens, rec, cell, table):
    rows = dens.shape[0]
    slots, bp = cell.shape
    samples = rec.shape[1]
    k2 = table.shape[0]
    vm = pl.BlockSpec(memory_space=pltpu.VMEM)
    return pl.pallas_call(
        spectra_kernel,
        out_shape=jax.ShapeDtypeStruct((slots, k2, bp), jnp.bfloat16),
        in_specs=[
            pl.BlockSpec(memory_space=pltpu.SMEM),
            vm,
            vm,
            vm,
            vm,
        ],
        out_specs=vm,
        scratch_shapes=[
            pltpu.VMEM((3, rows // 2, 256), jnp.bfloat16),
            pltpu.VMEM((WIDE * bp, rows // 2), jnp.bfloat16),
            pltpu.VMEM((WIDE * bp, samples), jnp.bfloat16),
        ],
        name="spectra",
        compiler_params=pltpu.CompilerParams(vmem_limit_bytes=7 * 1024 * 1024),
    )(live, dens, rec, cell, table)


def observe_kernel(live, centre, sp, wts, lis, *refs, chunk, part, parts, ties):
    slots, k2, bp = sp.shape
    tiles = lis.shape[1] // CHUNKS
    half = k2 // 2
    span = tiles * 128
    before, refs = (refs[0], refs[1 + ties :]) if part > 0 else (None, refs[ties:])
    out, prod, acc = refs if part == parts - 1 else (None, refs[1], refs[0])
    total = (live[0] + BATCH - 1) // BATCH
    turns = (total - part + parts - 1) // parts
    if before is None:
        acc[...] = jnp.zeros(acc.shape, jnp.float32)
    else:
        acc[...] = before[...]
    orders = lax.broadcasted_iota(jnp.int32, (8, 128), 0).astype(jnp.float32) + 1.0
    orders = orders * (WAVE_STEP / (2.0 * math.pi))

    def group(turn, _):
        g = turn * parts + part
        for h, pair in [(h, pair) for h in range(0, span, 256) for pair in range(0, BATCH, 2)]:
            for j in range(2):
                b = g * BATCH + pair + j
                held = wts[pl.ds(pl.multiple_of(chunk * slots * span + b * span + h, 256), 256), :]
                prod[pair + j, :, h : h + 256] = lax.dot_general(sp[b], held, NT, preferred_element_type=jnp.float32)
            for t in range(h // 128, h // 128 + 2):
                state = []
                for j in range(2):
                    b = g * BATCH + pair + j
                    u = chunk * tiles + t
                    away = [jnp.broadcast_to(lis[k, u : u + 1, :] - centre[k, pl.ds(b, 1), :], (8, 128)) for k in range(3)]
                    reach = jnp.sqrt(away[0] * away[0] + away[1] * away[1] + away[2] * away[2])
                    c, s = sincos_turns(reach * orders)
                    ec = jnp.broadcast_to(c[7:8, :], (8, 128))
                    es = jnp.broadcast_to(s[7:8, :], (8, 128))
                    state.append([c, s, ec * c - es * s, es * c + ec * s, ec + ec])
                for a in range(half // 8):
                    re_sum = acc[0, a * 8 : a * 8 + 8, t * 128 : t * 128 + 128]
                    im_sum = acc[1, a * 8 : a * 8 + 8, t * 128 : t * 128 + 128]
                    for j in range(2):
                        c, s, c_next, s_next, twice = state[j]
                        re = prod[pair + j, a * 8 : a * 8 + 8, t * 128 : t * 128 + 128]
                        im = prod[pair + j, half + a * 8 : half + a * 8 + 8, t * 128 : t * 128 + 128]
                        re_sum = re_sum + (re * c + im * s)
                        im_sum = im_sum + (im * c - re * s)
                        state[j] = [c_next, s_next, twice * c_next - c, twice * s_next - s, twice]
                    acc[0, a * 8 : a * 8 + 8, t * 128 : t * 128 + 128] = re_sum
                    acc[1, a * 8 : a * 8 + 8, t * 128 : t * 128 + 128] = im_sum
        return 0

    lax.fori_loop(0, turns, group, 0)
    if out is None:
        return
    shares, _, per, _ = out.shape
    each = 128 // per
    for k in range(2):
        for t in range(tiles):
            turned = jnp.transpose(acc[k, :, t * 128 : (t + 1) * 128])
            for e in range(each):
                out[t * each + e, k, :, :] = turned[e * per : (e + 1) * per, :]


def observe(chunk, part, parts, live, centre, sp, wts, lis, shares, before=None, ties=()):
    slots, k2, bp = sp.shape
    span = lis.shape[1] * 128 // CHUNKS
    vm = pl.BlockSpec(memory_space=pltpu.VMEM)
    sm = pl.BlockSpec(memory_space=pltpu.SMEM)
    sums = (2, k2 // 2, span)
    last = part == parts - 1
    scratch = [pltpu.VMEM((BATCH, k2, span), jnp.float32)]
    return pl.pallas_call(
        functools.partial(observe_kernel, chunk=chunk, part=part, parts=parts, ties=len(ties)),
        out_shape=jax.ShapeDtypeStruct((shares, 2, span // shares, k2 // 2) if last else sums, jnp.float32),
        in_specs=[sm, vm, vm, vm, vm] + [vm] * (part > 0) + [pl.BlockSpec(memory_space=pl.ANY)] * len(ties),
        out_specs=vm,
        scratch_shapes=scratch + [pltpu.VMEM(sums, jnp.float32)] * last,
        name="observe",
        cost_estimate=pl.CostEstimate(flops=4_000_000_000, transcendentals=0, bytes_accessed=1_000_000),
        compiler_params=pltpu.CompilerParams(vmem_limit_bytes=4 * 1024 * 1024),
    )(live, centre, sp, wts, lis, *([before] if part > 0 else []), *ties)


def swap(value, axis, bit):
    size = lax.axis_size(axis)
    return lax.ppermute(value, axis, [(i, i ^ bit) for i in range(size)])


def stages():
    def bits(axis):
        return [1 << k for k in range(lax.axis_size(axis).bit_length() - 1)]

    steps = [("halve", axis, bit) for axis in ("gz", "gx") for bit in bits(axis)]
    steps += [("sum", "gy", bit) for bit in bits("gy")]
    return steps + [("gather", "gx", bit) for bit in bits("gx")[::-1]]


def exchange(value, kind, axis, bit):
    if kind == "sum":
        return value + swap(value, axis, bit)
    up = (lax.axis_index(axis) // bit) % 2
    if kind == "gather":
        theirs = swap(value, axis, bit)
        first = jnp.where(up == 0, value, theirs)
        return jnp.concatenate([first, jnp.where(up == 0, theirs, value)], axis=2)
    if axis == "gz":
        pairs, dim = value.reshape((value.shape[0] // 2, 2) + value.shape[1:]), 1
    else:
        pairs, dim = value.reshape(value.shape[:2] + (2, value.shape[2] // 2) + value.shape[3:]), 2
    mine = lax.dynamic_index_in_dim(pairs, up, dim, keepdims=False)
    theirs = lax.dynamic_index_in_dim(pairs, 1 - up, dim, keepdims=False)
    return mine + swap(theirs, axis, bit)


def local(
    state_old,
    state_section,
    panel_record,
    panel_cell,
    panel_angles,
    owned_blocks,
    listener_angles,
    listener_range,
):
    sizes = state_section.shape[1:]
    axes = ("gx", "gy", "gz")
    counts = tuple(n * lax.axis_size(axis) for n, axis in zip(sizes, axes))
    step_size = COURANT / max(counts)
    slot_count, block_rows = panel_cell.shape
    samples = panel_record.shape[1]
    shares = lax.axis_size("gz")
    corner = jnp.stack([lax.axis_index(axis) * n for n, axis in zip(sizes, axes)]).astype(jnp.int32)
    raw = jnp.concatenate([listener_angles, listener_range[None]], axis=0)
    raw = jnp.transpose(raw.reshape(3, shares, CHUNKS, -1), (0, 2, 1, 3)).reshape(3, -1, 128)
    angles = panel_angles.reshape(2, slot_count, block_rows)
    wts, centres, listeners = weights(owned_blocks, corner, panel_cell, angles, raw, sizes, counts)
    updated, density = flow(state_old, state_section, counts, step_size)
    heard = spectra(owned_blocks, density, panel_record, panel_cell, dft_table(samples, FREQS))
    steps = stages()
    known = (owned_blocks, centres, heard, wts, listeners, shares)
    pieces, done = [], []
    for q in range(CHUNKS):
        parts = 1 if q == 0 else PARTS
        sums = None
        for part in range(parts):
            ties = []
            if part > 0:
                for k in range(len(pieces)):
                    if done[k] < len(steps):
                        pieces[k] = exchange(pieces[k], *steps[done[k]])
                        done[k] += 1
                        ties.append(pieces[k])
            sums = observe(q, part, parts, *known, sums, ties)
        pieces.append(sums)
        done.append(0)
    while min(done) < len(steps):
        for k in range(len(pieces)):
            if done[k] < len(steps):
                pieces[k] = exchange(pieces[k], *steps[done[k]])
                done[k] += 1
    pieces = [v.reshape((2, -1, FREQS)) for v in pieces]
    return (updated, jnp.concatenate(pieces, axis=1))


def solution(mesh):
    return jax.shard_map(
        local,
        mesh=mesh,
        in_specs=(
            P(None, "gx", "gy", "gz"),
            P(None, "gx", "gy", "gz"),
            P(("gx", "gy", "gz"), None),
            P(("gx", "gy", "gz"), None),
            P(None, ("gx", "gy", "gz")),
            P(("gx", "gy", "gz")),
            P(),
            P(),
        ),
        out_specs=(P(None, "gx", "gy", "gz"), P(None, "gz", None)),
        check_vma=False,
    )
```
